512 devices in a mesh: seq: 128 (over x, z, core), hid: 4 (over y).
Axes of the slice: x: 4, y: 4, z: 16, core: 2. Of those that a mesh axis runs over, the one named last changes fastest.
Arguments:
- hidden: bfloat16 [131072, 4096], P('seq', 'hid'), may hold values from -40 to 40, as said below
- seg_ids: int32 [131072], P('seq'), may hold values from 0 to 511, as said below
- lengths: int32 [512], replicated, may hold values from 64 to 16384, as said below
- owner_slot: int32 [512], replicated, may hold values from 0 to 511, each once
- pool_bias: float32 [4096], P('hid'), may hold values from -3 to 3
Outputs:
- pooled: bfloat16 [512, 4096], P('seq', 'hid')
The draws below stay inside these ranges and needn't reach their ends.
Inputs may be any that keep to these rules, and one draw needn't show every extreme that they name: `hidden`: float values; each feature's scale differs. `seg_ids`: never falls along the stream; document d occupies exactly lengths[d] consecutive tokens, documents in order. `lengths`: they sum to 131072; one of them is exactly 16384; the first 16 documents each have 1024 // 16 tokens and so fill the first index's tokens; hence at most 16 documents end within one index's tokens, and the first index has exactly 16. `owner_slot`: each row number once.
All inputs are finite; a program needn't handle non-finite values.
Results may differ from the reference program's by a relative error of at most 0.001.
Values may be sent and summed in bfloat16 or wider, within the bound.
No kernel may reach another device: no remote copies, remote signals or barrier semaphores. Data moves between devices by JAX's collectives and lax.ppermute only.
A program may use at most 64 MiB of HBM per device.

```python
import math
import jax
import jax.numpy as jnp
from jax import lax

D = 4096
TOK_DEV = 1024
FIN = 16
TOKENS = 131072
DOCS = 512
MOST = 16384
N_SEQ = 128


def doc_lengths(key):
    floor_size = TOK_DEV // FIN
    remaining = TOKENS - MOST - TOK_DEV
    others = DOCS - 1 - FIN
    even_share = remaining // others
    leftover = remaining % others
    positions = jnp.arange(others, dtype=jnp.int32)
    doc_sizes = even_share + (positions < leftover).astype(jnp.int32)
    pair_count = others // 2
    for sweep_index in range(6):
        key, pair_key, move_key = jax.random.split(key, 3)
        shuffled = jax.random.permutation(pair_key, others).astype(jnp.int32)
        giver = shuffled[0:2 * pair_count:2]
        taker = shuffled[1:2 * pair_count:2]
        headroom = jnp.minimum(doc_sizes[giver] - floor_size, MOST - doc_sizes[taker])
        transfer = jax.random.randint(move_key, (pair_count,), 0, headroom + 1).astype(jnp.int32)
        doc_sizes = doc_sizes.at[giver].add(-transfer).at[taker].add(transfer)
    tail_count = others + 1
    long_index = jax.random.randint(key, (), 0, tail_count).astype(jnp.int32)
    tail_iota = jnp.arange(tail_count, dtype=jnp.int32)
    shifted = jnp.clip(jnp.where(tail_iota < long_index, tail_iota, tail_iota - 1), 0, others - 1)
    tail = jnp.where(tail_iota == long_index, MOST, doc_sizes[shifted])
    head = jnp.full((FIN,), floor_size, jnp.int32)
    return jnp.concatenate([head, tail.astype(jnp.int32)]).astype(jnp.int32)


def draw_lengths(key, part):
    return doc_lengths(jax.random.fold_in(key, 11))


def draw_seg_ids(key, part):
    sizes_drawn = doc_lengths(jax.random.fold_in(key, 11))
    starts = jnp.cumsum(sizes_drawn) - sizes_drawn
    marks = jnp.zeros((TOKENS,), jnp.int32).at[starts[1:]].add(1)
    return jnp.cumsum(marks).astype(jnp.int32)


def draw_hidden(key, part):
    col_key = jax.random.fold_in(key, 0)
    value_key = jax.random.fold_in(key, 2)
    rising = jnp.exp2(jnp.arange(D, dtype=jnp.float32) / D)
    columns = jnp.exp(jax.random.uniform(col_key, (D,), jnp.float32, math.log(0.7), math.log(1.4)))
    values = jnp.clip(jax.random.normal(value_key, (TOKENS, D), jnp.float32), -4.0, 4.0)
    result = values * (columns * rising)[None, :]
    return result.astype(jnp.bfloat16)


def shard_levels(own_key, shape, cuts, least, high):
    def one(axis_at, shards_of):
        steps = jax.random.uniform(jax.random.fold_in(jax.random.fold_in(own_key, 6), axis_at), (shards_of,), jnp.float32, least / len(cuts), high / len(cuts))
        return jnp.repeat(jnp.exp(steps), shape[axis_at] // shards_of).reshape((-1,) + (1,) * (len(shape) - axis_at - 1))

    loudness = one(*cuts[0])
    for cut in cuts[1:]:
        loudness = loudness * one(*cut)
    return loudness


def centred(own_key, dims, scale, limit, pieces=(), kind=jnp.bfloat16):
    values = jax.random.normal(own_key, dims, jnp.float32) * scale
    if len(pieces) > 0:
        values = shard_levels(own_key, dims, pieces, -0.22, 0.18) * values
    return jnp.clip(values, min=-limit, max=limit).astype(kind)


def setup_inputs(seed: int = 0) -> dict:
    key_list = jax.random.split(jax.random.key(seed), 6)
    hidden = draw_hidden(jax.random.fold_in(key_list[5], 71), 0)
    seg_ids = draw_seg_ids(jax.random.fold_in(key_list[5], 71), 0)
    lengths = draw_lengths(jax.random.fold_in(key_list[5], 71), 0)
    owner_slot = jax.random.permutation(key_list[3], DOCS).astype(jnp.int32)
    pool_bias = centred(key_list[4], (D,), 0.5, 3.0, ((0, 4),), jnp.float32)
    return {"hidden": hidden, "seg_ids": seg_ids, "lengths": lengths, "owner_slot": owner_slot, "pool_bias": pool_bias}


def reference(hidden, seg_ids, lengths, owner_slot, pool_bias):
    token_blocks = hidden.reshape(N_SEQ, TOK_DEV, D)
    block_ids = seg_ids.reshape(N_SEQ, TOK_DEV)

    def accumulate(running, operands):
        token_block, block_docs = operands
        added = jax.ops.segment_sum(token_block.astype(jnp.float32), block_docs, num_segments=DOCS)
        return (running + added, None)
    totals, _ = lax.scan(accumulate, jnp.zeros((DOCS, D), jnp.float32), (token_blocks, block_ids))
    averages = totals / lengths.astype(jnp.float32)[:, None] + pool_bias[None, :]
    energy = lax.optimization_barrier(jnp.mean(averages * averages, axis=1, keepdims=True))
    normed = averages * lax.rsqrt(energy + 1e-06)
    placed = jnp.zeros((DOCS, D), jnp.float32).at[owner_slot].set(normed)
    return placed.astype(jnp.bfloat16)
```

```python
import functools

import jax
import jax.numpy as jnp
from jax import lax
from jax.experimental import pallas as pl
from jax.experimental.pallas import tpu as pltpu
from jax.sharding import Mesh
from jax.sharding import PartitionSpec as P

USED = 17
SLOTS = 24
LANES = 128


def plane_row(owner):
    return ((owner >> 3) & 15) * 32 + (owner >> 7) * 8 + (owner & 7)


def sums_kernel(steps, chunks, seg_ref, owner_ref, hidden_ref, out_ref):
    step = pl.program_id(0)
    first = seg_ref[0:1, 0:1]
    rows = hidden_ref.shape[0]
    seg = seg_ref[:, pl.ds(pl.multiple_of(step * rows, rows), rows)]
    slot = lax.broadcasted_iota(jnp.int32, (SLOTS, rows), 0)
    picker = jnp.where(slot == seg - first, 1.0, 0.0).astype(jnp.bfloat16)
    sums = jnp.dot(picker, hidden_ref[...], preferred_element_type=jnp.float32)

    @pl.when(step == 0)
    def _():
        docs = owner_ref.shape[1]
        source = lax.axis_index("x") * 2 + lax.axis_index("c")
        row = plane_row(owner_ref[...]) + 1
        part = lax.broadcasted_iota(jnp.int32, (8, docs), 0)
        digits = jnp.where(part == 0, row >> 5, jnp.where(part == 1, row & 31, 0))
        lane = lax.broadcasted_iota(jnp.int32, (docs, 2 * LANES), 1) - source * SLOTS
        doc = lax.broadcasted_iota(jnp.int32, (docs, 2 * LANES), 0)
        meets = (doc == first + lane) & (lane >= 0) & (lane < USED)
        found = jnp.dot(
            digits.astype(jnp.float32).astype(jnp.bfloat16),
            jnp.where(meets, 1.0, 0.0).astype(jnp.bfloat16),
            preferred_element_type=jnp.float32,
        )
        where = found[0:1, :] * 32.0 + found[1:2, :]
        line = lax.broadcasted_iota(jnp.int32, (SLOTS, LANES), 0)
        marks = jnp.where(
            line == SLOTS - 2,
            where[:, :LANES],
            jnp.where(line == SLOTS - 1, where[:, LANES:], 0.0),
        )
        for c in range(chunks):
            out_ref[c] = sums[:, c * LANES : (c + 1) * LANES] + marks

    @pl.when(step > 0)
    def _():
        for c in range(chunks):
            out_ref[c] += sums[:, c * LANES : (c + 1) * LANES]


def local_sums(seg_ids, owner_slot, hidden, chunks):
    tokens, width = hidden.shape
    steps = 4
    rows = tokens // steps
    return pl.pallas_call(
        functools.partial(sums_kernel, steps, chunks),
        grid=(steps,),
        in_specs=[
            pl.BlockSpec((1, tokens), lambda i: (0, 0)),
            pl.BlockSpec((1, owner_slot.shape[0]), lambda i: (0, 0)),
            pl.BlockSpec((rows, width), lambda i: (i, 0)),
        ],
        out_specs=pl.BlockSpec((chunks, SLOTS, LANES), lambda i: (0, 0, 0)),
        out_shape=jax.ShapeDtypeStruct((chunks, SLOTS, LANES), jnp.float32),
        name="local_sums",
    )(seg_ids.reshape(1, -1), owner_slot.reshape(1, -1), hidden)


def place_kernel(in_ref, out_ref):
    sources = in_ref.shape[0]
    planes, per_plane, _ = out_ref.shape
    slots = in_ref[...].reshape(sources * SLOTS, LANES)
    where = jnp.sum(in_ref[:, SLOTS - 2 : SLOTS, :], axis=0).astype(jnp.int32)
    row = lax.broadcasted_iota(jnp.int32, (planes * per_plane, LANES), 0) + 1
    rest = sources * SLOTS - LANES
    left = jnp.where(row == where[0:1, :], 1.0, 0.0).astype(jnp.bfloat16)
    right = jnp.where(row == where[1:2, :], 1.0, 0.0).astype(jnp.bfloat16)
    picker = jnp.concatenate([left, right], axis=1)
    total = jnp.concatenate([slots, jnp.zeros((LANES - rest, LANES), jnp.float32)], axis=0)
    high = total.astype(jnp.bfloat16)
    left_over = total - high.astype(jnp.float32)
    middle = left_over.astype(jnp.bfloat16)
    low = (left_over - middle.astype(jnp.float32)).astype(jnp.bfloat16)
    placed = jnp.dot(
        picker, jnp.concatenate([high, middle, low], axis=1), preferred_element_type=jnp.float32
    )
    whole = placed[:, :LANES] + (placed[:, LANES : 2 * LANES] + placed[:, 2 * LANES :])
    out_ref[...] = whole.reshape(out_ref.shape)


def place(slots, planes, per_plane):
    return pl.pallas_call(
        place_kernel,
        out_shape=jax.ShapeDtypeStruct((planes, per_plane, LANES), jnp.float32),
        name="place",
    )(slots)


def average_kernel(owner_ref, length_ref, bias_ref, in_ref, out_ref):
    per_plane = in_ref.shape[1]
    total = jnp.sum(in_ref[...], axis=0)
    mine = lax.axis_index("z") * per_plane
    row = lax.broadcasted_iota(jnp.int32, (per_plane, owner_ref.shape[1]), 0) + mine
    length = jnp.sum(
        jnp.where(row == plane_row(owner_ref[...]), length_ref[...], 0).astype(jnp.float32),
        axis=1,
        keepdims=True,
    )
    chunk = lax.axis_index("x") * 2 + lax.axis_index("c")
    average = total / length + bias_ref[pl.ds(chunk, 1), :]
    owners, copies, rows, _ = out_ref.shape
    for o in range(owners):
        for y in range(copies):
            out_ref[o, y] = average[o * rows : (o + 1) * rows, :]


def averages_for_owners(arrived, owner_slot, lengths, pool_bias, owners, copies):
    rows = arrived.shape[1] // owners
    return pl.pallas_call(
        average_kernel,
        out_shape=jax.ShapeDtypeStruct((owners, copies, rows, LANES), jnp.float32),
        name="average",
    )(owner_slot.reshape(1, -1), lengths.reshape(1, -1), pool_bias.reshape(-1, LANES), arrived)


def norm_kernel(in_ref, out_ref):
    chunks, slices, rows, _ = in_ref.shape
    every = in_ref[...]
    square = jnp.sum(every * every, axis=(0, 1))
    energy = jnp.sum(square, axis=1, keepdims=True) / (chunks * slices * LANES)
    scale = lax.rsqrt(energy + 1e-06)
    mine = lax.axis_index("y")
    for c in range(chunks):
        out_ref[:, c * LANES : (c + 1) * LANES] = (in_ref[c, mine] * scale).astype(jnp.bfloat16)


def normed(arrived):
    chunks, _, rows, _ = arrived.shape
    return pl.pallas_call(
        norm_kernel,
        out_shape=jax.ShapeDtypeStruct((rows, chunks * LANES), jnp.bfloat16),
        name="norm",
    )(arrived)


def swap(array, axes):
    return lax.all_to_all(array, axes, split_axis=0, concat_axis=0, tiled=True)


def local(hidden, seg_ids, lengths, owner_slot, pool_bias):
    chunks = lax.axis_size(("x", "c"))
    planes = lax.axis_size("z")
    slices = lax.axis_size("y")
    docs = lengths.shape[0]
    slots = swap(local_sums(seg_ids, owner_slot, hidden, chunks), ("x", "c"))
    rows = swap(place(slots, planes, docs // planes), "z")
    average = averages_for_owners(rows, owner_slot, lengths, pool_bias, chunks, slices)
    mine = swap(average.reshape(chunks * slices, -1, LANES), ("x", "c", "y"))
    return normed(mine.reshape(average.shape))


def solution(mesh):
    torus = Mesh(mesh.devices.reshape(4, 16, 2, mesh.shape["hid"]), ("x", "z", "c", "y"))
    seq = ("x", "z", "c")
    return jax.shard_map(
        local,
        mesh=torus,
        in_specs=(P(seq, "y"), P(seq), P(), P(), P("y")),
        out_specs=P(seq, "y"),
        check_vma=False,
    )
```

```python
import functools

import jax
import jax.numpy as jnp
from jax import lax
from jax.experimental import pallas as pl
from jax.experimental.pallas import tpu as pltpu
from jax.sharding import Mesh
from jax.sharding import PartitionSpec as P

USED = 17
SLOTS = 24
LANES = 128
GRANT = 16 * 1024 * 1024


def plane_row(owner):
    return ((owner >> 3) & 15) * 32 + (owner >> 7) * 8 + (owner & 7)


def sums_kernel(steps, chunks, seg_ref, owner_ref, hidden_ref, out_ref):
    step = pl.program_id(0)
    first = seg_ref[0:1, 0:1]
    rows = hidden_ref.shape[0]
    seg = seg_ref[:, pl.ds(pl.multiple_of(step * rows, rows), rows)]
    slot = lax.broadcasted_iota(jnp.int32, (SLOTS, rows), 0)
    picker = jnp.where(slot == seg - first, 1.0, 0.0).astype(jnp.bfloat16)
    sums = jnp.dot(picker, hidden_ref[...], preferred_element_type=jnp.float32)

    @pl.when(step == 0)
    def _():
        docs = owner_ref.shape[1]
        source = lax.axis_index("x") * 2 + lax.axis_index("c")
        row = plane_row(owner_ref[...]) + 1
        part = lax.broadcasted_iota(jnp.int32, (8, docs), 0)
        digits = jnp.where(part == 0, row >> 5, jnp.where(part == 1, row & 31, 0))
        lane = lax.broadcasted_iota(jnp.int32, (docs, 2 * LANES), 1) - source * SLOTS
        doc = lax.broadcasted_iota(jnp.int32, (docs, 2 * LANES), 0)
        meets = (doc == first + lane) & (lane >= 0) & (lane < USED)
        found = jnp.dot(
            digits.astype(jnp.float32).astype(jnp.bfloat16),
            jnp.where(meets, 1.0, 0.0).astype(jnp.bfloat16),
            preferred_element_type=jnp.float32,
        )
        where = found[0:1, :] * 32.0 + found[1:2, :]
        line = lax.broadcasted_iota(jnp.int32, (SLOTS, LANES), 0)
        marks = jnp.where(
            line == SLOTS - 2,
            where[:, :LANES],
            jnp.where(line == SLOTS - 1, where[:, LANES:], 0.0),
        )
        for c in range(chunks):
            out_ref[c] = sums[:, c * LANES : (c + 1) * LANES] + marks

    @pl.when(step > 0)
    def _():
        for c in range(chunks):
            out_ref[c] += sums[:, c * LANES : (c + 1) * LANES]


def local_sums(seg_ids, owner_slot, hidden, chunks):
    tokens, width = hidden.shape
    steps = 4
    rows = tokens // steps
    return pl.pallas_call(
        functools.partial(sums_kernel, steps, chunks),
        grid=(steps,),
        in_specs=[
            pl.BlockSpec((1, tokens), lambda i: (0, 0)),
            pl.BlockSpec((1, owner_slot.shape[0]), lambda i: (0, 0)),
            pl.BlockSpec((rows, width), lambda i: (i, 0)),
        ],
        out_specs=pl.BlockSpec((chunks, SLOTS, LANES), lambda i: (0, 0, 0)),
        out_shape=jax.ShapeDtypeStruct((chunks, SLOTS, LANES), jnp.float32),
        compiler_params=pltpu.CompilerParams(vmem_limit_bytes=GRANT),
        name="local_sums",
    )(seg_ids.reshape(1, -1), owner_slot.reshape(1, -1), hidden)


def place_kernel(in_ref, out_ref):
    sources = in_ref.shape[0]
    planes, per_plane, _ = out_ref.shape
    slots = in_ref[...].reshape(sources * SLOTS, LANES)
    where = jnp.sum(in_ref[:, SLOTS - 2 : SLOTS, :], axis=0).astype(jnp.int32)
    row = lax.broadcasted_iota(jnp.int32, (planes * per_plane, LANES), 0) + 1
    rest = sources * SLOTS - LANES
    left = jnp.where(row == where[0:1, :], 1.0, 0.0).astype(jnp.bfloat16)
    right = jnp.where(row == where[1:2, :], 1.0, 0.0).astype(jnp.bfloat16)
    picker = jnp.concatenate([left, right], axis=1)
    total = jnp.concatenate([slots, jnp.zeros((LANES - rest, LANES), jnp.float32)], axis=0)
    high = total.astype(jnp.bfloat16)
    left_over = total - high.astype(jnp.float32)
    middle = left_over.astype(jnp.bfloat16)
    low = (left_over - middle.astype(jnp.float32)).astype(jnp.bfloat16)
    placed = jnp.dot(
        picker, jnp.concatenate([high, middle, low], axis=1), preferred_element_type=jnp.float32
    )
    whole = placed[:, :LANES] + (placed[:, LANES : 2 * LANES] + placed[:, 2 * LANES :])
    out_ref[...] = whole.reshape(out_ref.shape)


def place(slots, planes, per_plane):
    return pl.pallas_call(
        place_kernel,
        out_shape=jax.ShapeDtypeStruct((planes, per_plane, LANES), jnp.float32),
        compiler_params=pltpu.CompilerParams(vmem_limit_bytes=GRANT),
        name="place",
    )(slots)


def average_kernel(owner_ref, length_ref, bias_ref, in_ref, out_ref):
    per_plane = in_ref.shape[1]
    total = jnp.sum(in_ref[...], axis=0)
    mine = lax.axis_index("z") * per_plane
    row = lax.broadcasted_iota(jnp.int32, (per_plane, owner_ref.shape[1]), 0) + mine
    length = jnp.sum(
        jnp.where(row == plane_row(owner_ref[...]), length_ref[...], 0).astype(jnp.float32),
        axis=1,
        keepdims=True,
    )
    chunk = lax.axis_index("x") * 2 + lax.axis_index("c")
    average = total / length + bias_ref[pl.ds(chunk, 1), :]
    owners, copies, rows, _ = out_ref.shape
    for o in range(owners):
        for y in range(copies):
            out_ref[o, y] = average[o * rows : (o + 1) * rows, :]


def averages_for_owners(arrived, owner_slot, lengths, pool_bias, owners, copies):
    rows = arrived.shape[1] // owners
    return pl.pallas_call(
        average_kernel,
        out_shape=jax.ShapeDtypeStruct((owners, copies, rows, LANES), jnp.float32),
        compiler_params=pltpu.CompilerParams(vmem_limit_bytes=GRANT),
        name="average",
    )(owner_slot.reshape(1, -1), lengths.reshape(1, -1), pool_bias.reshape(-1, LANES), arrived)


def norm_kernel(in_ref, out_ref):
    chunks, slices, rows, _ = in_ref.shape
    every = in_ref[...]
    square = jnp.sum(every * every, axis=(0, 1))
    energy = jnp.sum(square, axis=1, keepdims=True) / (chunks * slices * LANES)
    scale = lax.rsqrt(energy + 1e-06)
    mine = lax.axis_index("y")
    for c in range(chunks):
        out_ref[:, c * LANES : (c + 1) * LANES] = (in_ref[c, mine] * scale).astype(jnp.bfloat16)


def normed(arrived):
    chunks, _, rows, _ = arrived.shape
    return pl.pallas_call(
        norm_kernel,
        out_shape=jax.ShapeDtypeStruct((rows, chunks * LANES), jnp.bfloat16),
        compiler_params=pltpu.CompilerParams(vmem_limit_bytes=GRANT),
        name="norm",
    )(arrived)


def swap(array, axes):
    return lax.all_to_all(array, axes, split_axis=0, concat_axis=0, tiled=True)


def local(hidden, seg_ids, lengths, owner_slot, pool_bias):
    chunks = lax.axis_size(("x", "c"))
    planes = lax.axis_size("z")
    slices = lax.axis_size("y")
    docs = lengths.shape[0]
    slots = swap(local_sums(seg_ids, owner_slot, hidden, chunks), ("x", "c"))
    rows = swap(place(slots, planes, docs // planes), "z")
    average = averages_for_owners(rows, owner_slot, lengths, pool_bias, chunks, slices)
    mine = swap(average.reshape(chunks * slices, -1, LANES), ("x", "c", "y"))
    return normed(mine.reshape(average.shape))


def solution(mesh):
    torus = Mesh(mesh.devices.reshape(4, 16, 2, mesh.shape["hid"]), ("x", "z", "c", "y"))
    seq = ("x", "z", "c")
    return jax.shard_map(
        local,
        mesh=torus,
        in_specs=(P(seq, "y"), P(seq), P(), P(), P("y")),
        out_specs=P(seq, "y"),
        check_vma=False,
    )
```

```python
import functools

import jax
import jax.numpy as jnp
from jax import lax
from jax.experimental import pallas as pl
from jax.experimental.pallas import tpu as pltpu
from jax.sharding import Mesh
from jax.sharding import PartitionSpec as P

USED = 17
SLOTS = 24
LANES = 128
GRANT = 16 * 1024 * 1024
WIDE = 53 * 1024 * 1024


def plane_row(owner):
    return ((owner >> 3) & 15) * 32 + (owner >> 7) * 8 + (owner & 7)


def marks_of(first, owner):
    docs = owner.shape[1]
    source = lax.axis_index("x") * 2 + lax.axis_index("c")
    row = plane_row(owner) + 1
    part = lax.broadcasted_iota(jnp.int32, (8, docs), 0)
    digits = jnp.where(part == 0, row >> 5, jnp.where(part == 1, row & 31, 0))
    lane = lax.broadcasted_iota(jnp.int32, (docs, 2 * LANES), 1) - source * SLOTS
    doc = lax.broadcasted_iota(jnp.int32, (docs, 2 * LANES), 0)
    meets = (doc == first + lane) & (lane >= 0) & (lane < USED)
    found = jnp.dot(
        digits.astype(jnp.float32).astype(jnp.bfloat16),
        jnp.where(meets, 1.0, 0.0).astype(jnp.bfloat16),
        preferred_element_type=jnp.float32,
    )
    where = found[0:1, :] * 32.0 + found[1:2, :]
    line = lax.broadcasted_iota(jnp.int32, (SLOTS, LANES), 0)
    second = jnp.where(line == SLOTS - 1, where[:, LANES:], 0.0)
    return jnp.where(line == SLOTS - 2, where[:, :LANES], second)


def sums_kernel(pieces, seg_hbm, owner_hbm, hidden_hbm, out_ref, seg, owner, hidden, sems):
    tokens = hidden.shape[0]
    rows = tokens // pieces
    copies = [
        pltpu.make_async_copy(seg_hbm, seg, sems.at[pieces]),
        pltpu.make_async_copy(owner_hbm, owner, sems.at[pieces + 1]),
    ]
    for p in range(pieces):
        here = pl.ds(p * rows, rows)
        copies.append(pltpu.make_async_copy(hidden_hbm.at[here], hidden.at[here], sems.at[p]))
    for copy in copies:
        copy.start()
    copies[0].wait()
    first = seg[0:1, 0:1]
    copies[1].wait()
    marks = marks_of(first, owner[...])
    slot = lax.broadcasted_iota(jnp.int32, (SLOTS, rows), 0) + first
    sums = None
    for p in range(pieces):
        picker = jnp.where(slot == seg[:, p * rows : (p + 1) * rows], 1.0, 0.0)
        copies[2 + p].wait()
        term = jnp.dot(
            picker.astype(jnp.bfloat16),
            hidden[p * rows : (p + 1) * rows, :],
            preferred_element_type=jnp.float32,
        )
        sums = term if sums is None else sums + term
    for c in range(out_ref.shape[0]):
        out_ref[c] = sums[:, c * LANES : (c + 1) * LANES] + marks


def local_sums(seg_ids, owner_slot, hidden, chunks):
    tokens, width = hidden.shape
    docs = owner_slot.shape[0]
    pieces = 4
    return pl.pallas_call(
        functools.partial(sums_kernel, pieces),
        in_specs=[pl.BlockSpec(memory_space=pltpu.HBM)] * 3,
        out_specs=pl.BlockSpec(memory_space=pltpu.VMEM),
        out_shape=jax.ShapeDtypeStruct((chunks, SLOTS, LANES), jnp.float32),
        scratch_shapes=[
            pltpu.VMEM((1, tokens), jnp.int32),
            pltpu.VMEM((1, docs), jnp.int32),
            pltpu.VMEM((tokens, width), hidden.dtype),
            pltpu.SemaphoreType.DMA((pieces + 2,)),
        ],
        compiler_params=pltpu.CompilerParams(vmem_limit_bytes=WIDE),
        name="local_sums",
    )(seg_ids.reshape(1, -1), owner_slot.reshape(1, -1), hidden)


def place_kernel(in_ref, out_ref):
    sources = in_ref.shape[0]
    planes, per_plane, _ = out_ref.shape
    slots = in_ref[...].reshape(sources * SLOTS, LANES)
    where = jnp.sum(in_ref[:, SLOTS - 2 : SLOTS, :], axis=0).astype(jnp.int32)
    row = lax.broadcasted_iota(jnp.int32, (planes * per_plane, LANES), 0) + 1
    rest = sources * SLOTS - LANES
    left = jnp.where(row == where[0:1, :], 1.0, 0.0).astype(jnp.bfloat16)
    right = jnp.where(row == where[1:2, :], 1.0, 0.0).astype(jnp.bfloat16)
    picker = jnp.concatenate([left, right], axis=1)
    total = jnp.concatenate([slots, jnp.zeros((LANES - rest, LANES), jnp.float32)], axis=0)
    high = total.astype(jnp.bfloat16)
    left_over = total - high.astype(jnp.float32)
    middle = left_over.astype(jnp.bfloat16)
    low = (left_over - middle.astype(jnp.float32)).astype(jnp.bfloat16)
    placed = jnp.dot(
        picker, jnp.concatenate([high, middle, low], axis=1), preferred_element_type=jnp.float32
    )
    whole = placed[:, :LANES] + (placed[:, LANES : 2 * LANES] + placed[:, 2 * LANES :])
    out_ref[...] = whole.reshape(out_ref.shape)


def place(slots, planes, per_plane):
    return pl.pallas_call(
        place_kernel,
        out_shape=jax.ShapeDtypeStruct((planes, per_plane, LANES), jnp.float32),
        compiler_params=pltpu.CompilerParams(vmem_limit_bytes=GRANT),
        name="place",
    )(slots)


def average_kernel(owner_ref, length_ref, bias_ref, in_ref, out_ref):
    per_plane = in_ref.shape[1]
    total = jnp.sum(in_ref[...], axis=0)
    mine = lax.axis_index("z") * per_plane
    row = lax.broadcasted_iota(jnp.int32, (per_plane, owner_ref.shape[1]), 0) + mine
    length = jnp.sum(
        jnp.where(row == plane_row(owner_ref[...]), length_ref[...], 0).astype(jnp.float32),
        axis=1,
        keepdims=True,
    )
    chunk = lax.axis_index("x") * 2 + lax.axis_index("c")
    average = total / length + bias_ref[pl.ds(chunk, 1), :]
    owners, copies, rows, _ = out_ref.shape
    for o in range(owners):
        for y in range(copies):
            out_ref[o, y] = average[o * rows : (o + 1) * rows, :]


def averages_for_owners(arrived, owner_slot, lengths, pool_bias, owners, copies):
    rows = arrived.shape[1] // owners
    return pl.pallas_call(
        average_kernel,
        out_shape=jax.ShapeDtypeStruct((owners, copies, rows, LANES), jnp.float32),
        compiler_params=pltpu.CompilerParams(vmem_limit_bytes=GRANT),
        name="average",
    )(owner_slot.reshape(1, -1), lengths.reshape(1, -1), pool_bias.reshape(-1, LANES), arrived)


def norm_kernel(in_ref, out_ref):
    chunks, slices, rows, _ = in_ref.shape
    every = in_ref[...]
    square = jnp.sum(every * every, axis=(0, 1))
    energy = jnp.sum(square, axis=1, keepdims=True) / (chunks * slices * LANES)
    scale = lax.rsqrt(energy + 1e-06)
    mine = lax.axis_index("y")
    for c in range(chunks):
        out_ref[:, c * LANES : (c + 1) * LANES] = (in_ref[c, mine] * scale).astype(jnp.bfloat16)


def normed(arrived):
    chunks, _, rows, _ = arrived.shape
    return pl.pallas_call(
        norm_kernel,
        out_shape=jax.ShapeDtypeStruct((rows, chunks * LANES), jnp.bfloat16),
        compiler_params=pltpu.CompilerParams(vmem_limit_bytes=GRANT),
        name="norm",
    )(arrived)


def swap(array, axes):
    return lax.all_to_all(array, axes, split_axis=0, concat_axis=0, tiled=True)


def local(hidden, seg_ids, lengths, owner_slot, pool_bias):
    chunks = lax.axis_size(("x", "c"))
    planes = lax.axis_size("z")
    slices = lax.axis_size("y")
    docs = lengths.shape[0]
    slots = swap(local_sums(seg_ids, owner_slot, hidden, chunks), ("x", "c"))
    rows = swap(place(slots, planes, docs // planes), "z")
    average = averages_for_owners(rows, owner_slot, lengths, pool_bias, chunks, slices)
    mine = swap(average.reshape(chunks * slices, -1, LANES), ("x", "c", "y"))
    return normed(mine.reshape(average.shape))


def solution(mesh):
    torus = Mesh(mesh.devices.reshape(4, 16, 2, mesh.shape["hid"]), ("x", "z", "c", "y"))
    seq = ("x", "z", "c")
    return jax.shard_map(
        local,
        mesh=torus,
        in_specs=(P(seq, "y"), P(seq), P(), P(), P("y")),
        out_specs=P(seq, "y"),
        check_vma=False,
    )
```

```python
import functools

import jax
import jax.numpy as jnp
from jax import lax
from jax.experimental import pallas as pl
from jax.experimental.pallas import tpu as pltpu
from jax.sharding import Mesh
from jax.sharding import PartitionSpec as P

USED = 17
SLOTS = 24
LANES = 128
GRANT = 16 * 1024 * 1024
WIDE = 56 * 1024 * 1024


def plane_row(owner):
    return ((owner >> 3) & 15) * 32 + (owner >> 7) * 8 + (owner & 7)


def marks_of(first, owner):
    docs = owner.shape[1]
    source = lax.axis_index("x") * 2 + lax.axis_index("c")
    row = plane_row(owner) + 1
    part = lax.broadcasted_iota(jnp.int32, (8, docs), 0)
    digits = jnp.where(part == 0, row >> 5, jnp.where(part == 1, row & 31, 0))
    lane = lax.broadcasted_iota(jnp.int32, (docs, 2 * LANES), 1) - source * SLOTS
    doc = lax.broadcasted_iota(jnp.int32, (docs, 2 * LANES), 0)
    meets = (doc == first + lane) & (lane >= 0) & (lane < USED)
    found = jnp.dot(
        digits.astype(jnp.float32).astype(jnp.bfloat16),
        jnp.where(meets, 1.0, 0.0).astype(jnp.bfloat16),
        preferred_element_type=jnp.float32,
    )
    where = found[0:1, :] * 32.0 + found[1:2, :]
    line = lax.broadcasted_iota(jnp.int32, (SLOTS, LANES), 0)
    second = jnp.where(line == SLOTS - 1, where[:, LANES:], 0.0)
    return jnp.where(line == SLOTS - 2, where[:, :LANES], second)


def sums_kernel(pieces, seg_hbm, owner_hbm, hidden_hbm, out_ref, seg, owner, hidden, sems):
    tokens = hidden.shape[0]
    rows = tokens // pieces
    copies = [
        pltpu.make_async_copy(seg_hbm, seg, sems.at[pieces]),
        pltpu.make_async_copy(owner_hbm, owner, sems.at[pieces + 1]),
    ]
    for p in range(pieces):
        here = pl.ds(p * rows, rows)
        copies.append(pltpu.make_async_copy(hidden_hbm.at[here], hidden.at[here], sems.at[p]))
    for copy in copies:
        copy.start()
    copies[0].wait()
    first = seg[0:1, 0:1]
    copies[1].wait()
    marks = marks_of(first, owner[...])
    slot = lax.broadcasted_iota(jnp.int32, (SLOTS, rows), 0) + first
    sums = None
    for p in range(pieces):
        picker = jnp.where(slot == seg[:, p * rows : (p + 1) * rows], 1.0, 0.0)
        copies[2 + p].wait()
        term = jnp.dot(
            picker.astype(jnp.bfloat16),
            hidden[p * rows : (p + 1) * rows, :],
            preferred_element_type=jnp.float32,
        )
        sums = term if sums is None else sums + term
    for c in range(out_ref.shape[0]):
        out_ref[c] = sums[:, c * LANES : (c + 1) * LANES] + marks


def local_sums(seg_ids, owner_slot, hidden, chunks):
    tokens, width = hidden.shape
    docs = owner_slot.shape[0]
    pieces = 4
    return pl.pallas_call(
        functools.partial(sums_kernel, pieces),
        in_specs=[pl.BlockSpec(memory_space=pltpu.HBM)] * 3,
        out_specs=pl.BlockSpec(memory_space=pltpu.VMEM),
        out_shape=pltpu.VMEM((chunks, SLOTS, LANES), jnp.float32),
        scratch_shapes=[
            pltpu.VMEM((1, tokens), jnp.int32),
            pltpu.VMEM((1, docs), jnp.int32),
            pltpu.VMEM((tokens, width), hidden.dtype),
            pltpu.SemaphoreType.DMA((pieces + 2,)),
        ],
        compiler_params=pltpu.CompilerParams(vmem_limit_bytes=WIDE),
        name="local_sums",
    )(seg_ids.reshape(1, -1), owner_slot.reshape(1, -1), hidden)


def place_kernel(in_ref, out_ref):
    sources = in_ref.shape[0]
    planes, per_plane, _ = out_ref.shape
    slots = in_ref[...].reshape(sources * SLOTS, LANES)
    where = jnp.sum(in_ref[:, SLOTS - 2 : SLOTS, :], axis=0).astype(jnp.int32)
    row = lax.broadcasted_iota(jnp.int32, (planes * per_plane, LANES), 0) + 1
    rest = sources * SLOTS - LANES
    left = jnp.where(row == where[0:1, :], 1.0, 0.0).astype(jnp.bfloat16)
    right = jnp.where(row == where[1:2, :], 1.0, 0.0).astype(jnp.bfloat16)
    picker = jnp.concatenate([left, right], axis=1)
    total = jnp.concatenate([slots, jnp.zeros((LANES - rest, LANES), jnp.float32)], axis=0)
    high = total.astype(jnp.bfloat16)
    left_over = total - high.astype(jnp.float32)
    middle = left_over.astype(jnp.bfloat16)
    low = (left_over - middle.astype(jnp.float32)).astype(jnp.bfloat16)
    placed = jnp.dot(
        picker, jnp.concatenate([high, middle, low], axis=1), preferred_element_type=jnp.float32
    )
    whole = placed[:, :LANES] + (placed[:, LANES : 2 * LANES] + placed[:, 2 * LANES :])
    out_ref[...] = whole.reshape(out_ref.shape)


def place(slots, planes, per_plane):
    return pl.pallas_call(
        place_kernel,
        out_shape=jax.ShapeDtypeStruct((planes, per_plane, LANES), jnp.float32),
        compiler_params=pltpu.CompilerParams(vmem_limit_bytes=GRANT),
        name="place",
    )(slots)


def average_kernel(owner_ref, length_ref, bias_ref, in_ref, out_ref):
    per_plane = in_ref.shape[1]
    total = jnp.sum(in_ref[...], axis=0)
    mine = lax.axis_index("z") * per_plane
    row = lax.broadcasted_iota(jnp.int32, (per_plane, owner_ref.shape[1]), 0) + mine
    length = jnp.sum(
        jnp.where(row == plane_row(owner_ref[...]), length_ref[...], 0).astype(jnp.float32),
        axis=1,
        keepdims=True,
    )
    chunk = lax.axis_index("x") * 2 + lax.axis_index("c")
    average = total / length + bias_ref[pl.ds(chunk, 1), :]
    owners, copies, rows, _ = out_ref.shape
    for o in range(owners):
        for y in range(copies):
            out_ref[o, y] = average[o * rows : (o + 1) * rows, :]


def averages_for_owners(arrived, owner_slot, lengths, pool_bias, owners, copies):
    rows = arrived.shape[1] // owners
    return pl.pallas_call(
        average_kernel,
        out_shape=jax.ShapeDtypeStruct((owners, copies, rows, LANES), jnp.float32),
        compiler_params=pltpu.CompilerParams(vmem_limit_bytes=GRANT),
        name="average",
    )(owner_slot.reshape(1, -1), lengths.reshape(1, -1), pool_bias.reshape(-1, LANES), arrived)


def norm_kernel(in_ref, out_ref):
    chunks, slices, rows, _ = in_ref.shape
    every = in_ref[...]
    square = jnp.sum(every * every, axis=(0, 1))
    energy = jnp.sum(square, axis=1, keepdims=True) / (chunks * slices * LANES)
    scale = lax.rsqrt(energy + 1e-06)
    mine = lax.axis_index("y")
    for c in range(chunks):
        out_ref[:, c * LANES : (c + 1) * LANES] = (in_ref[c, mine] * scale).astype(jnp.bfloat16)


def normed(arrived):
    chunks, _, rows, _ = arrived.shape
    return pl.pallas_call(
        norm_kernel,
        out_shape=jax.ShapeDtypeStruct((rows, chunks * LANES), jnp.bfloat16),
        compiler_params=pltpu.CompilerParams(vmem_limit_bytes=GRANT),
        name="norm",
    )(arrived)


def swap(array, axes):
    return lax.all_to_all(array, axes, split_axis=0, concat_axis=0, tiled=True)


def local(hidden, seg_ids, lengths, owner_slot, pool_bias):
    chunks = lax.axis_size(("x", "c"))
    planes = lax.axis_size("z")
    slices = lax.axis_size("y")
    docs = lengths.shape[0]
    slots = swap(local_sums(seg_ids, owner_slot, hidden, chunks), ("x", "c"))
    rows = swap(place(slots, planes, docs // planes), "z")
    average = averages_for_owners(rows, owner_slot, lengths, pool_bias, chunks, slices)
    mine = swap(average.reshape(chunks * slices, -1, LANES), ("x", "c", "y"))
    return normed(mine.reshape(average.shape))


def solution(mesh):
    torus = Mesh(mesh.devices.reshape(4, 16, 2, mesh.shape["hid"]), ("x", "z", "c", "y"))
    seq = ("x", "z", "c")
    return jax.shard_map(
        local,
        mesh=torus,
        in_specs=(P(seq, "y"), P(seq), P(), P(), P("y")),
        out_specs=P(seq, "y"),
        check_vma=False,
    )
```

```python
import functools

import jax
import jax.numpy as jnp
from jax import lax
from jax.experimental import pallas as pl
from jax.experimental.pallas import tpu as pltpu
from jax.sharding import Mesh
from jax.sharding import PartitionSpec as P

USED = 17
SLOTS = 24
LANES = 128
FIT = 14
ROWS = 16
GRANT = 16 * 1024 * 1024
WIDE = 56 * 1024 * 1024


def plane_row(owner):
    return ((owner >> 3) & 15) * 32 + (owner >> 7) * 8 + (owner & 7)


def ones(mask):
    return jnp.where(mask, 1.0, 0.0).astype(jnp.bfloat16)


def iota(shape, dim):
    return lax.broadcasted_iota(jnp.int32, shape, dim)


def small(array):
    return array.astype(jnp.float32).astype(jnp.bfloat16)


def dot(left, right):
    return jnp.dot(left, right, preferred_element_type=jnp.float32)


def dot_rows(left, right):
    return lax.dot_general(
        left, right, (((1,), (1,)), ((), ())), preferred_element_type=jnp.float32
    )


def picked(picker, values):
    high = values.astype(jnp.bfloat16)
    left_over = values - high.astype(jnp.float32)
    middle = left_over.astype(jnp.bfloat16)
    low = (left_over - middle.astype(jnp.float32)).astype(jnp.bfloat16)
    parts = dot(picker, jnp.concatenate([high, middle, low], axis=1))
    return parts[:, :LANES] + (parts[:, LANES : 2 * LANES] + parts[:, 2 * LANES :])


def marks_of(first, last, owner):
    docs = owner.shape[1]
    source = lax.axis_index("x") * 2 + lax.axis_index("c")
    row = plane_row(owner) + 1
    part = iota((8, docs), 0)
    digits = jnp.where(part == 0, row >> 5, jnp.where(part == 1, row & 31, 0))
    lane = iota((docs, 2 * LANES), 1) - source * SLOTS
    doc = iota((docs, 2 * LANES), 0)
    meets = (doc == first + lane) & (doc <= last) & (lane >= 0) & (lane < USED)
    found = dot(small(digits), ones(meets))
    where = found[0:1, :] * 32.0 + found[1:2, :]
    line = iota((SLOTS, LANES), 0)
    second = jnp.where(line == SLOTS - 1, where[:, LANES:], 0.0)
    return jnp.where(line == SLOTS - 2, where[:, :LANES], second)


def most_rows(lengths, owner, tokens):
    docs = owner.shape[1]
    part = iota((8, docs), 0)
    digits = jnp.where(part == 0, lengths >> 7, jnp.where(part == 1, lengths & 127, 0))
    until = ones(iota((docs, docs), 0) <= iota((docs, docs), 1))
    sums = dot(small(digits), until)
    end = (sums[0:1, :] * 128.0 + sums[1:2, :]).astype(jnp.int32)
    start = end - lengths
    line = iota((LANES, docs), 0)
    device = (line >> 5) * 32 + (line & 15) * 2 + ((line >> 4) & 1)
    touches = (start < (device + 1) * tokens) & (end > device * tokens)
    owned = ((owner >> 3) & 15) == line
    counts = dot_rows(ones(touches), ones(owned))
    return jnp.max(jnp.sum(counts.reshape(8, 16, LANES), axis=0))


def sums_kernel(
    pieces, seg_hbm, owner_hbm, length_hbm, hidden_hbm, out_ref, seg, owner, length, hidden, sems
):
    tokens = hidden.shape[0]
    rows = tokens // pieces
    copies = [
        pltpu.make_async_copy(seg_hbm, seg, sems.at[pieces]),
        pltpu.make_async_copy(owner_hbm, owner, sems.at[pieces + 1]),
        pltpu.make_async_copy(length_hbm, length, sems.at[pieces + 2]),
    ]
    for p in range(pieces):
        here = pl.ds(p * rows, rows)
        copies.append(pltpu.make_async_copy(hidden_hbm.at[here], hidden.at[here], sems.at[p]))
    for copy in copies:
        copy.start()
    copies[0].wait()
    first = seg[0:1, 0:1]
    last = seg[0:1, tokens - 1 : tokens]
    copies[1].wait()
    marks = marks_of(first, last, owner[...])
    copies[2].wait()
    over = jnp.where(most_rows(length[...], owner[...], tokens) > FIT, 1.0, 0.0)
    marks = jnp.where((iota((SLOTS, LANES), 0) == SLOTS - 1) & (iota((SLOTS, LANES), 1) == LANES - 1), over, marks)
    slot = iota((SLOTS, rows), 0) + first
    sums = None
    for p in range(pieces):
        picker = ones(slot == seg[:, p * rows : (p + 1) * rows])
        copies[3 + p].wait()
        term = dot(picker, hidden[p * rows : (p + 1) * rows, :])
        sums = term if sums is None else sums + term
    for c in range(out_ref.shape[0]):
        out_ref[c] = sums[:, c * LANES : (c + 1) * LANES] + marks


def local_sums(seg_ids, owner_slot, lengths, hidden, chunks):
    tokens, width = hidden.shape
    docs = owner_slot.shape[0]
    pieces = 4
    return pl.pallas_call(
        functools.partial(sums_kernel, pieces),
        in_specs=[pl.BlockSpec(memory_space=pltpu.HBM)] * 4,
        out_specs=pl.BlockSpec(memory_space=pltpu.VMEM),
        out_shape=pltpu.VMEM((chunks, SLOTS, LANES), jnp.float32),
        scratch_shapes=[
            pltpu.VMEM((1, tokens), jnp.int32),
            pltpu.VMEM((1, docs), jnp.int32),
            pltpu.VMEM((1, docs), jnp.int32),
            pltpu.VMEM((tokens, width), hidden.dtype),
            pltpu.SemaphoreType.DMA((pieces + 3,)),
        ],
        compiler_params=pltpu.CompilerParams(vmem_limit_bytes=WIDE),
        name="local_sums",
    )(seg_ids.reshape(1, -1), owner_slot.reshape(1, -1), lengths.reshape(1, -1), hidden)


def slots_of(in_ref):
    sources = in_ref.shape[0]
    values = in_ref[...].reshape(sources * SLOTS, LANES)
    empty = jnp.zeros((2 * LANES - sources * SLOTS, LANES), jnp.float32)
    marks = jnp.sum(in_ref[:, SLOTS - 2 : SLOTS, :], axis=0).astype(jnp.int32)
    where = jnp.concatenate([marks[0:1, :], marks[1:2, :]], axis=1)
    where = jnp.where(iota(where.shape, 1) < sources * SLOTS, where, 0)
    plane = jnp.where(where > 0, (where - 1) >> 5, -1)
    bound = iota((16, 2 * LANES), 0) == plane
    ahead = iota((2 * LANES, 2 * LANES), 0) < iota((2 * LANES, 2 * LANES), 1)
    seen = dot(ones(bound), ones(ahead))
    rank = jnp.sum(jnp.where(bound, seen, 0.0), axis=0, keepdims=True).astype(jnp.int32)
    return jnp.concatenate([values, empty], axis=0), where, plane, bound, rank


def place_kernel(in_ref, out_ref, kept_ref, none_ref, over_ref):
    planes = out_ref.shape[0]
    kept_ref[...] = in_ref[...]
    none_ref[...] = jnp.zeros_like(none_ref)
    over_ref[0] = jnp.max(in_ref[0, SLOTS - 1 : SLOTS, LANES - 1 : LANES]).astype(jnp.int32)
    values, where, plane, bound, rank = slots_of(in_ref)
    target = jnp.where((where > 0) & (rank < FIT), plane * ROWS + rank, -1)
    placed = picked(ones(iota((planes * ROWS, 2 * LANES), 0) == target), values)
    number = jnp.where(bound, ((where - 1) & 31) + 1, 0)
    lane = iota((2 * LANES, 2 * LANES), 0) - lax.axis_index("z") * ROWS
    numbers = dot_rows(small(number), ones((lane == rank) & (rank < FIT)))
    placed = placed.reshape(out_ref.shape)
    line = iota(out_ref.shape, 1)
    near = numbers[:, :LANES].reshape(planes, 1, LANES)
    far = numbers[:, LANES:].reshape(planes, 1, LANES)
    out_ref[...] = jnp.where(line == FIT, near, jnp.where(line == FIT + 1, far, placed))


def place(slots, planes, per_plane):
    return pl.pallas_call(
        place_kernel,
        out_specs=[
            pl.BlockSpec(memory_space=pltpu.VMEM),
            pl.BlockSpec(memory_space=pltpu.VMEM),
            pl.BlockSpec(memory_space=pltpu.VMEM),
            pl.BlockSpec(memory_space=pltpu.SMEM),
        ],
        out_shape=[
            pltpu.VMEM((planes, ROWS, LANES), jnp.float32),
            pltpu.VMEM(slots.shape, slots.dtype),
            pltpu.VMEM((per_plane, LANES), jnp.float32),
            jax.ShapeDtypeStruct((1,), jnp.int32),
        ],
        compiler_params=pltpu.CompilerParams(vmem_limit_bytes=GRANT),
        name="place",
    )(slots)


def place_rest_kernel(in_ref, out_ref):
    planes, per_plane, _ = out_ref.shape
    values, where, _, _, rank = slots_of(in_ref)
    row = iota((planes * per_plane, 2 * LANES), 0) + 1
    out_ref[...] = picked(ones((row == where) & (rank >= FIT)), values).reshape(out_ref.shape)


def place_rest(slots, planes, per_plane):
    return pl.pallas_call(
        place_rest_kernel,
        out_shape=jax.ShapeDtypeStruct((planes, per_plane, LANES), jnp.float32),
        compiler_params=pltpu.CompilerParams(vmem_limit_bytes=GRANT),
        name="place_rest",
    )(slots)


def average_kernel(owner_ref, length_ref, bias_ref, in_ref, rest_ref, out_ref):
    planes = in_ref.shape[0]
    per_plane = rest_ref.shape[0]
    marks = jnp.sum(in_ref[:, FIT : FIT + 2, :], axis=0).astype(jnp.int32)
    where = jnp.concatenate([marks[0:1, :], marks[1:2, :]], axis=1)
    picker = ones(iota((per_plane, planes * ROWS), 0) + 1 == where)
    total = picked(picker, in_ref[...].reshape(planes * ROWS, LANES)) + rest_ref[...]
    mine = lax.axis_index("z") * per_plane
    row = iota((per_plane, owner_ref.shape[1]), 0) + mine
    length = jnp.sum(
        jnp.where(row == plane_row(owner_ref[...]), length_ref[...], 0).astype(jnp.float32),
        axis=1,
        keepdims=True,
    )
    chunk = lax.axis_index("x") * 2 + lax.axis_index("c")
    average = total / length + bias_ref[pl.ds(chunk, 1), :]
    owners, copies, rows, _ = out_ref.shape
    for o in range(owners):
        for y in range(copies):
            out_ref[o, y] = average[o * rows : (o + 1) * rows, :]


def averages_for_owners(arrived, rest, owner_slot, lengths, pool_bias, owners, copies):
    rows = rest.shape[0] // owners
    return pl.pallas_call(
        average_kernel,
        out_shape=jax.ShapeDtypeStruct((owners, copies, rows, LANES), jnp.float32),
        compiler_params=pltpu.CompilerParams(vmem_limit_bytes=GRANT),
        name="average",
    )(owner_slot.reshape(1, -1), lengths.reshape(1, -1), pool_bias.reshape(-1, LANES), arrived, rest)


def norm_kernel(in_ref, out_ref):
    chunks, slices, rows, _ = in_ref.shape
    every = in_ref[...]
    square = jnp.sum(every * every, axis=(0, 1))
    energy = jnp.sum(square, axis=1, keepdims=True) / (chunks * slices * LANES)
    scale = lax.rsqrt(energy + 1e-06)
    mine = lax.axis_index("y")
    for c in range(chunks):
        out_ref[:, c * LANES : (c + 1) * LANES] = (in_ref[c, mine] * scale).astype(jnp.bfloat16)


def normed(arrived):
    chunks, _, rows, _ = arrived.shape
    return pl.pallas_call(
        norm_kernel,
        out_shape=jax.ShapeDtypeStruct((rows, chunks * LANES), jnp.bfloat16),
        compiler_params=pltpu.CompilerParams(vmem_limit_bytes=GRANT),
        name="norm",
    )(arrived)


def swap(array, axes):
    return lax.all_to_all(array, axes, split_axis=0, concat_axis=0, tiled=True)


def local(hidden, seg_ids, lengths, owner_slot, pool_bias):
    chunks = lax.axis_size(("x", "c"))
    planes = lax.axis_size("z")
    slices = lax.axis_size("y")
    per_plane = lengths.shape[0] // planes
    slots = swap(local_sums(seg_ids, owner_slot, lengths, hidden, chunks), ("x", "c"))
    placed, kept, none, over = place(slots, planes, per_plane)
    rows = swap(placed, "z")
    rest = lax.cond(
        over[0] > 0,
        lambda slots, none: jnp.sum(swap(place_rest(slots, planes, per_plane), "z"), axis=0),
        lambda slots, none: none,
        kept,
        none,
    )
    average = averages_for_owners(rows, rest, owner_slot, lengths, pool_bias, chunks, slices)
    mine = swap(average.reshape(chunks * slices, -1, LANES), ("x", "c", "y"))
    return normed(mine.reshape(average.shape))


def solution(mesh):
    torus = Mesh(mesh.devices.reshape(4, 16, 2, mesh.shape["hid"]), ("x", "z", "c", "y"))
    seq = ("x", "z", "c")
    return jax.shard_map(
        local,
        mesh=torus,
        in_specs=(P(seq, "y"), P(seq), P(), P(), P("y")),
        out_specs=P(seq, "y"),
        check_vma=False,
    )
```

```python
import functools

import jax
import jax.numpy as jnp
from jax import lax
from jax.experimental import pallas as pl
from jax.experimental.pallas import tpu as pltpu
from jax.sharding import Mesh
from jax.sharding import PartitionSpec as P

USED = 17
SLOTS = 24
LANES = 128
FIT = 14
ROWS = 16
GRANT = 16 * 1024 * 1024
WIDE = 56 * 1024 * 1024


def plane_row(owner):
    return ((owner >> 3) & 15) * 32 + (owner >> 7) * 8 + (owner & 7)


def ones(mask):
    return jnp.where(mask, 1.0, 0.0).astype(jnp.bfloat16)


def iota(shape, dim):
    return lax.broadcasted_iota(jnp.int32, shape, dim)


def small(array):
    return array.astype(jnp.float32).astype(jnp.bfloat16)


def dot(left, right):
    return jnp.dot(left, right, preferred_element_type=jnp.float32)


def dot_rows(left, right):
    return lax.dot_general(
        left, right, (((1,), (1,)), ((), ())), preferred_element_type=jnp.float32
    )


def picked(picker, values):
    high = values.astype(jnp.bfloat16)
    left_over = values - high.astype(jnp.float32)
    middle = left_over.astype(jnp.bfloat16)
    low = (left_over - middle.astype(jnp.float32)).astype(jnp.bfloat16)
    parts = dot(picker, jnp.concatenate([high, middle, low], axis=1))
    return parts[:, :LANES] + (parts[:, LANES : 2 * LANES] + parts[:, 2 * LANES :])


def marks_of(first, last, owner):
    docs = owner.shape[1]
    source = lax.axis_index("x") * 2 + lax.axis_index("c")
    row = plane_row(owner) + 1
    part = iota((8, docs), 0)
    digits = jnp.where(part == 0, row >> 5, jnp.where(part == 1, row & 31, 0))
    lane = iota((docs, 2 * LANES), 1) - source * SLOTS
    doc = iota((docs, 2 * LANES), 0)
    meets = (doc == first + lane) & (doc <= last) & (lane >= 0) & (lane < USED)
    found = dot(small(digits), ones(meets))
    where = found[0:1, :] * 32.0 + found[1:2, :]
    line = iota((SLOTS, LANES), 0)
    second = jnp.where(line == SLOTS - 1, where[:, LANES:], 0.0)
    return jnp.where(line == SLOTS - 2, where[:, :LANES], second)


def most_rows(lengths, owner, tokens):
    docs = owner.shape[1]
    part = iota((8, docs), 0)
    digits = jnp.where(part == 0, lengths >> 7, jnp.where(part == 1, lengths & 127, 0))
    until = ones(iota((docs, docs), 0) <= iota((docs, docs), 1))
    sums = dot(small(digits), until)
    end = (sums[0:1, :] * 128.0 + sums[1:2, :]).astype(jnp.int32)
    start = end - lengths
    line = iota((LANES, docs), 0)
    device = (line >> 5) * 32 + (line & 15) * 2 + ((line >> 4) & 1)
    touches = (start < (device + 1) * tokens) & (end > device * tokens)
    owned = ((owner >> 3) & 15) == line
    counts = dot_rows(ones(touches), ones(owned))
    return jnp.max(jnp.sum(counts.reshape(8, 16, LANES), axis=0))


def sums_kernel(
    pieces, seg_hbm, owner_hbm, length_hbm, hidden_hbm, out_ref, seg, owner, length, hidden, sems
):
    tokens = hidden.shape[0]
    rows = tokens // pieces
    copies = [
        pltpu.make_async_copy(seg_hbm, seg, sems.at[pieces]),
        pltpu.make_async_copy(owner_hbm, owner, sems.at[pieces + 1]),
        pltpu.make_async_copy(length_hbm, length, sems.at[pieces + 2]),
    ]
    for p in range(pieces):
        here = pl.ds(p * rows, rows)
        copies.append(pltpu.make_async_copy(hidden_hbm.at[here], hidden.at[here], sems.at[p]))
    for copy in copies:
        copy.start()
    copies[0].wait()
    first = seg[0:1, 0:1]
    last = seg[0:1, tokens - 1 : tokens]
    copies[1].wait()
    marks = marks_of(first, last, owner[...])
    copies[2].wait()
    over = jnp.where(most_rows(length[...], owner[...], tokens) > FIT, 1.0, 0.0)
    marks = jnp.where((iota((SLOTS, LANES), 0) == SLOTS - 1) & (iota((SLOTS, LANES), 1) == LANES - 1), over, marks)
    slot = iota((SLOTS, rows), 0) + first
    sums = None
    for p in range(pieces):
        picker = ones(slot == seg[:, p * rows : (p + 1) * rows])
        copies[3 + p].wait()
        term = dot(picker, hidden[p * rows : (p + 1) * rows, :])
        sums = term if sums is None else sums + term
    for c in range(out_ref.shape[0]):
        out_ref[c] = sums[:, c * LANES : (c + 1) * LANES] + marks


def local_sums(seg_ids, owner_slot, lengths, hidden, chunks):
    tokens, width = hidden.shape
    docs = owner_slot.shape[0]
    pieces = 4
    return pl.pallas_call(
        functools.partial(sums_kernel, pieces),
        in_specs=[pl.BlockSpec(memory_space=pltpu.HBM)] * 4,
        out_specs=pl.BlockSpec(memory_space=pltpu.VMEM),
        out_shape=pltpu.VMEM((chunks, SLOTS, LANES), jnp.float32),
        scratch_shapes=[
            pltpu.VMEM((1, tokens), jnp.int32),
            pltpu.VMEM((1, docs), jnp.int32),
            pltpu.VMEM((1, docs), jnp.int32),
            pltpu.VMEM((tokens, width), hidden.dtype),
            pltpu.SemaphoreType.DMA((pieces + 3,)),
        ],
        compiler_params=pltpu.CompilerParams(vmem_limit_bytes=WIDE),
        name="local_sums",
    )(seg_ids.reshape(1, -1), owner_slot.reshape(1, -1), lengths.reshape(1, -1), hidden)


def slots_of(in_ref):
    sources = in_ref.shape[0]
    values = in_ref[...].reshape(sources * SLOTS, LANES)
    empty = jnp.zeros((2 * LANES - sources * SLOTS, LANES), jnp.float32)
    marks = jnp.sum(in_ref[:, SLOTS - 2 : SLOTS, :], axis=0).astype(jnp.int32)
    where = jnp.concatenate([marks[0:1, :], marks[1:2, :]], axis=1)
    where = jnp.where(iota(where.shape, 1) < sources * SLOTS, where, 0)
    plane = jnp.where(where > 0, (where - 1) >> 5, -1)
    bound = iota((16, 2 * LANES), 0) == plane
    ahead = iota((2 * LANES, 2 * LANES), 0) < iota((2 * LANES, 2 * LANES), 1)
    seen = dot(ones(bound), ones(ahead))
    rank = jnp.sum(jnp.where(bound, seen, 0.0), axis=0, keepdims=True).astype(jnp.int32)
    return jnp.concatenate([values, empty], axis=0), where, plane, bound, rank


def place_kernel(in_ref, out_ref, kept_ref, over_ref):
    planes = out_ref.shape[0]
    kept_ref[...] = in_ref[...]
    over_ref[0] = jnp.max(in_ref[0, SLOTS - 1 : SLOTS, LANES - 1 : LANES]).astype(jnp.int32)
    values, where, plane, bound, rank = slots_of(in_ref)
    target = jnp.where((where > 0) & (rank < FIT), plane * ROWS + rank, -1)
    placed = picked(ones(iota((planes * ROWS, 2 * LANES), 0) == target), values)
    number = jnp.where(bound, ((where - 1) & 31) + 1, 0)
    lane = iota((2 * LANES, 2 * LANES), 0) - lax.axis_index("z") * ROWS
    numbers = dot_rows(small(number), ones((lane == rank) & (rank < FIT)))
    placed = placed.reshape(out_ref.shape)
    line = iota(out_ref.shape, 1)
    near = numbers[:, :LANES].reshape(planes, 1, LANES)
    far = numbers[:, LANES:].reshape(planes, 1, LANES)
    out_ref[...] = jnp.where(line == FIT, near, jnp.where(line == FIT + 1, far, placed))


def place(slots, planes):
    return pl.pallas_call(
        place_kernel,
        out_specs=[
            pl.BlockSpec(memory_space=pltpu.VMEM),
            pl.BlockSpec(memory_space=pltpu.VMEM),
            pl.BlockSpec(memory_space=pltpu.SMEM),
        ],
        out_shape=[
            pltpu.VMEM((planes, ROWS, LANES), jnp.float32),
            pltpu.VMEM(slots.shape, slots.dtype),
            jax.ShapeDtypeStruct((1,), jnp.int32),
        ],
        compiler_params=pltpu.CompilerParams(vmem_limit_bytes=GRANT),
        name="place",
    )(slots)


def place_rest_kernel(in_ref, out_ref):
    planes, per_plane, _ = out_ref.shape
    values, where, _, _, rank = slots_of(in_ref)
    row = iota((planes * per_plane, 2 * LANES), 0) + 1
    out_ref[...] = picked(ones((row == where) & (rank >= FIT)), values).reshape(out_ref.shape)


def place_rest(slots, planes, per_plane):
    return pl.pallas_call(
        place_rest_kernel,
        out_shape=jax.ShapeDtypeStruct((planes, per_plane, LANES), jnp.float32),
        compiler_params=pltpu.CompilerParams(vmem_limit_bytes=GRANT),
        name="place_rest",
    )(slots)


def average_kernel(owner_ref, length_ref, bias_ref, in_ref, *rest_and_out):
    out_ref = rest_and_out[-1]
    planes = in_ref.shape[0]
    per_plane = owner_ref.shape[1] // planes
    marks = jnp.sum(in_ref[:, FIT : FIT + 2, :], axis=0).astype(jnp.int32)
    where = jnp.concatenate([marks[0:1, :], marks[1:2, :]], axis=1)
    picker = ones(iota((per_plane, planes * ROWS), 0) + 1 == where)
    total = picked(picker, in_ref[...].reshape(planes * ROWS, LANES))
    for rest_ref in rest_and_out[:-1]:
        total = total + jnp.sum(rest_ref[...], axis=0)
    mine = lax.axis_index("z") * per_plane
    row = iota((per_plane, owner_ref.shape[1]), 0) + mine
    length = jnp.sum(
        jnp.where(row == plane_row(owner_ref[...]), length_ref[...], 0).astype(jnp.float32),
        axis=1,
        keepdims=True,
    )
    chunk = lax.axis_index("x") * 2 + lax.axis_index("c")
    average = total / length + bias_ref[pl.ds(chunk, 1), :]
    owners, copies, rows, _ = out_ref.shape
    for o in range(owners):
        for y in range(copies):
            out_ref[o, y] = average[o * rows : (o + 1) * rows, :]


def averages_for_owners(arrived, owner_slot, lengths, pool_bias, owners, copies, *rest):
    rows = owner_slot.shape[0] // (arrived.shape[0] * owners)
    return pl.pallas_call(
        average_kernel,
        out_shape=jax.ShapeDtypeStruct((owners, copies, rows, LANES), jnp.float32),
        compiler_params=pltpu.CompilerParams(vmem_limit_bytes=GRANT),
        name="average",
    )(owner_slot.reshape(1, -1), lengths.reshape(1, -1), pool_bias.reshape(-1, LANES), arrived, *rest)


def norm_kernel(in_ref, out_ref):
    chunks, slices, rows, _ = in_ref.shape
    every = in_ref[...]
    square = jnp.sum(every * every, axis=(0, 1))
    energy = jnp.sum(square, axis=1, keepdims=True) / (chunks * slices * LANES)
    scale = lax.rsqrt(energy + 1e-06)
    mine = lax.axis_index("y")
    for c in range(chunks):
        out_ref[:, c * LANES : (c + 1) * LANES] = (in_ref[c, mine] * scale).astype(jnp.bfloat16)


def normed(arrived):
    chunks, _, rows, _ = arrived.shape
    return pl.pallas_call(
        norm_kernel,
        out_shape=jax.ShapeDtypeStruct((rows, chunks * LANES), jnp.bfloat16),
        compiler_params=pltpu.CompilerParams(vmem_limit_bytes=GRANT),
        name="norm",
    )(arrived)


def swap(array, axes):
    return lax.all_to_all(array, axes, split_axis=0, concat_axis=0, tiled=True)


def local(hidden, seg_ids, lengths, owner_slot, pool_bias):
    chunks = lax.axis_size(("x", "c"))
    planes = lax.axis_size("z")
    slices = lax.axis_size("y")
    per_plane = lengths.shape[0] // planes
    slots = swap(local_sums(seg_ids, owner_slot, lengths, hidden, chunks), ("x", "c"))
    placed, kept, over = place(slots, planes)
    rows = swap(placed, "z")
    args = (owner_slot, lengths, pool_bias, chunks, slices)

    def with_rest(rows, kept):
        rest = swap(place_rest(kept, planes, per_plane), "z")
        return averages_for_owners(rows, *args, rest)

    def alone(rows, kept):
        return averages_for_owners(rows, *args)

    average = lax.cond(over[0] > 0, with_rest, alone, rows, kept)
    mine = swap(average.reshape(chunks * slices, -1, LANES), ("x", "c", "y"))
    return normed(mine.reshape(average.shape))


def solution(mesh):
    torus = Mesh(mesh.devices.reshape(4, 16, 2, mesh.shape["hid"]), ("x", "z", "c", "y"))
    seq = ("x", "z", "c")
    return jax.shard_map(
        local,
        mesh=torus,
        in_specs=(P(seq, "y"), P(seq), P(), P(), P("y")),
        out_specs=P(seq, "y"),
        check_vma=False,
    )
```

```python
import functools

import jax
import jax.numpy as jnp
from jax import lax
from jax.experimental import pallas as pl
from jax.experimental.pallas import tpu as pltpu
from jax.sharding import Mesh
from jax.sharding import PartitionSpec as P

USED = 17
SLOTS = 24
LANES = 128
FIT = 14
ROWS = 16
GRANT = 16 * 1024 * 1024
WIDE = 56 * 1024 * 1024


def chunk_place():
    return (((lax.axis_index("x") + 2) & 3) * 2 + lax.axis_index("c")) ^ 1


def plane_place(z):
    return (z + 8) & 15


def slice_place():
    return (lax.axis_index("y") + 2) & 3


CHUNK_GROUP = [[(((j >> 1) + 2) & 3) * 2 + (j & 1) ^ 1 for j in range(8)]]
PLANE_GROUP = [[(j + 8) & 15 for j in range(16)]]
OWNER_GROUP = [[(j & ~3) + ((j + 2) & 3) for j in range(32)]]


def plane_row(owner):
    return plane_place(owner >> 3) * 32 + (owner >> 7) * 8 + (owner & 7)


def ones(mask):
    return jnp.where(mask, 1.0, 0.0).astype(jnp.bfloat16)


def iota(shape, dim):
    return lax.broadcasted_iota(jnp.int32, shape, dim)


def small(array):
    return array.astype(jnp.float32).astype(jnp.bfloat16)


def dot(left, right):
    return jnp.dot(left, right, preferred_element_type=jnp.float32)


def dot_rows(left, right):
    return lax.dot_general(
        left, right, (((1,), (1,)), ((), ())), preferred_element_type=jnp.float32
    )


def picked(picker, values):
    high = values.astype(jnp.bfloat16)
    left_over = values - high.astype(jnp.float32)
    middle = left_over.astype(jnp.bfloat16)
    low = (left_over - middle.astype(jnp.float32)).astype(jnp.bfloat16)
    parts = dot(picker, jnp.concatenate([high, middle, low], axis=1))
    return parts[:, :LANES] + (parts[:, LANES : 2 * LANES] + parts[:, 2 * LANES :])


def marks_of(first, last, owner):
    docs = owner.shape[1]
    source = chunk_place()
    row = plane_row(owner) + 1
    part = iota((8, docs), 0)
    digits = jnp.where(part == 0, row >> 5, jnp.where(part == 1, row & 31, 0))
    lane = iota((docs, 2 * LANES), 1) - source * SLOTS
    doc = iota((docs, 2 * LANES), 0)
    meets = (doc == first + lane) & (doc <= last) & (lane >= 0) & (lane < USED)
    found = dot(small(digits), ones(meets))
    where = found[0:1, :] * 32.0 + found[1:2, :]
    line = iota((SLOTS, LANES), 0)
    second = jnp.where(line == SLOTS - 1, where[:, LANES:], 0.0)
    return jnp.where(line == SLOTS - 2, where[:, :LANES], second)


def most_rows(lengths, owner, tokens):
    docs = owner.shape[1]
    part = iota((8, docs), 0)
    digits = jnp.where(part == 0, lengths >> 7, jnp.where(part == 1, lengths & 127, 0))
    until = ones(iota((docs, docs), 0) <= iota((docs, docs), 1))
    sums = dot(small(digits), until)
    end = (sums[0:1, :] * 128.0 + sums[1:2, :]).astype(jnp.int32)
    start = end - lengths
    line = iota((LANES, docs), 0)
    device = (line >> 5) * 32 + (line & 15) * 2 + ((line >> 4) & 1)
    touches = (start < (device + 1) * tokens) & (end > device * tokens)
    owned = ((owner >> 3) & 15) == line
    counts = dot_rows(ones(touches), ones(owned))
    return jnp.max(jnp.sum(counts.reshape(8, 16, LANES), axis=0))


def sums_kernel(
    pieces, seg_hbm, owner_hbm, length_hbm, hidden_hbm, out_ref, seg, owner, length, hidden, sems
):
    tokens = hidden.shape[0]
    rows = tokens // pieces
    copies = [
        pltpu.make_async_copy(seg_hbm, seg, sems.at[pieces]),
        pltpu.make_async_copy(owner_hbm, owner, sems.at[pieces + 1]),
        pltpu.make_async_copy(length_hbm, length, sems.at[pieces + 2]),
    ]
    for p in range(pieces):
        here = pl.ds(p * rows, rows)
        copies.append(pltpu.make_async_copy(hidden_hbm.at[here], hidden.at[here], sems.at[p]))
    for copy in copies:
        copy.start()
    copies[0].wait()
    first = seg[0:1, 0:1]
    last = seg[0:1, tokens - 1 : tokens]
    copies[1].wait()
    marks = marks_of(first, last, owner[...])
    copies[2].wait()
    over = jnp.where(most_rows(length[...], owner[...], tokens) > FIT, 1.0, 0.0)
    marks = jnp.where((iota((SLOTS, LANES), 0) == SLOTS - 1) & (iota((SLOTS, LANES), 1) == LANES - 1), over, marks)
    slot = iota((SLOTS, rows), 0) + first
    sums = None
    for p in range(pieces):
        picker = ones(slot == seg[:, p * rows : (p + 1) * rows])
        copies[3 + p].wait()
        term = dot(picker, hidden[p * rows : (p + 1) * rows, :])
        sums = term if sums is None else sums + term
    for c in range(out_ref.shape[0]):
        out_ref[c] = sums[:, c * LANES : (c + 1) * LANES] + marks


def local_sums(seg_ids, owner_slot, lengths, hidden, chunks):
    tokens, width = hidden.shape
    docs = owner_slot.shape[0]
    pieces = 4
    return pl.pallas_call(
        functools.partial(sums_kernel, pieces),
        in_specs=[pl.BlockSpec(memory_space=pltpu.HBM)] * 4,
        out_specs=pl.BlockSpec(memory_space=pltpu.VMEM),
        out_shape=pltpu.VMEM((chunks, SLOTS, LANES), jnp.float32),
        scratch_shapes=[
            pltpu.VMEM((1, tokens), jnp.int32),
            pltpu.VMEM((1, docs), jnp.int32),
            pltpu.VMEM((1, docs), jnp.int32),
            pltpu.VMEM((tokens, width), hidden.dtype),
            pltpu.SemaphoreType.DMA((pieces + 3,)),
        ],
        compiler_params=pltpu.CompilerParams(vmem_limit_bytes=WIDE),
        name="local_sums",
    )(seg_ids.reshape(1, -1), owner_slot.reshape(1, -1), lengths.reshape(1, -1), hidden)


def slots_of(in_ref):
    sources = in_ref.shape[0]
    values = in_ref[...].reshape(sources * SLOTS, LANES)
    empty = jnp.zeros((2 * LANES - sources * SLOTS, LANES), jnp.float32)
    marks = jnp.sum(in_ref[:, SLOTS - 2 : SLOTS, :], axis=0).astype(jnp.int32)
    where = jnp.concatenate([marks[0:1, :], marks[1:2, :]], axis=1)
    where = jnp.where(iota(where.shape, 1) < sources * SLOTS, where, 0)
    plane = jnp.where(where > 0, (where - 1) >> 5, -1)
    bound = iota((16, 2 * LANES), 0) == plane
    ahead = iota((2 * LANES, 2 * LANES), 0) < iota((2 * LANES, 2 * LANES), 1)
    seen = dot(ones(bound), ones(ahead))
    rank = jnp.sum(jnp.where(bound, seen, 0.0), axis=0, keepdims=True).astype(jnp.int32)
    return jnp.concatenate([values, empty], axis=0), where, plane, bound, rank


def place_kernel(in_ref, out_ref, kept_ref, over_ref):
    planes = out_ref.shape[0]
    kept_ref[...] = in_ref[...]
    over_ref[0] = jnp.max(in_ref[0, SLOTS - 1 : SLOTS, LANES - 1 : LANES]).astype(jnp.int32)
    values, where, plane, bound, rank = slots_of(in_ref)
    target = jnp.where((where > 0) & (rank < FIT), plane * ROWS + rank, -1)
    placed = picked(ones(iota((planes * ROWS, 2 * LANES), 0) == target), values)
    number = jnp.where(bound, ((where - 1) & 31) + 1, 0)
    lane = iota((2 * LANES, 2 * LANES), 0) - plane_place(lax.axis_index("z")) * ROWS
    numbers = dot_rows(small(number), ones((lane == rank) & (rank < FIT)))
    placed = placed.reshape(out_ref.shape)
    line = iota(out_ref.shape, 1)
    near = numbers[:, :LANES].reshape(planes, 1, LANES)
    far = numbers[:, LANES:].reshape(planes, 1, LANES)
    out_ref[...] = jnp.where(line == FIT, near, jnp.where(line == FIT + 1, far, placed))


def place(slots, planes):
    return pl.pallas_call(
        place_kernel,
        out_specs=[
            pl.BlockSpec(memory_space=pltpu.VMEM),
            pl.BlockSpec(memory_space=pltpu.VMEM),
            pl.BlockSpec(memory_space=pltpu.SMEM),
        ],
        out_shape=[
            pltpu.VMEM((planes, ROWS, LANES), jnp.float32),
            pltpu.VMEM(slots.shape, slots.dtype),
            jax.ShapeDtypeStruct((1,), jnp.int32),
        ],
        compiler_params=pltpu.CompilerParams(vmem_limit_bytes=GRANT),
        name="place",
    )(slots)


def place_rest_kernel(in_ref, out_ref):
    planes, per_plane, _ = out_ref.shape
    values, where, _, _, rank = slots_of(in_ref)
    row = iota((planes * per_plane, 2 * LANES), 0) + 1
    out_ref[...] = picked(ones((row == where) & (rank >= FIT)), values).reshape(out_ref.shape)


def place_rest(slots, planes, per_plane):
    return pl.pallas_call(
        place_rest_kernel,
        out_shape=jax.ShapeDtypeStruct((planes, per_plane, LANES), jnp.float32),
        compiler_params=pltpu.CompilerParams(vmem_limit_bytes=GRANT),
        name="place_rest",
    )(slots)


def average_kernel(owner_ref, length_ref, bias_ref, in_ref, *rest_and_out):
    out_ref = rest_and_out[-1]
    planes = in_ref.shape[0]
    per_plane = owner_ref.shape[1] // planes
    marks = jnp.sum(in_ref[:, FIT : FIT + 2, :], axis=0).astype(jnp.int32)
    where = jnp.concatenate([marks[0:1, :], marks[1:2, :]], axis=1)
    picker = ones(iota((per_plane, planes * ROWS), 0) + 1 == where)
    total = picked(picker, in_ref[...].reshape(planes * ROWS, LANES))
    for rest_ref in rest_and_out[:-1]:
        total = total + jnp.sum(rest_ref[...], axis=0)
    mine = plane_place(lax.axis_index("z")) * per_plane
    row = iota((per_plane, owner_ref.shape[1]), 0) + mine
    length = jnp.sum(
        jnp.where(row == plane_row(owner_ref[...]), length_ref[...], 0).astype(jnp.float32),
        axis=1,
        keepdims=True,
    )
    chunk = chunk_place()
    average = total / length + bias_ref[pl.ds(chunk, 1), :]
    owners, copies, rows, _ = out_ref.shape
    for o in range(owners):
        for y in range(copies):
            out_ref[o, y] = average[o * rows : (o + 1) * rows, :]


def averages_for_owners(arrived, owner_slot, lengths, pool_bias, owners, copies, *rest):
    rows = owner_slot.shape[0] // (arrived.shape[0] * owners)
    return pl.pallas_call(
        average_kernel,
        out_shape=jax.ShapeDtypeStruct((owners, copies, rows, LANES), jnp.float32),
        compiler_params=pltpu.CompilerParams(vmem_limit_bytes=GRANT),
        name="average",
    )(owner_slot.reshape(1, -1), lengths.reshape(1, -1), pool_bias.reshape(-1, LANES), arrived, *rest)


def norm_kernel(in_ref, out_ref):
    chunks, slices, rows, _ = in_ref.shape
    every = in_ref[...]
    square = jnp.sum(every * every, axis=(0, 1))
    energy = jnp.sum(square, axis=1, keepdims=True) / (chunks * slices * LANES)
    scale = lax.rsqrt(energy + 1e-06)
    mine = slice_place()
    for c, device in enumerate(CHUNK_GROUP[0]):
        values = in_ref[device, mine] * scale
        out_ref[:, c * LANES : (c + 1) * LANES] = values.astype(jnp.bfloat16)


def normed(arrived):
    chunks, _, rows, _ = arrived.shape
    return pl.pallas_call(
        norm_kernel,
        out_shape=jax.ShapeDtypeStruct((rows, chunks * LANES), jnp.bfloat16),
        compiler_params=pltpu.CompilerParams(vmem_limit_bytes=GRANT),
        name="norm",
    )(arrived)


def swap(array, axes, group):
    return lax.all_to_all(
        array, axes, split_axis=0, concat_axis=0, tiled=True, axis_index_groups=group
    )


def local(hidden, seg_ids, lengths, owner_slot, pool_bias):
    chunks = lax.axis_size(("x", "c"))
    planes = lax.axis_size("z")
    slices = lax.axis_size("y")
    per_plane = lengths.shape[0] // planes
    slots = swap(local_sums(seg_ids, owner_slot, lengths, hidden, chunks), ("x", "c"), CHUNK_GROUP)
    placed, kept, over = place(slots, planes)
    rows = swap(placed, "z", PLANE_GROUP)
    args = (owner_slot, lengths, pool_bias, chunks, slices)

    def with_rest(rows, kept):
        rest = swap(place_rest(kept, planes, per_plane), "z", PLANE_GROUP)
        return averages_for_owners(rows, *args, rest)

    def alone(rows, kept):
        return averages_for_owners(rows, *args)

    average = lax.cond(over[0] > 0, with_rest, alone, rows, kept)
    mine = swap(average.reshape(chunks * slices, -1, LANES), ("x", "c", "y"), OWNER_GROUP)
    return normed(mine.reshape(average.shape))


def solution(mesh):
    torus = Mesh(mesh.devices.reshape(4, 16, 2, mesh.shape["hid"]), ("x", "z", "c", "y"))
    seq = ("x", "z", "c")
    return jax.shard_map(
        local,
        mesh=torus,
        in_specs=(P(seq, "y"), P(seq), P(), P(), P("y")),
        out_specs=P(seq, "y"),
        check_vma=False,
    )
```

```python
import functools

import jax
import jax.numpy as jnp
from jax import lax
from jax.experimental import pallas as pl
from jax.experimental.pallas import tpu as pltpu
from jax.sharding import Mesh
from jax.sharding import PartitionSpec as P

USED = 17
SLOTS = 24
LANES = 128
FIT = 14
ROWS = 16
GRANT = 16 * 1024 * 1024
WIDE = 56 * 1024 * 1024


def chunk_place():
    return (((lax.axis_index("x") + 2) & 3) * 2 + lax.axis_index("c")) ^ 1


def plane_place(z):
    return (z + 4) & 15


def slice_place():
    return (lax.axis_index("y") + 2) & 3


CHUNK_GROUP = [[(((j >> 1) + 2) & 3) * 2 + (j & 1) ^ 1 for j in range(8)]]
PLANE_GROUP = [[(j + 12) & 15 for j in range(16)]]
OWNER_GROUP = [[(j & ~3) + ((j + 2) & 3) for j in range(32)]]


def plane_row(owner):
    return plane_place(owner >> 3) * 32 + (owner >> 7) * 8 + (owner & 7)


def ones(mask):
    return jnp.where(mask, 1.0, 0.0).astype(jnp.bfloat16)


def iota(shape, dim):
    return lax.broadcasted_iota(jnp.int32, shape, dim)


def small(array):
    return array.astype(jnp.float32).astype(jnp.bfloat16)


def dot(left, right):
    return jnp.dot(left, right, preferred_element_type=jnp.float32)


def dot_rows(left, right):
    return lax.dot_general(
        left, right, (((1,), (1,)), ((), ())), preferred_element_type=jnp.float32
    )


def picked(picker, values):
    high = values.astype(jnp.bfloat16)
    left_over = values - high.astype(jnp.float32)
    middle = left_over.astype(jnp.bfloat16)
    low = (left_over - middle.astype(jnp.float32)).astype(jnp.bfloat16)
    parts = dot(picker, jnp.concatenate([high, middle, low], axis=1))
    return parts[:, :LANES] + (parts[:, LANES : 2 * LANES] + parts[:, 2 * LANES :])


def marks_of(first, last, owner):
    docs = owner.shape[1]
    source = chunk_place()
    row = plane_row(owner) + 1
    part = iota((8, docs), 0)
    digits = jnp.where(part == 0, row >> 5, jnp.where(part == 1, row & 31, 0))
    lane = iota((docs, 2 * LANES), 1) - source * SLOTS
    doc = iota((docs, 2 * LANES), 0)
    meets = (doc == first + lane) & (doc <= last) & (lane >= 0) & (lane < USED)
    found = dot(small(digits), ones(meets))
    where = found[0:1, :] * 32.0 + found[1:2, :]
    line = iota((SLOTS, LANES), 0)
    second = jnp.where(line == SLOTS - 1, where[:, LANES:], 0.0)
    return jnp.where(line == SLOTS - 2, where[:, :LANES], second)


def most_rows(lengths, owner, tokens):
    docs = owner.shape[1]
    part = iota((8, docs), 0)
    digits = jnp.where(part == 0, lengths >> 7, jnp.where(part == 1, lengths & 127, 0))
    until = ones(iota((docs, docs), 0) <= iota((docs, docs), 1))
    sums = dot(small(digits), until)
    end = (sums[0:1, :] * 128.0 + sums[1:2, :]).astype(jnp.int32)
    start = end - lengths
    line = iota((LANES, docs), 0)
    device = (line >> 5) * 32 + (line & 15) * 2 + ((line >> 4) & 1)
    touches = (start < (device + 1) * tokens) & (end > device * tokens)
    owned = ((owner >> 3) & 15) == line
    counts = dot_rows(ones(touches), ones(owned))
    return jnp.max(jnp.sum(counts.reshape(8, 16, LANES), axis=0))


def sums_kernel(
    pieces, seg_hbm, owner_hbm, length_hbm, hidden_hbm, out_ref, seg, owner, length, hidden, sems
):
    tokens = hidden.shape[0]
    rows = tokens // pieces
    copies = [
        pltpu.make_async_copy(seg_hbm, seg, sems.at[pieces]),
        pltpu.make_async_copy(owner_hbm, owner, sems.at[pieces + 1]),
        pltpu.make_async_copy(length_hbm, length, sems.at[pieces + 2]),
    ]
    for p in range(pieces):
        here = pl.ds(p * rows, rows)
        copies.append(pltpu.make_async_copy(hidden_hbm.at[here], hidden.at[here], sems.at[p]))
    for copy in copies:
        copy.start()
    copies[0].wait()
    first = seg[0:1, 0:1]
    last = seg[0:1, tokens - 1 : tokens]
    copies[1].wait()
    marks = marks_of(first, last, owner[...])
    copies[2].wait()
    over = jnp.where(most_rows(length[...], owner[...], tokens) > FIT, 1.0, 0.0)
    marks = jnp.where((iota((SLOTS, LANES), 0) == SLOTS - 1) & (iota((SLOTS, LANES), 1) == LANES - 1), over, marks)
    slot = iota((SLOTS, rows), 0) + first
    sums = None
    for p in range(pieces):
        picker = ones(slot == seg[:, p * rows : (p + 1) * rows])
        copies[3 + p].wait()
        term = dot(picker, hidden[p * rows : (p + 1) * rows, :])
        sums = term if sums is None else sums + term
    for c in range(out_ref.shape[0]):
        out_ref[c] = sums[:, c * LANES : (c + 1) * LANES] + marks


def local_sums(seg_ids, owner_slot, lengths, hidden, chunks):
    tokens, width = hidden.shape
    docs = owner_slot.shape[0]
    pieces = 4
    return pl.pallas_call(
        functools.partial(sums_kernel, pieces),
        in_specs=[pl.BlockSpec(memory_space=pltpu.HBM)] * 4,
        out_specs=pl.BlockSpec(memory_space=pltpu.VMEM),
        out_shape=pltpu.VMEM((chunks, SLOTS, LANES), jnp.float32),
        scratch_shapes=[
            pltpu.VMEM((1, tokens), jnp.int32),
            pltpu.VMEM((1, docs), jnp.int32),
            pltpu.VMEM((1, docs), jnp.int32),
            pltpu.VMEM((tokens, width), hidden.dtype),
            pltpu.SemaphoreType.DMA((pieces + 3,)),
        ],
        compiler_params=pltpu.CompilerParams(vmem_limit_bytes=WIDE),
        name="local_sums",
    )(seg_ids.reshape(1, -1), owner_slot.reshape(1, -1), lengths.reshape(1, -1), hidden)


def slots_of(in_ref):
    sources = in_ref.shape[0]
    values = in_ref[...].reshape(sources * SLOTS, LANES)
    empty = jnp.zeros((2 * LANES - sources * SLOTS, LANES), jnp.float32)
    marks = jnp.sum(in_ref[:, SLOTS - 2 : SLOTS, :], axis=0).astype(jnp.int32)
    where = jnp.concatenate([marks[0:1, :], marks[1:2, :]], axis=1)
    where = jnp.where(iota(where.shape, 1) < sources * SLOTS, where, 0)
    plane = jnp.where(where > 0, (where - 1) >> 5, -1)
    bound = iota((16, 2 * LANES), 0) == plane
    ahead = iota((2 * LANES, 2 * LANES), 0) < iota((2 * LANES, 2 * LANES), 1)
    seen = dot(ones(bound), ones(ahead))
    rank = jnp.sum(jnp.where(bound, seen, 0.0), axis=0, keepdims=True).astype(jnp.int32)
    return jnp.concatenate([values, empty], axis=0), where, plane, bound, rank


def place_kernel(in_ref, out_ref, kept_ref, over_ref):
    planes = out_ref.shape[0]
    kept_ref[...] = in_ref[...]
    over_ref[0] = jnp.max(in_ref[0, SLOTS - 1 : SLOTS, LANES - 1 : LANES]).astype(jnp.int32)
    values, where, plane, bound, rank = slots_of(in_ref)
    target = jnp.where((where > 0) & (rank < FIT), plane * ROWS + rank, -1)
    placed = picked(ones(iota((planes * ROWS, 2 * LANES), 0) == target), values)
    number = jnp.where(bound, ((where - 1) & 31) + 1, 0)
    lane = iota((2 * LANES, 2 * LANES), 0) - plane_place(lax.axis_index("z")) * ROWS
    numbers = dot_rows(small(number), ones((lane == rank) & (rank < FIT)))
    placed = placed.reshape(out_ref.shape)
    line = iota(out_ref.shape, 1)
    near = numbers[:, :LANES].reshape(planes, 1, LANES)
    far = numbers[:, LANES:].reshape(planes, 1, LANES)
    out_ref[...] = jnp.where(line == FIT, near, jnp.where(line == FIT + 1, far, placed))


def place(slots, planes):
    return pl.pallas_call(
        place_kernel,
        out_specs=[
            pl.BlockSpec(memory_space=pltpu.VMEM),
            pl.BlockSpec(memory_space=pltpu.VMEM),
            pl.BlockSpec(memory_space=pltpu.SMEM),
        ],
        out_shape=[
            pltpu.VMEM((planes, ROWS, LANES), jnp.float32),
            pltpu.VMEM(slots.shape, slots.dtype),
            jax.ShapeDtypeStruct((1,), jnp.int32),
        ],
        compiler_params=pltpu.CompilerParams(vmem_limit_bytes=GRANT),
        name="place",
    )(slots)


def place_rest_kernel(in_ref, out_ref):
    planes, per_plane, _ = out_ref.shape
    values, where, _, _, rank = slots_of(in_ref)
    row = iota((planes * per_plane, 2 * LANES), 0) + 1
    out_ref[...] = picked(ones((row == where) & (rank >= FIT)), values).reshape(out_ref.shape)


def place_rest(slots, planes, per_plane):
    return pl.pallas_call(
        place_rest_kernel,
        out_shape=jax.ShapeDtypeStruct((planes, per_plane, LANES), jnp.float32),
        compiler_params=pltpu.CompilerParams(vmem_limit_bytes=GRANT),
        name="place_rest",
    )(slots)


def average_kernel(owner_ref, length_ref, bias_ref, in_ref, *rest_and_out):
    out_ref = rest_and_out[-1]
    planes = in_ref.shape[0]
    per_plane = owner_ref.shape[1] // planes
    marks = jnp.sum(in_ref[:, FIT : FIT + 2, :], axis=0).astype(jnp.int32)
    where = jnp.concatenate([marks[0:1, :], marks[1:2, :]], axis=1)
    picker = ones(iota((per_plane, planes * ROWS), 0) + 1 == where)
    total = picked(picker, in_ref[...].reshape(planes * ROWS, LANES))
    for rest_ref in rest_and_out[:-1]:
        total = total + jnp.sum(rest_ref[...], axis=0)
    mine = plane_place(lax.axis_index("z")) * per_plane
    row = iota((per_plane, owner_ref.shape[1]), 0) + mine
    length = jnp.sum(
        jnp.where(row == plane_row(owner_ref[...]), length_ref[...], 0).astype(jnp.float32),
        axis=1,
        keepdims=True,
    )
    chunk = chunk_place()
    average = total / length + bias_ref[pl.ds(chunk, 1), :]
    owners, copies, rows, _ = out_ref.shape
    for o in range(owners):
        for y in range(copies):
            out_ref[o, y] = average[o * rows : (o + 1) * rows, :]


def averages_for_owners(arrived, owner_slot, lengths, pool_bias, owners, copies, *rest):
    rows = owner_slot.shape[0] // (arrived.shape[0] * owners)
    return pl.pallas_call(
        average_kernel,
        out_shape=jax.ShapeDtypeStruct((owners, copies, rows, LANES), jnp.float32),
        compiler_params=pltpu.CompilerParams(vmem_limit_bytes=GRANT),
        name="average",
    )(owner_slot.reshape(1, -1), lengths.reshape(1, -1), pool_bias.reshape(-1, LANES), arrived, *rest)


def norm_kernel(in_ref, out_ref):
    chunks, slices, rows, _ = in_ref.shape
    every = in_ref[...]
    square = jnp.sum(every * every, axis=(0, 1))
    energy = jnp.sum(square, axis=1, keepdims=True) / (chunks * slices * LANES)
    scale = lax.rsqrt(energy + 1e-06)
    mine = slice_place()
    for c, device in enumerate(CHUNK_GROUP[0]):
        values = in_ref[device, mine] * scale
        out_ref[:, c * LANES : (c + 1) * LANES] = values.astype(jnp.bfloat16)


def normed(arrived):
    chunks, _, rows, _ = arrived.shape
    return pl.pallas_call(
        norm_kernel,
        out_shape=jax.ShapeDtypeStruct((rows, chunks * LANES), jnp.bfloat16),
        compiler_params=pltpu.CompilerParams(vmem_limit_bytes=GRANT),
        name="norm",
    )(arrived)


def swap(array, axes, group):
    return lax.all_to_all(
        array, axes, split_axis=0, concat_axis=0, tiled=True, axis_index_groups=group
    )


def local(hidden, seg_ids, lengths, owner_slot, pool_bias):
    chunks = lax.axis_size(("x", "c"))
    planes = lax.axis_size("z")
    slices = lax.axis_size("y")
    per_plane = lengths.shape[0] // planes
    slots = swap(local_sums(seg_ids, owner_slot, lengths, hidden, chunks), ("x", "c"), CHUNK_GROUP)
    placed, kept, over = place(slots, planes)
    rows = swap(placed, "z", PLANE_GROUP)
    args = (owner_slot, lengths, pool_bias, chunks, slices)

    def with_rest(rows, kept):
        rest = swap(place_rest(kept, planes, per_plane), "z", PLANE_GROUP)
        return averages_for_owners(rows, *args, rest)

    def alone(rows, kept):
        return averages_for_owners(rows, *args)

    average = lax.cond(over[0] > 0, with_rest, alone, rows, kept)
    mine = swap(average.reshape(chunks * slices, -1, LANES), ("x", "c", "y"), OWNER_GROUP)
    return normed(mine.reshape(average.shape))


def solution(mesh):
    torus = Mesh(mesh.devices.reshape(4, 16, 2, mesh.shape["hid"]), ("x", "z", "c", "y"))
    seq = ("x", "z", "c")
    return jax.shard_map(
        local,
        mesh=torus,
        in_specs=(P(seq, "y"), P(seq), P(), P(), P("y")),
        out_specs=P(seq, "y"),
        check_vma=False,
    )
```

```python
import functools

import jax
import jax.numpy as jnp
from jax import lax
from jax.experimental import pallas as pl
from jax.experimental.pallas import tpu as pltpu
from jax.sharding import Mesh
from jax.sharding import PartitionSpec as P

USED = 17
SLOTS = 24
LANES = 128
FIT = 14
ROWS = 16
GRANT = 16 * 1024 * 1024
WIDE = 56 * 1024 * 1024


def chunk_place():
    return (((lax.axis_index("x") + 2) & 3) * 2 + lax.axis_index("c")) ^ 1


def plane_place(z):
    return (z + 8) & 15


def slice_place():
    return (lax.axis_index("y") + 2) & 3


CHUNK_GROUP = [[(((j >> 1) + 2) & 3) * 2 + (j & 1) ^ 1 for j in range(8)]]
PLANE_GROUP = [[(j + 8) & 15 for j in range(16)]]
OWNER_GROUP = [[(j & ~3) + ((j + 2) & 3) for j in range(32)]]


def plane_row(owner):
    return plane_place(owner >> 3) * 32 + (owner >> 7) * 8 + (owner & 7)


def ones(mask):
    return jnp.where(mask, 1.0, 0.0).astype(jnp.bfloat16)


def iota(shape, dim):
    return lax.broadcasted_iota(jnp.int32, shape, dim)


def small(array):
    return array.astype(jnp.float32).astype(jnp.bfloat16)


def dot(left, right):
    return jnp.dot(left, right, preferred_element_type=jnp.float32)


def dot_rows(left, right):
    return lax.dot_general(
        left, right, (((1,), (1,)), ((), ())), preferred_element_type=jnp.float32
    )


def picked(picker, values):
    high = values.astype(jnp.bfloat16)
    left_over = values - high.astype(jnp.float32)
    middle = left_over.astype(jnp.bfloat16)
    low = (left_over - middle.astype(jnp.float32)).astype(jnp.bfloat16)
    parts = dot(picker, jnp.concatenate([high, middle, low], axis=1))
    return parts[:, :LANES] + (parts[:, LANES : 2 * LANES] + parts[:, 2 * LANES :])


def marks_of(first, last, owner):
    docs = owner.shape[1]
    source = chunk_place()
    row = plane_row(owner) + 1
    part = iota((8, docs), 0)
    digits = jnp.where(part == 0, row >> 5, jnp.where(part == 1, row & 31, 0))
    lane = iota((docs, 2 * LANES), 1) - source * SLOTS
    doc = iota((docs, 2 * LANES), 0)
    meets = (doc == first + lane) & (doc <= last) & (lane >= 0) & (lane < USED)
    found = dot(small(digits), ones(meets))
    where = found[0:1, :] * 32.0 + found[1:2, :]
    line = iota((SLOTS, LANES), 0)
    second = jnp.where(line == SLOTS - 1, where[:, LANES:], 0.0)
    return jnp.where(line == SLOTS - 2, where[:, :LANES], second)


def most_rows(lengths, owner, tokens):
    docs = owner.shape[1]
    part = iota((8, docs), 0)
    digits = jnp.where(part == 0, lengths >> 7, jnp.where(part == 1, lengths & 127, 0))
    until = ones(iota((docs, docs), 0) <= iota((docs, docs), 1))
    sums = dot(small(digits), until)
    end = (sums[0:1, :] * 128.0 + sums[1:2, :]).astype(jnp.int32)
    start = end - lengths
    line = iota((LANES, docs), 0)
    device = (line >> 5) * 32 + (line & 15) * 2 + ((line >> 4) & 1)
    touches = (start < (device + 1) * tokens) & (end > device * tokens)
    owned = ((owner >> 3) & 15) == line
    counts = dot_rows(ones(touches), ones(owned))
    return jnp.max(jnp.sum(counts.reshape(8, 16, LANES), axis=0)).astype(jnp.int32)


def sums_kernel(
    pieces, seg_hbm, owner_hbm, hidden_hbm, out_ref, seg, owner, hidden, sems
):
    tokens = hidden.shape[0]
    rows = tokens // pieces
    copies = [
        pltpu.make_async_copy(seg_hbm, seg, sems.at[pieces]),
        pltpu.make_async_copy(owner_hbm, owner, sems.at[pieces + 1]),
    ]
    for p in range(pieces):
        here = pl.ds(p * rows, rows)
        copies.append(pltpu.make_async_copy(hidden_hbm.at[here], hidden.at[here], sems.at[p]))
    for copy in copies:
        copy.start()
    copies[0].wait()
    first = seg[0:1, 0:1]
    last = seg[0:1, tokens - 1 : tokens]
    copies[1].wait()
    marks = marks_of(first, last, owner[...])
    slot = iota((SLOTS, rows), 0) + first
    sums = None
    for p in range(pieces):
        picker = ones(slot == seg[:, p * rows : (p + 1) * rows])
        copies[2 + p].wait()
        term = dot(picker, hidden[p * rows : (p + 1) * rows, :])
        sums = term if sums is None else sums + term
    for c in range(out_ref.shape[0]):
        out_ref[c] = sums[:, c * LANES : (c + 1) * LANES] + marks


def local_sums(seg_ids, owner_slot, hidden, chunks):
    tokens, width = hidden.shape
    docs = owner_slot.shape[0]
    pieces = 4
    return pl.pallas_call(
        functools.partial(sums_kernel, pieces),
        in_specs=[pl.BlockSpec(memory_space=pltpu.HBM)] * 3,
        out_specs=pl.BlockSpec(memory_space=pltpu.VMEM),
        out_shape=pltpu.VMEM((chunks, SLOTS, LANES), jnp.float32),
        scratch_shapes=[
            pltpu.VMEM((1, tokens), jnp.int32),
            pltpu.VMEM((1, docs), jnp.int32),
            pltpu.VMEM((tokens, width), hidden.dtype),
            pltpu.SemaphoreType.DMA((pieces + 2,)),
        ],
        compiler_params=pltpu.CompilerParams(vmem_limit_bytes=WIDE),
        name="local_sums",
    )(seg_ids.reshape(1, -1), owner_slot.reshape(1, -1), hidden)


def slots_of(in_ref):
    sources = in_ref.shape[0]
    values = in_ref[...].reshape(sources * SLOTS, LANES)
    empty = jnp.zeros((2 * LANES - sources * SLOTS, LANES), jnp.float32)
    marks = jnp.sum(in_ref[:, SLOTS - 2 : SLOTS, :], axis=0).astype(jnp.int32)
    where = jnp.concatenate([marks[0:1, :], marks[1:2, :]], axis=1)
    plane = jnp.where(where > 0, (where - 1) >> 5, -1)
    bound = iota((16, 2 * LANES), 0) == plane
    ahead = iota((2 * LANES, 2 * LANES), 0) < iota((2 * LANES, 2 * LANES), 1)
    seen = dot(ones(bound), ones(ahead))
    rank = jnp.sum(jnp.where(bound, seen, 0.0), axis=0, keepdims=True).astype(jnp.int32)
    return jnp.concatenate([values, empty], axis=0), where, plane, bound, rank


def place_kernel(in_ref, out_ref, ready_ref):
    planes = out_ref.shape[0]
    ready_ref[...] = jnp.zeros_like(ready_ref)
    values, where, plane, bound, rank = slots_of(in_ref)
    target = jnp.where((where > 0) & (rank < FIT), plane * ROWS + rank, -1)
    placed = picked(ones(iota((planes * ROWS, 2 * LANES), 0) == target), values)
    number = jnp.where(bound, ((where - 1) & 31) + 1, 0)
    lane = iota((2 * LANES, 2 * LANES), 0) - plane_place(lax.axis_index("z")) * ROWS
    numbers = dot_rows(small(number), ones((lane == rank) & (rank < FIT)))
    placed = placed.reshape(out_ref.shape)
    line = iota(out_ref.shape, 1)
    near = numbers[:, :LANES].reshape(planes, 1, LANES)
    far = numbers[:, LANES:].reshape(planes, 1, LANES)
    out_ref[...] = jnp.where(line == FIT, near, jnp.where(line == FIT + 1, far, placed))


def place(slots, planes):
    return pl.pallas_call(
        place_kernel,
        out_specs=[
            pl.BlockSpec(memory_space=pltpu.VMEM),
            pl.BlockSpec(memory_space=pltpu.VMEM),
        ],
        out_shape=[
            pltpu.VMEM((planes, ROWS, LANES), jnp.float32),
            pltpu.VMEM((8, LANES), jnp.int32),
        ],
        compiler_params=pltpu.CompilerParams(vmem_limit_bytes=GRANT),
        name="place",
    )(slots)


def crowded_kernel(tokens, ready_ref, owner_ref, length_ref, over_ref):
    most = most_rows(length_ref[...], owner_ref[...], tokens)
    over_ref[0] = (most + jnp.max(ready_ref[...]) > FIT).astype(jnp.int32)


def crowded(ready, owner_slot, lengths, tokens):
    docs = owner_slot.shape[0]
    return pl.pallas_call(
        functools.partial(crowded_kernel, tokens),
        out_specs=pl.BlockSpec(memory_space=pltpu.SMEM),
        out_shape=jax.ShapeDtypeStruct((1,), jnp.int32),
        cost_estimate=pl.CostEstimate(
            flops=64 * docs * docs, bytes_accessed=8 * docs, transcendentals=0
        ),
        compiler_params=pltpu.CompilerParams(vmem_limit_bytes=GRANT),
        name="crowded",
    )(ready, owner_slot.reshape(1, -1), lengths.reshape(1, -1))


def place_rest_kernel(in_ref, out_ref):
    planes, per_plane, _ = out_ref.shape
    values, where, _, _, rank = slots_of(in_ref)
    row = iota((planes * per_plane, 2 * LANES), 0) + 1
    out_ref[...] = picked(ones((row == where) & (rank >= FIT)), values).reshape(out_ref.shape)


def place_rest(slots, planes, per_plane):
    return pl.pallas_call(
        place_rest_kernel,
        out_shape=jax.ShapeDtypeStruct((planes, per_plane, LANES), jnp.float32),
        compiler_params=pltpu.CompilerParams(vmem_limit_bytes=GRANT),
        name="place_rest",
    )(slots)


def average_kernel(owner_ref, length_ref, bias_ref, in_ref, *rest_and_out):
    out_ref = rest_and_out[-1]
    planes = in_ref.shape[0]
    per_plane = owner_ref.shape[1] // planes
    marks = jnp.sum(in_ref[:, FIT : FIT + 2, :], axis=0).astype(jnp.int32)
    where = jnp.concatenate([marks[0:1, :], marks[1:2, :]], axis=1)
    picker = ones(iota((per_plane, planes * ROWS), 0) + 1 == where)
    total = picked(picker, in_ref[...].reshape(planes * ROWS, LANES))
    for rest_ref in rest_and_out[:-1]:
        total = total + jnp.sum(rest_ref[...], axis=0)
    mine = plane_place(lax.axis_index("z")) * per_plane
    row = iota((per_plane, owner_ref.shape[1]), 0) + mine
    length = jnp.sum(
        jnp.where(row == plane_row(owner_ref[...]), length_ref[...], 0).astype(jnp.float32),
        axis=1,
        keepdims=True,
    )
    chunk = chunk_place()
    average = total / length + bias_ref[pl.ds(chunk, 1), :]
    owners, copies, rows, _ = out_ref.shape
    for o in range(owners):
        for y in range(copies):
            out_ref[o, y] = average[o * rows : (o + 1) * rows, :]


def averages_for_owners(arrived, owner_slot, lengths, pool_bias, owners, copies, *rest):
    rows = owner_slot.shape[0] // (arrived.shape[0] * owners)
    return pl.pallas_call(
        average_kernel,
        out_shape=jax.ShapeDtypeStruct((owners, copies, rows, LANES), jnp.float32),
        compiler_params=pltpu.CompilerParams(vmem_limit_bytes=GRANT),
        name="average",
    )(owner_slot.reshape(1, -1), lengths.reshape(1, -1), pool_bias.reshape(-1, LANES), arrived, *rest)


def norm_kernel(in_ref, out_ref):
    chunks, slices, rows, _ = in_ref.shape
    every = in_ref[...]
    square = jnp.sum(every * every, axis=(0, 1))
    energy = jnp.sum(square, axis=1, keepdims=True) / (chunks * slices * LANES)
    scale = lax.rsqrt(energy + 1e-06)
    mine = slice_place()
    for c, device in enumerate(CHUNK_GROUP[0]):
        values = in_ref[device, mine] * scale
        out_ref[:, c * LANES : (c + 1) * LANES] = values.astype(jnp.bfloat16)


def normed(arrived):
    chunks, _, rows, _ = arrived.shape
    return pl.pallas_call(
        norm_kernel,
        out_shape=jax.ShapeDtypeStruct((rows, chunks * LANES), jnp.bfloat16),
        compiler_params=pltpu.CompilerParams(vmem_limit_bytes=GRANT),
        name="norm",
    )(arrived)


def swap(array, axes, group):
    return lax.all_to_all(
        array, axes, split_axis=0, concat_axis=0, tiled=True, axis_index_groups=group
    )


def local(hidden, seg_ids, lengths, owner_slot, pool_bias):
    chunks = lax.axis_size(("x", "c"))
    planes = lax.axis_size("z")
    slices = lax.axis_size("y")
    per_plane = lengths.shape[0] // planes
    slots = swap(local_sums(seg_ids, owner_slot, hidden, chunks), ("x", "c"), CHUNK_GROUP)
    placed, ready = place(slots, planes)
    over = crowded(ready, owner_slot, lengths, hidden.shape[0])
    rows = swap(placed, "z", PLANE_GROUP)
    args = (owner_slot, lengths, pool_bias, chunks, slices)

    def with_rest(rows, kept):
        rest = swap(place_rest(kept, planes, per_plane), "z", PLANE_GROUP)
        return averages_for_owners(rows, *args, rest)

    def alone(rows, kept):
        return averages_for_owners(rows, *args)

    average = lax.cond(over[0] > 0, with_rest, alone, rows, slots)
    mine = swap(average.reshape(chunks * slices, -1, LANES), ("x", "c", "y"), OWNER_GROUP)
    return normed(mine.reshape(average.shape))


def solution(mesh):
    torus = Mesh(mesh.devices.reshape(4, 16, 2, mesh.shape["hid"]), ("x", "z", "c", "y"))
    seq = ("x", "z", "c")
    return jax.shard_map(
        local,
        mesh=torus,
        in_specs=(P(seq, "y"), P(seq), P(), P(), P("y")),
        out_specs=P(seq, "y"),
        check_vma=False,
    )
```

```python
import functools

import jax
import jax.numpy as jnp
from jax import lax
from jax.experimental import pallas as pl
from jax.experimental.pallas import tpu as pltpu
from jax.sharding import Mesh
from jax.sharding import PartitionSpec as P

USED = 17
SLOTS = 24
LANES = 128
FIT = 11
ROWS = 12
PAIRS = 8
GRANT = 16 * 1024 * 1024
WIDE = 56 * 1024 * 1024


def chunk_place():
    return (((lax.axis_index("x") + 2) & 3) * 2 + lax.axis_index("c")) ^ 1


def plane_place(z):
    return (z + 6) & 15


def slice_place():
    return (lax.axis_index("y") + 2) & 3


CHUNK_GROUP = [[(((j >> 1) + 2) & 3) * 2 + (j & 1) ^ 1 for j in range(8)]]
PLANE_GROUP = [[(j + 10) & 15 for j in range(16)]]
OWNER_GROUP = [[((j & ~3) ^ 4) + ((j + 2) & 3) for j in range(32)]]


def plane_row(owner):
    return plane_place(owner >> 3) * 32 + (owner >> 7) * 8 + (owner & 7)


def ones(mask):
    return jnp.where(mask, 1.0, 0.0).astype(jnp.bfloat16)


def iota(shape, dim):
    return lax.broadcasted_iota(jnp.int32, shape, dim)


def small(array):
    return array.astype(jnp.float32).astype(jnp.bfloat16)


def dot(left, right):
    return jnp.dot(left, right, preferred_element_type=jnp.float32)


def dot_rows(left, right):
    return lax.dot_general(
        left, right, (((1,), (1,)), ((), ())), preferred_element_type=jnp.float32
    )


def picked(picker, values):
    high = values.astype(jnp.bfloat16)
    left_over = values - high.astype(jnp.float32)
    middle = left_over.astype(jnp.bfloat16)
    low = (left_over - middle.astype(jnp.float32)).astype(jnp.bfloat16)
    parts = dot(picker, jnp.concatenate([high, middle, low], axis=1))
    return parts[:, :LANES] + (parts[:, LANES : 2 * LANES] + parts[:, 2 * LANES :])


def marks_of(first, last, owner):
    docs = owner.shape[1]
    source = chunk_place()
    row = plane_row(owner) + 1
    part = iota((8, docs), 0)
    digits = jnp.where(part == 0, row >> 5, jnp.where(part == 1, row & 31, 0))
    lane = iota((docs, 2 * LANES), 1) - source * SLOTS
    doc = iota((docs, 2 * LANES), 0)
    meets = (doc == first + lane) & (doc <= last) & (lane >= 0) & (lane < USED)
    found = dot(small(digits), ones(meets))
    where = found[0:1, :] * 32.0 + found[1:2, :]
    line = iota((SLOTS, LANES), 0)
    second = jnp.where(line == SLOTS - 1, where[:, LANES:], 0.0)
    return jnp.where(line == SLOTS - 2, where[:, :LANES], second)


def most_rows(lengths, owner, tokens):
    docs = owner.shape[1]
    part = iota((8, docs), 0)
    digits = jnp.where(part == 0, lengths >> 7, jnp.where(part == 1, lengths & 127, 0))
    until = ones(iota((docs, docs), 0) <= iota((docs, docs), 1))
    sums = dot(small(digits), until)
    end = (sums[0:1, :] * 128.0 + sums[1:2, :]).astype(jnp.int32)
    start = end - lengths
    line = iota((LANES, docs), 0)
    device = (line >> 5) * 32 + (line & 15) * 2 + ((line >> 4) & 1)
    touches = (start < (device + 1) * tokens) & (end > device * tokens)
    owned = ((owner >> 3) & 15) == line
    counts = dot_rows(ones(touches), ones(owned))
    return jnp.max(jnp.sum(counts.reshape(8, 16, LANES), axis=0)).astype(jnp.int32)


def sums_kernel(
    pieces, seg_hbm, owner_hbm, hidden_hbm, out_ref, seg, owner, hidden, sems
):
    tokens = hidden.shape[0]
    rows = tokens // pieces
    copies = [
        pltpu.make_async_copy(seg_hbm, seg, sems.at[pieces]),
        pltpu.make_async_copy(owner_hbm, owner, sems.at[pieces + 1]),
    ]
    for p in range(pieces):
        here = pl.ds(p * rows, rows)
        copies.append(pltpu.make_async_copy(hidden_hbm.at[here], hidden.at[here], sems.at[p]))
    for copy in copies:
        copy.start()
    copies[0].wait()
    first = seg[0:1, 0:1]
    last = seg[0:1, tokens - 1 : tokens]
    copies[1].wait()
    marks = marks_of(first, last, owner[...])
    slot = iota((SLOTS, rows), 0) + first
    sums = None
    for p in range(pieces):
        picker = ones(slot == seg[:, p * rows : (p + 1) * rows])
        copies[2 + p].wait()
        term = dot(picker, hidden[p * rows : (p + 1) * rows, :])
        sums = term if sums is None else sums + term
    for c in range(out_ref.shape[0]):
        out_ref[c] = sums[:, c * LANES : (c + 1) * LANES] + marks


def local_sums(seg_ids, owner_slot, hidden, chunks):
    tokens, width = hidden.shape
    docs = owner_slot.shape[0]
    pieces = 4
    return pl.pallas_call(
        functools.partial(sums_kernel, pieces),
        in_specs=[pl.BlockSpec(memory_space=pltpu.HBM)] * 3,
        out_specs=pl.BlockSpec(memory_space=pltpu.VMEM),
        out_shape=pltpu.VMEM((chunks, SLOTS, LANES), jnp.float32),
        scratch_shapes=[
            pltpu.VMEM((1, tokens), jnp.int32),
            pltpu.VMEM((1, docs), jnp.int32),
            pltpu.VMEM((tokens, width), hidden.dtype),
            pltpu.SemaphoreType.DMA((pieces + 2,)),
        ],
        compiler_params=pltpu.CompilerParams(vmem_limit_bytes=WIDE),
        name="local_sums",
    )(seg_ids.reshape(1, -1), owner_slot.reshape(1, -1), hidden)


def slots_of(in_ref):
    sources = in_ref.shape[0]
    values = in_ref[...].reshape(sources * SLOTS, LANES)
    empty = jnp.zeros((2 * LANES - sources * SLOTS, LANES), jnp.float32)
    marks = jnp.sum(in_ref[:, SLOTS - 2 : SLOTS, :], axis=0).astype(jnp.int32)
    where = jnp.concatenate([marks[0:1, :], marks[1:2, :]], axis=1)
    plane = jnp.where(where > 0, (where - 1) >> 5, -1)
    bound = iota((16, 2 * LANES), 0) == plane
    ahead = iota((2 * LANES, 2 * LANES), 0) < iota((2 * LANES, 2 * LANES), 1)
    seen = dot(ones(bound), ones(ahead))
    rank = jnp.sum(jnp.where(bound, seen, 0.0), axis=0, keepdims=True).astype(jnp.int32)
    return jnp.concatenate([values, empty], axis=0), where, plane, bound, rank


def place_kernel(in_ref, out_ref, ready_ref):
    planes = out_ref.shape[0] // ROWS
    ready_ref[...] = jnp.zeros_like(ready_ref)
    values, where, plane, bound, rank = slots_of(in_ref)
    target = jnp.where((where > 0) & (rank < FIT), plane * ROWS + rank, -1)
    out_ref[...] = picked(ones(iota((planes * ROWS, 2 * LANES), 0) == target), values)
    number = (((where - 1) & 31) + 1) * jnp.where((rank & 1) == 1, 64, 1)
    lane = iota((LANES, 2 * LANES), 0) - plane_place(lax.axis_index("z")) * PAIRS
    numbers = dot_rows(small(jnp.where(bound, number, 0)), ones((lane == rank >> 1) & (rank < FIT)))
    for p in range(planes):
        out_ref[p * ROWS + FIT : (p + 1) * ROWS, :] = numbers[p : p + 1, :]


def place(slots, planes):
    return pl.pallas_call(
        place_kernel,
        out_specs=[
            pl.BlockSpec(memory_space=pltpu.VMEM),
            pl.BlockSpec(memory_space=pltpu.VMEM),
        ],
        out_shape=[
            pltpu.VMEM((planes * ROWS, LANES), jnp.float32),
            pltpu.VMEM((8, LANES), jnp.int32),
        ],
        compiler_params=pltpu.CompilerParams(vmem_limit_bytes=GRANT),
        name="place",
    )(slots)


def crowded_kernel(tokens, ready_ref, owner_ref, length_ref, over_ref):
    most = most_rows(length_ref[...], owner_ref[...], tokens)
    over_ref[0] = (most + jnp.max(ready_ref[...]) > FIT).astype(jnp.int32)


def crowded(ready, owner_slot, lengths, tokens):
    docs = owner_slot.shape[0]
    return pl.pallas_call(
        functools.partial(crowded_kernel, tokens),
        out_specs=pl.BlockSpec(memory_space=pltpu.SMEM),
        out_shape=jax.ShapeDtypeStruct((1,), jnp.int32),
        cost_estimate=pl.CostEstimate(
            flops=64 * docs * docs, bytes_accessed=8 * docs, transcendentals=0
        ),
        compiler_params=pltpu.CompilerParams(vmem_limit_bytes=GRANT),
        name="crowded",
    )(ready, owner_slot.reshape(1, -1), lengths.reshape(1, -1))


def place_rest_kernel(in_ref, out_ref):
    planes, per_plane, _ = out_ref.shape
    values, where, _, _, rank = slots_of(in_ref)
    row = iota((planes * per_plane, 2 * LANES), 0) + 1
    out_ref[...] = picked(ones((row == where) & (rank >= FIT)), values).reshape(out_ref.shape)


def place_rest(slots, planes, per_plane):
    return pl.pallas_call(
        place_rest_kernel,
        out_shape=jax.ShapeDtypeStruct((planes, per_plane, LANES), jnp.float32),
        compiler_params=pltpu.CompilerParams(vmem_limit_bytes=GRANT),
        name="place_rest",
    )(slots)


def average_kernel(owner_ref, length_ref, bias_ref, in_ref, *rest_and_out):
    out_ref = rest_and_out[-1]
    count = in_ref.shape[0]
    planes = count // ROWS
    per_plane = owner_ref.shape[1] // planes
    marks = in_ref[FIT:ROWS, :]
    for p in range(1, planes):
        marks = marks + in_ref[p * ROWS + FIT : (p + 1) * ROWS, :]
    marks = marks.astype(jnp.int32)
    part = iota((8, LANES), 0)
    halves = jnp.where(part == 0, marks & 63, jnp.where(part == 1, marks >> 6, 0))
    line = iota((LANES, count), 1)
    source = (line * 171) >> 11
    spread = dot(small(halves), ones(iota((LANES, count), 0) == source * PAIRS + ((line - source * ROWS) >> 1)))
    line = line[0:1, :]
    line = line - ((line * 171) >> 11) * ROWS
    where = jnp.where((line & 1) == 1, spread[1:2, :], spread[0:1, :]).astype(jnp.int32)
    where = jnp.where(line < FIT, where, 0)
    picker = ones(iota((per_plane, count), 0) + 1 == where)
    total = picked(picker, in_ref[...])
    for rest_ref in rest_and_out[:-1]:
        total = total + jnp.sum(rest_ref[...], axis=0)
    mine = plane_place(lax.axis_index("z")) * per_plane
    row = iota((per_plane, owner_ref.shape[1]), 0) + mine
    length = jnp.sum(
        jnp.where(row == plane_row(owner_ref[...]), length_ref[...], 0).astype(jnp.float32),
        axis=1,
        keepdims=True,
    )
    chunk = chunk_place()
    average = total / length + bias_ref[pl.ds(chunk, 1), :]
    owners, copies, rows, _ = out_ref.shape
    for o in range(owners):
        for y in range(copies):
            out_ref[o ^ 1, y] = average[o * rows : (o + 1) * rows, :]


def averages_for_owners(arrived, owner_slot, lengths, pool_bias, owners, copies, *rest):
    rows = owner_slot.shape[0] // (arrived.shape[0] // ROWS * owners)
    return pl.pallas_call(
        average_kernel,
        out_shape=jax.ShapeDtypeStruct((owners, copies, rows, LANES), jnp.float32),
        compiler_params=pltpu.CompilerParams(vmem_limit_bytes=GRANT),
        name="average",
    )(owner_slot.reshape(1, -1), lengths.reshape(1, -1), pool_bias.reshape(-1, LANES), arrived, *rest)


def norm_kernel(in_ref, out_ref):
    chunks, slices, rows, _ = in_ref.shape
    every = in_ref[...]
    square = jnp.sum(every * every, axis=(0, 1))
    energy = jnp.sum(square, axis=1, keepdims=True) / (chunks * slices * LANES)
    scale = lax.rsqrt(energy + 1e-06)
    mine = slice_place()
    for c, device in enumerate(CHUNK_GROUP[0]):
        values = in_ref[device ^ 1, mine] * scale
        out_ref[:, c * LANES : (c + 1) * LANES] = values.astype(jnp.bfloat16)


def normed(arrived):
    chunks, _, rows, _ = arrived.shape
    return pl.pallas_call(
        norm_kernel,
        out_shape=jax.ShapeDtypeStruct((rows, chunks * LANES), jnp.bfloat16),
        compiler_params=pltpu.CompilerParams(vmem_limit_bytes=GRANT),
        name="norm",
    )(arrived)


def swap(array, axes, group):
    return lax.all_to_all(
        array, axes, split_axis=0, concat_axis=0, tiled=True, axis_index_groups=group
    )


def local(hidden, seg_ids, lengths, owner_slot, pool_bias):
    chunks = lax.axis_size(("x", "c"))
    planes = lax.axis_size("z")
    slices = lax.axis_size("y")
    per_plane = lengths.shape[0] // planes
    slots = swap(local_sums(seg_ids, owner_slot, hidden, chunks), ("x", "c"), CHUNK_GROUP)
    placed, ready = place(slots, planes)
    over = crowded(ready, owner_slot, lengths, hidden.shape[0])
    rows = swap(placed.reshape(-1, 4, LANES), "z", PLANE_GROUP).reshape(placed.shape)
    args = (owner_slot, lengths, pool_bias, chunks, slices)

    def with_rest(rows, kept):
        rest = swap(place_rest(kept, planes, per_plane), "z", PLANE_GROUP)
        return averages_for_owners(rows, *args, rest)

    def alone(rows, kept):
        return averages_for_owners(rows, *args)

    average = lax.cond(over[0] > 0, with_rest, alone, rows, slots)
    mine = swap(average.reshape(chunks * slices, -1, LANES), ("x", "c", "y"), OWNER_GROUP)
    return normed(mine.reshape(average.shape))


def solution(mesh):
    torus = Mesh(mesh.devices.reshape(4, 16, 2, mesh.shape["hid"]), ("x", "z", "c", "y"))
    seq = ("x", "z", "c")
    return jax.shard_map(
        local,
        mesh=torus,
        in_specs=(P(seq, "y"), P(seq), P(), P(), P("y")),
        out_specs=P(seq, "y"),
        check_vma=False,
    )
```

```python
import functools

import jax
import jax.numpy as jnp
from jax import lax
from jax.experimental import pallas as pl
from jax.experimental.pallas import tpu as pltpu
from jax.sharding import Mesh
from jax.sharding import PartitionSpec as P

USED = 17
SLOTS = 24
LANES = 128
FIT = 11
ROWS = 12
PAIRS = 8
GRANT = 16 * 1024 * 1024
WIDE = 56 * 1024 * 1024


def chunk_place():
    return (((lax.axis_index("x") + 2) & 3) * 2 + lax.axis_index("c")) ^ 1


def plane_place(z):
    return (z + 4) & 15


def slice_place():
    return (lax.axis_index("y") + 2) & 3


CHUNK_GROUP = [[(((j >> 1) + 2) & 3) * 2 + (j & 1) ^ 1 for j in range(8)]]
PLANE_GROUP = [[(j + 12) & 15 for j in range(16)]]
OWNER_GROUP = [[((j & ~3) ^ 4) + ((j + 2) & 3) for j in range(32)]]


def plane_row(owner):
    return plane_place(owner >> 3) * 32 + (owner >> 7) * 8 + (owner & 7)


def ones(mask):
    return jnp.where(mask, 1.0, 0.0).astype(jnp.bfloat16)


def iota(shape, dim):
    return lax.broadcasted_iota(jnp.int32, shape, dim)


def small(array):
    return array.astype(jnp.float32).astype(jnp.bfloat16)


def dot(left, right):
    return jnp.dot(left, right, preferred_element_type=jnp.float32)


def dot_rows(left, right):
    return lax.dot_general(
        left, right, (((1,), (1,)), ((), ())), preferred_element_type=jnp.float32
    )


def picked(picker, values):
    high = values.astype(jnp.bfloat16)
    left_over = values - high.astype(jnp.float32)
    middle = left_over.astype(jnp.bfloat16)
    low = (left_over - middle.astype(jnp.float32)).astype(jnp.bfloat16)
    parts = dot(picker, jnp.concatenate([high, middle, low], axis=1))
    return parts[:, :LANES] + (parts[:, LANES : 2 * LANES] + parts[:, 2 * LANES :])


def marks_of(first, last, owner):
    docs = owner.shape[1]
    source = chunk_place()
    row = plane_row(owner) + 1
    part = iota((8, docs), 0)
    digits = jnp.where(part == 0, row >> 5, jnp.where(part == 1, row & 31, 0))
    lane = iota((docs, 2 * LANES), 1) - source * SLOTS
    doc = iota((docs, 2 * LANES), 0)
    meets = (doc == first + lane) & (doc <= last) & (lane >= 0) & (lane < USED)
    found = dot(small(digits), ones(meets))
    where = found[0:1, :] * 32.0 + found[1:2, :]
    line = iota((SLOTS, LANES), 0)
    second = jnp.where(line == SLOTS - 1, where[:, LANES:], 0.0)
    return jnp.where(line == SLOTS - 2, where[:, :LANES], second)


def most_rows(lengths, owner, tokens):
    docs = owner.shape[1]
    part = iota((8, docs), 0)
    digits = jnp.where(part == 0, lengths >> 7, jnp.where(part == 1, lengths & 127, 0))
    until = ones(iota((docs, docs), 0) <= iota((docs, docs), 1))
    sums = dot(small(digits), until)
    end = (sums[0:1, :] * 128.0 + sums[1:2, :]).astype(jnp.int32)
    start = end - lengths
    line = iota((LANES, docs), 0)
    device = (line >> 5) * 32 + (line & 15) * 2 + ((line >> 4) & 1)
    touches = (start < (device + 1) * tokens) & (end > device * tokens)
    owned = ((owner >> 3) & 15) == line
    counts = dot_rows(ones(touches), ones(owned))
    return jnp.max(jnp.sum(counts.reshape(8, 16, LANES), axis=0)).astype(jnp.int32)


def sums_kernel(
    pieces, seg_hbm, owner_hbm, hidden_hbm, out_ref, seg, owner, hidden, sems
):
    tokens = hidden.shape[0]
    rows = tokens // pieces
    copies = [
        pltpu.make_async_copy(seg_hbm, seg, sems.at[pieces]),
        pltpu.make_async_copy(owner_hbm, owner, sems.at[pieces + 1]),
    ]
    for p in range(pieces):
        here = pl.ds(p * rows, rows)
        copies.append(pltpu.make_async_copy(hidden_hbm.at[here], hidden.at[here], sems.at[p]))
    for copy in copies:
        copy.start()
    copies[0].wait()
    first = seg[0:1, 0:1]
    last = seg[0:1, tokens - 1 : tokens]
    copies[1].wait()
    marks = marks_of(first, last, owner[...])
    slot = iota((SLOTS, rows), 0) + first
    sums = None
    for p in range(pieces):
        picker = ones(slot == seg[:, p * rows : (p + 1) * rows])
        copies[2 + p].wait()
        term = dot(picker, hidden[p * rows : (p + 1) * rows, :])
        sums = term if sums is None else sums + term
    for c in range(out_ref.shape[0]):
        out_ref[c] = sums[:, c * LANES : (c + 1) * LANES] + marks


def local_sums(seg_ids, owner_slot, hidden, chunks):
    tokens, width = hidden.shape
    docs = owner_slot.shape[0]
    pieces = 8
    return pl.pallas_call(
        functools.partial(sums_kernel, pieces),
        in_specs=[pl.BlockSpec(memory_space=pltpu.HBM)] * 3,
        out_specs=pl.BlockSpec(memory_space=pltpu.VMEM),
        out_shape=pltpu.VMEM((chunks, SLOTS, LANES), jnp.float32),
        scratch_shapes=[
            pltpu.VMEM((1, tokens), jnp.int32),
            pltpu.VMEM((1, docs), jnp.int32),
            pltpu.VMEM((tokens, width), hidden.dtype),
            pltpu.SemaphoreType.DMA((pieces + 2,)),
        ],
        compiler_params=pltpu.CompilerParams(vmem_limit_bytes=WIDE),
        name="local_sums",
    )(seg_ids.reshape(1, -1), owner_slot.reshape(1, -1), hidden)


def slots_of(in_ref):
    sources = in_ref.shape[0]
    values = in_ref[...].reshape(sources * SLOTS, LANES)
    empty = jnp.zeros((2 * LANES - sources * SLOTS, LANES), jnp.float32)
    marks = jnp.sum(in_ref[:, SLOTS - 2 : SLOTS, :], axis=0).astype(jnp.int32)
    where = jnp.concatenate([marks[0:1, :], marks[1:2, :]], axis=1)
    plane = jnp.where(where > 0, (where - 1) >> 5, -1)
    bound = iota((16, 2 * LANES), 0) == plane
    ahead = iota((2 * LANES, 2 * LANES), 0) < iota((2 * LANES, 2 * LANES), 1)
    seen = dot(ones(bound), ones(ahead))
    rank = jnp.sum(jnp.where(bound, seen, 0.0), axis=0, keepdims=True).astype(jnp.int32)
    return jnp.concatenate([values, empty], axis=0), where, plane, bound, rank


def place_kernel(in_ref, out_ref, ready_ref):
    planes = out_ref.shape[0] // ROWS
    ready_ref[...] = jnp.zeros_like(ready_ref)
    values, where, plane, bound, rank = slots_of(in_ref)
    target = jnp.where((where > 0) & (rank < FIT), plane * ROWS + rank, -1)
    out_ref[...] = picked(ones(iota((planes * ROWS, 2 * LANES), 0) == target), values)
    number = (((where - 1) & 31) + 1) * jnp.where((rank & 1) == 1, 64, 1)
    lane = iota((LANES, 2 * LANES), 0) - plane_place(lax.axis_index("z")) * PAIRS
    numbers = dot_rows(small(jnp.where(bound, number, 0)), ones((lane == rank >> 1) & (rank < FIT)))
    for p in range(planes):
        out_ref[p * ROWS + FIT : (p + 1) * ROWS, :] = numbers[p : p + 1, :]


def place(slots, planes):
    return pl.pallas_call(
        place_kernel,
        out_specs=[
            pl.BlockSpec(memory_space=pltpu.VMEM),
            pl.BlockSpec(memory_space=pltpu.VMEM),
        ],
        out_shape=[
            pltpu.VMEM((planes * ROWS, LANES), jnp.float32),
            pltpu.VMEM((8, LANES), jnp.int32),
        ],
        compiler_params=pltpu.CompilerParams(vmem_limit_bytes=GRANT),
        name="place",
    )(slots)


def crowded_kernel(tokens, ready_ref, owner_ref, length_ref, over_ref):
    most = most_rows(length_ref[...], owner_ref[...], tokens)
    over_ref[0] = (most + jnp.max(ready_ref[...]) > FIT).astype(jnp.int32)


def crowded(ready, owner_slot, lengths, tokens):
    docs = owner_slot.shape[0]
    return pl.pallas_call(
        functools.partial(crowded_kernel, tokens),
        out_specs=pl.BlockSpec(memory_space=pltpu.SMEM),
        out_shape=jax.ShapeDtypeStruct((1,), jnp.int32),
        cost_estimate=pl.CostEstimate(
            flops=64 * docs * docs, bytes_accessed=8 * docs, transcendentals=0
        ),
        compiler_params=pltpu.CompilerParams(vmem_limit_bytes=GRANT),
        name="crowded",
    )(ready, owner_slot.reshape(1, -1), lengths.reshape(1, -1))


def place_rest_kernel(in_ref, out_ref):
    planes, per_plane, _ = out_ref.shape
    values, where, _, _, rank = slots_of(in_ref)
    row = iota((planes * per_plane, 2 * LANES), 0) + 1
    out_ref[...] = picked(ones((row == where) & (rank >= FIT)), values).reshape(out_ref.shape)


def place_rest(slots, planes, per_plane):
    return pl.pallas_call(
        place_rest_kernel,
        out_shape=jax.ShapeDtypeStruct((planes, per_plane, LANES), jnp.float32),
        compiler_params=pltpu.CompilerParams(vmem_limit_bytes=GRANT),
        name="place_rest",
    )(slots)


def average_kernel(owner_ref, length_ref, bias_ref, in_ref, *rest_and_out):
    out_ref = rest_and_out[-1]
    count = in_ref.shape[0]
    planes = count // ROWS
    per_plane = owner_ref.shape[1] // planes
    marks = in_ref[FIT:ROWS, :]
    for p in range(1, planes):
        marks = marks + in_ref[p * ROWS + FIT : (p + 1) * ROWS, :]
    marks = marks.astype(jnp.int32)
    part = iota((8, LANES), 0)
    halves = jnp.where(part == 0, marks & 63, jnp.where(part == 1, marks >> 6, 0))
    line = iota((LANES, count), 1)
    source = (line * 171) >> 11
    spread = dot(small(halves), ones(iota((LANES, count), 0) == source * PAIRS + ((line - source * ROWS) >> 1)))
    line = line[0:1, :]
    line = line - ((line * 171) >> 11) * ROWS
    where = jnp.where((line & 1) == 1, spread[1:2, :], spread[0:1, :]).astype(jnp.int32)
    where = jnp.where(line < FIT, where, 0)
    picker = ones(iota((per_plane, count), 0) + 1 == where)
    total = picked(picker, in_ref[...])
    for rest_ref in rest_and_out[:-1]:
        total = total + jnp.sum(rest_ref[...], axis=0)
    mine = plane_place(lax.axis_index("z")) * per_plane
    row = iota((per_plane, owner_ref.shape[1]), 0) + mine
    length = jnp.sum(
        jnp.where(row == plane_row(owner_ref[...]), length_ref[...], 0).astype(jnp.float32),
        axis=1,
        keepdims=True,
    )
    chunk = chunk_place()
    average = total / length + bias_ref[pl.ds(chunk, 1), :]
    owners, copies, rows, _ = out_ref.shape
    for o in range(owners):
        for y in range(copies):
            out_ref[o ^ 1, y] = average[o * rows : (o + 1) * rows, :]


def averages_for_owners(arrived, owner_slot, lengths, pool_bias, owners, copies, *rest):
    rows = owner_slot.shape[0] // (arrived.shape[0] // ROWS * owners)
    return pl.pallas_call(
        average_kernel,
        out_shape=jax.ShapeDtypeStruct((owners, copies, rows, LANES), jnp.float32),
        compiler_params=pltpu.CompilerParams(vmem_limit_bytes=GRANT),
        name="average",
    )(owner_slot.reshape(1, -1), lengths.reshape(1, -1), pool_bias.reshape(-1, LANES), arrived, *rest)


def norm_kernel(in_ref, out_ref):
    chunks, slices, rows, _ = in_ref.shape
    every = in_ref[...]
    square = jnp.sum(every * every, axis=(0, 1))
    energy = jnp.sum(square, axis=1, keepdims=True) / (chunks * slices * LANES)
    scale = lax.rsqrt(energy + 1e-06)
    mine = slice_place()
    for c, device in enumerate(CHUNK_GROUP[0]):
        values = in_ref[device ^ 1, mine] * scale
        out_ref[:, c * LANES : (c + 1) * LANES] = values.astype(jnp.bfloat16)


def normed(arrived):
    chunks, _, rows, _ = arrived.shape
    return pl.pallas_call(
        norm_kernel,
        out_shape=jax.ShapeDtypeStruct((rows, chunks * LANES), jnp.bfloat16),
        compiler_params=pltpu.CompilerParams(vmem_limit_bytes=GRANT),
        name="norm",
    )(arrived)


def swap(array, axes, group):
    return lax.all_to_all(
        array, axes, split_axis=0, concat_axis=0, tiled=True, axis_index_groups=group
    )


def local(hidden, seg_ids, lengths, owner_slot, pool_bias):
    chunks = lax.axis_size(("x", "c"))
    planes = lax.axis_size("z")
    slices = lax.axis_size("y")
    per_plane = lengths.shape[0] // planes
    slots = swap(local_sums(seg_ids, owner_slot, hidden, chunks), ("x", "c"), CHUNK_GROUP)
    placed, ready = place(slots, planes)
    over = crowded(ready, owner_slot, lengths, hidden.shape[0])
    rows = swap(placed.reshape(-1, 4, LANES), "z", PLANE_GROUP).reshape(placed.shape)
    args = (owner_slot, lengths, pool_bias, chunks, slices)

    def with_rest(rows, kept):
        rest = swap(place_rest(kept, planes, per_plane), "z", PLANE_GROUP)
        return averages_for_owners(rows, *args, rest)

    def alone(rows, kept):
        return averages_for_owners(rows, *args)

    average = lax.cond(over[0] > 0, with_rest, alone, rows, slots)
    mine = swap(average.reshape(chunks * slices, -1, LANES), ("x", "c", "y"), OWNER_GROUP)
    return normed(mine.reshape(average.shape))


def solution(mesh):
    torus = Mesh(mesh.devices.reshape(4, 16, 2, mesh.shape["hid"]), ("x", "z", "c", "y"))
    seq = ("x", "z", "c")
    return jax.shard_map(
        local,
        mesh=torus,
        in_specs=(P(seq, "y"), P(seq), P(), P(), P("y")),
        out_specs=P(seq, "y"),
        check_vma=False,
    )
```

```python
import functools

import jax
import jax.numpy as jnp
from jax import lax
from jax.experimental import pallas as pl
from jax.experimental.pallas import tpu as pltpu
from jax.sharding import Mesh
from jax.sharding import PartitionSpec as P

USED = 17
SLOTS = 24
LANES = 128
FIT = 11
ROWS = 12
PAIRS = 8
GRANT = 16 * 1024 * 1024
WIDE = 56 * 1024 * 1024


def chunk_place():
    return (((lax.axis_index("x") + 2) & 3) * 2 + lax.axis_index("c")) ^ 1


def plane_place(z):
    return (z + 6) & 15


def slice_place():
    return (lax.axis_index("y") + 2) & 3


CHUNK_GROUP = [[(((j >> 1) + 2) & 3) * 2 + (j & 1) ^ 1 for j in range(8)]]
PLANE_GROUP = [[(j + 10) & 15 for j in range(16)]]
OWNER_GROUP = [[((j & ~3) ^ 4) + ((j + 2) & 3) for j in range(32)]]


def plane_row(owner):
    return plane_place(owner >> 3) * 32 + (owner >> 7) * 8 + (owner & 7)


def ones(mask):
    return jnp.where(mask, 1.0, 0.0).astype(jnp.bfloat16)


def iota(shape, dim):
    return lax.broadcasted_iota(jnp.int32, shape, dim)


def small(array):
    return array.astype(jnp.float32).astype(jnp.bfloat16)


def dot(left, right):
    return jnp.dot(left, right, preferred_element_type=jnp.float32)


def dot_rows(left, right):
    return lax.dot_general(
        left, right, (((1,), (1,)), ((), ())), preferred_element_type=jnp.float32
    )


def picked(picker, values):
    high = values.astype(jnp.bfloat16)
    left_over = values - high.astype(jnp.float32)
    middle = left_over.astype(jnp.bfloat16)
    low = (left_over - middle.astype(jnp.float32)).astype(jnp.bfloat16)
    parts = dot(picker, jnp.concatenate([high, middle, low], axis=1))
    return parts[:, :LANES] + (parts[:, LANES : 2 * LANES] + parts[:, 2 * LANES :])


def marks_of(first, last, owner):
    docs = owner.shape[1]
    source = chunk_place()
    row = plane_row(owner) + 1
    part = iota((8, docs), 0)
    digits = jnp.where(part == 0, row >> 5, jnp.where(part == 1, row & 31, 0))
    lane = iota((docs, 2 * LANES), 1) - source * SLOTS
    doc = iota((docs, 2 * LANES), 0)
    meets = (doc == first + lane) & (doc <= last) & (lane >= 0) & (lane < USED)
    found = dot(small(digits), ones(meets))
    where = found[0:1, :] * 32.0 + found[1:2, :]
    line = iota((SLOTS, LANES), 0)
    second = jnp.where(line == SLOTS - 1, where[:, LANES:], 0.0)
    return jnp.where(line == SLOTS - 2, where[:, :LANES], second)


def most_rows(lengths, owner, tokens):
    docs = owner.shape[1]
    part = iota((8, docs), 0)
    digits = jnp.where(part == 0, lengths >> 7, jnp.where(part == 1, lengths & 127, 0))
    until = ones(iota((docs, docs), 0) <= iota((docs, docs), 1))
    sums = dot(small(digits), until)
    end = (sums[0:1, :] * 128.0 + sums[1:2, :]).astype(jnp.int32)
    start = end - lengths
    line = iota((LANES, docs), 0)
    device = (line >> 5) * 32 + (line & 15) * 2 + ((line >> 4) & 1)
    touches = (start < (device + 1) * tokens) & (end > device * tokens)
    owned = ((owner >> 3) & 15) == line
    counts = dot_rows(ones(touches), ones(owned))
    return jnp.max(jnp.sum(counts.reshape(8, 16, LANES), axis=0)).astype(jnp.int32)


def sums_kernel(
    pieces, seg_hbm, owner_hbm, hidden_hbm, out_ref, seg, owner, hidden, sems
):
    tokens = hidden.shape[0]
    rows = tokens // pieces
    copies = [
        pltpu.make_async_copy(seg_hbm, seg, sems.at[pieces]),
        pltpu.make_async_copy(owner_hbm, owner, sems.at[pieces + 1]),
    ]
    for p in range(pieces):
        here = pl.ds(p * rows, rows)
        copies.append(pltpu.make_async_copy(hidden_hbm.at[here], hidden.at[here], sems.at[p]))
    for copy in copies:
        copy.start()
    copies[0].wait()
    first = seg[0:1, 0:1]
    last = seg[0:1, tokens - 1 : tokens]
    copies[1].wait()
    marks = marks_of(first, last, owner[...])
    slot = iota((SLOTS, rows), 0) + first
    sums = None
    for p in range(pieces):
        picker = ones(slot == seg[:, p * rows : (p + 1) * rows])
        copies[2 + p].wait()
        term = dot(picker, hidden[p * rows : (p + 1) * rows, :])
        sums = term if sums is None else sums + term
    for c in range(out_ref.shape[0]):
        out_ref[c] = sums[:, c * LANES : (c + 1) * LANES] + marks


def local_sums(seg_ids, owner_slot, hidden, chunks):
    tokens, width = hidden.shape
    docs = owner_slot.shape[0]
    pieces = 2
    return pl.pallas_call(
        functools.partial(sums_kernel, pieces),
        in_specs=[pl.BlockSpec(memory_space=pltpu.HBM)] * 3,
        out_specs=pl.BlockSpec(memory_space=pltpu.VMEM),
        out_shape=pltpu.VMEM((chunks, SLOTS, LANES), jnp.float32),
        scratch_shapes=[
            pltpu.VMEM((1, tokens), jnp.int32),
            pltpu.VMEM((1, docs), jnp.int32),
            pltpu.VMEM((tokens, width), hidden.dtype),
            pltpu.SemaphoreType.DMA((pieces + 2,)),
        ],
        compiler_params=pltpu.CompilerParams(vmem_limit_bytes=WIDE),
        name="local_sums",
    )(seg_ids.reshape(1, -1), owner_slot.reshape(1, -1), hidden)


def slots_of(in_ref):
    sources = in_ref.shape[0]
    values = in_ref[...].reshape(sources * SLOTS, LANES)
    empty = jnp.zeros((2 * LANES - sources * SLOTS, LANES), jnp.float32)
    marks = jnp.sum(in_ref[:, SLOTS - 2 : SLOTS, :], axis=0).astype(jnp.int32)
    where = jnp.concatenate([marks[0:1, :], marks[1:2, :]], axis=1)
    plane = jnp.where(where > 0, (where - 1) >> 5, -1)
    bound = iota((16, 2 * LANES), 0) == plane
    ahead = iota((2 * LANES, 2 * LANES), 0) < iota((2 * LANES, 2 * LANES), 1)
    seen = dot(ones(bound), ones(ahead))
    rank = jnp.sum(jnp.where(bound, seen, 0.0), axis=0, keepdims=True).astype(jnp.int32)
    return jnp.concatenate([values, empty], axis=0), where, plane, bound, rank


def place_kernel(in_ref, out_ref, ready_ref):
    planes = out_ref.shape[0] // ROWS
    ready_ref[...] = jnp.zeros_like(ready_ref)
    values, where, plane, bound, rank = slots_of(in_ref)
    target = jnp.where((where > 0) & (rank < FIT), plane * ROWS + rank, -1)
    out_ref[...] = picked(ones(iota((planes * ROWS, 2 * LANES), 0) == target), values)
    number = (((where - 1) & 31) + 1) * jnp.where((rank & 1) == 1, 64, 1)
    lane = iota((LANES, 2 * LANES), 0) - plane_place(lax.axis_index("z")) * PAIRS
    numbers = dot_rows(small(jnp.where(bound, number, 0)), ones((lane == rank >> 1) & (rank < FIT)))
    for p in range(planes):
        out_ref[p * ROWS + FIT : (p + 1) * ROWS, :] = numbers[p : p + 1, :]


def place(slots, planes):
    return pl.pallas_call(
        place_kernel,
        out_specs=[
            pl.BlockSpec(memory_space=pltpu.VMEM),
            pl.BlockSpec(memory_space=pltpu.VMEM),
        ],
        out_shape=[
            pltpu.VMEM((planes * ROWS, LANES), jnp.float32),
            pltpu.VMEM((8, LANES), jnp.int32),
        ],
        compiler_params=pltpu.CompilerParams(vmem_limit_bytes=GRANT),
        name="place",
    )(slots)


def crowded_kernel(tokens, ready_ref, owner_ref, length_ref, over_ref):
    most = most_rows(length_ref[...], owner_ref[...], tokens)
    over_ref[0] = (most + jnp.max(ready_ref[...]) > FIT).astype(jnp.int32)


def crowded(ready, owner_slot, lengths, tokens):
    docs = owner_slot.shape[0]
    return pl.pallas_call(
        functools.partial(crowded_kernel, tokens),
        out_specs=pl.BlockSpec(memory_space=pltpu.SMEM),
        out_shape=jax.ShapeDtypeStruct((1,), jnp.int32),
        cost_estimate=pl.CostEstimate(
            flops=64 * docs * docs, bytes_accessed=8 * docs, transcendentals=0
        ),
        compiler_params=pltpu.CompilerParams(vmem_limit_bytes=GRANT),
        name="crowded",
    )(ready, owner_slot.reshape(1, -1), lengths.reshape(1, -1))


def place_rest_kernel(in_ref, out_ref):
    planes, per_plane, _ = out_ref.shape
    values, where, _, _, rank = slots_of(in_ref)
    row = iota((planes * per_plane, 2 * LANES), 0) + 1
    out_ref[...] = picked(ones((row == where) & (rank >= FIT)), values).reshape(out_ref.shape)


def place_rest(slots, planes, per_plane):
    return pl.pallas_call(
        place_rest_kernel,
        out_shape=jax.ShapeDtypeStruct((planes, per_plane, LANES), jnp.float32),
        compiler_params=pltpu.CompilerParams(vmem_limit_bytes=GRANT),
        name="place_rest",
    )(slots)


def average_kernel(owner_ref, length_ref, bias_ref, in_ref, *rest_and_out):
    out_ref = rest_and_out[-1]
    count = in_ref.shape[0]
    planes = count // ROWS
    per_plane = owner_ref.shape[1] // planes
    marks = in_ref[FIT:ROWS, :]
    for p in range(1, planes):
        marks = marks + in_ref[p * ROWS + FIT : (p + 1) * ROWS, :]
    marks = marks.astype(jnp.int32)
    part = iota((8, LANES), 0)
    halves = jnp.where(part == 0, marks & 63, jnp.where(part == 1, marks >> 6, 0))
    line = iota((LANES, count), 1)
    source = (line * 171) >> 11
    spread = dot(small(halves), ones(iota((LANES, count), 0) == source * PAIRS + ((line - source * ROWS) >> 1)))
    line = line[0:1, :]
    line = line - ((line * 171) >> 11) * ROWS
    where = jnp.where((line & 1) == 1, spread[1:2, :], spread[0:1, :]).astype(jnp.int32)
    where = jnp.where(line < FIT, where, 0)
    picker = ones(iota((per_plane, count), 0) + 1 == where)
    total = picked(picker, in_ref[...])
    for rest_ref in rest_and_out[:-1]:
        total = total + jnp.sum(rest_ref[...], axis=0)
    mine = plane_place(lax.axis_index("z")) * per_plane
    row = iota((per_plane, owner_ref.shape[1]), 0) + mine
    length = jnp.sum(
        jnp.where(row == plane_row(owner_ref[...]), length_ref[...], 0).astype(jnp.float32),
        axis=1,
        keepdims=True,
    )
    chunk = chunk_place()
    average = total / length + bias_ref[pl.ds(chunk, 1), :]
    owners, copies, rows, _ = out_ref.shape
    for o in range(owners):
        for y in range(copies):
            out_ref[o ^ 1, y] = average[o * rows : (o + 1) * rows, :]


def averages_for_owners(arrived, owner_slot, lengths, pool_bias, owners, copies, *rest):
    rows = owner_slot.shape[0] // (arrived.shape[0] // ROWS * owners)
    return pl.pallas_call(
        average_kernel,
        out_shape=jax.ShapeDtypeStruct((owners, copies, rows, LANES), jnp.float32),
        compiler_params=pltpu.CompilerParams(vmem_limit_bytes=GRANT),
        name="average",
    )(owner_slot.reshape(1, -1), lengths.reshape(1, -1), pool_bias.reshape(-1, LANES), arrived, *rest)


def norm_kernel(in_ref, out_ref):
    chunks, slices, rows, _ = in_ref.shape
    every = in_ref[...]
    square = jnp.sum(every * every, axis=(0, 1))
    energy = jnp.sum(square, axis=1, keepdims=True) / (chunks * slices * LANES)
    scale = lax.rsqrt(energy + 1e-06)
    mine = slice_place()
    for c, device in enumerate(CHUNK_GROUP[0]):
        values = in_ref[device ^ 1, mine] * scale
        out_ref[:, c * LANES : (c + 1) * LANES] = values.astype(jnp.bfloat16)


def normed(arrived):
    chunks, _, rows, _ = arrived.shape
    return pl.pallas_call(
        norm_kernel,
        out_shape=jax.ShapeDtypeStruct((rows, chunks * LANES), jnp.bfloat16),
        compiler_params=pltpu.CompilerParams(vmem_limit_bytes=GRANT),
        name="norm",
    )(arrived)


def swap(array, axes, group):
    return lax.all_to_all(
        array, axes, split_axis=0, concat_axis=0, tiled=True, axis_index_groups=group
    )


def local(hidden, seg_ids, lengths, owner_slot, pool_bias):
    chunks = lax.axis_size(("x", "c"))
    planes = lax.axis_size("z")
    slices = lax.axis_size("y")
    per_plane = lengths.shape[0] // planes
    slots = swap(local_sums(seg_ids, owner_slot, hidden, chunks), ("x", "c"), CHUNK_GROUP)
    placed, ready = place(slots, planes)
    over = crowded(ready, owner_slot, lengths, hidden.shape[0])
    rows = swap(placed.reshape(-1, 4, LANES), "z", PLANE_GROUP).reshape(placed.shape)
    args = (owner_slot, lengths, pool_bias, chunks, slices)

    def with_rest(rows, kept):
        rest = swap(place_rest(kept, planes, per_plane), "z", PLANE_GROUP)
        return averages_for_owners(rows, *args, rest)

    def alone(rows, kept):
        return averages_for_owners(rows, *args)

    average = lax.cond(over[0] > 0, with_rest, alone, rows, slots)
    mine = swap(average.reshape(chunks * slices, -1, LANES), ("x", "c", "y"), OWNER_GROUP)
    return normed(mine.reshape(average.shape))


def solution(mesh):
    torus = Mesh(mesh.devices.reshape(4, 16, 2, mesh.shape["hid"]), ("x", "z", "c", "y"))
    seq = ("x", "z", "c")
    return jax.shard_map(
        local,
        mesh=torus,
        in_specs=(P(seq, "y"), P(seq), P(), P(), P("y")),
        out_specs=P(seq, "y"),
        check_vma=False,
    )
```

```python
import functools

import jax
import jax.numpy as jnp
from jax import lax
from jax.experimental import pallas as pl
from jax.experimental.pallas import tpu as pltpu
from jax.sharding import Mesh
from jax.sharding import PartitionSpec as P

USED = 17
SLOTS = 24
LANES = 128
FIT = 11
ROWS = 12
PAIRS = 8
SPLIT = 4
GRANT = 16 * 1024 * 1024
WIDE = 56 * 1024 * 1024


def chunk_place():
    return (((lax.axis_index("x") + 2) & 3) * 2 + lax.axis_index("c")) ^ 1


def plane_place(z):
    return (z + 7) & 15


def slice_place():
    return (lax.axis_index("y") + 2) & 3


CHUNK_GROUP = [[(((j >> 1) + 2) & 3) * 2 + (j & 1) ^ 1 for j in range(8)]]
PLANE_GROUP = [[(j + 9) & 15 for j in range(16)]]
OWNER_GROUP = [[((j & ~3) ^ 4) + ((j + 2) & 3) for j in range(32)]]


def plane_row(owner):
    return plane_place(owner >> 3) * 32 + (owner >> 7) * 8 + (owner & 7)


def ones(mask):
    return jnp.where(mask, 1.0, 0.0).astype(jnp.bfloat16)


def iota(shape, dim):
    return lax.broadcasted_iota(jnp.int32, shape, dim)


def small(array):
    return array.astype(jnp.float32).astype(jnp.bfloat16)


def dot(left, right):
    return jnp.dot(left, right, preferred_element_type=jnp.float32)


def dot_rows(left, right):
    return lax.dot_general(
        left, right, (((1,), (1,)), ((), ())), preferred_element_type=jnp.float32
    )


def picked(picker, values):
    high = values.astype(jnp.bfloat16)
    left_over = values - high.astype(jnp.float32)
    middle = left_over.astype(jnp.bfloat16)
    low = (left_over - middle.astype(jnp.float32)).astype(jnp.bfloat16)
    parts = dot(picker, jnp.concatenate([high, middle, low], axis=1))
    return parts[:, :LANES] + (parts[:, LANES : 2 * LANES] + parts[:, 2 * LANES :])


def marks_of(first, last, owner):
    docs = owner.shape[1]
    source = chunk_place()
    row = plane_row(owner) + 1
    part = iota((8, docs), 0)
    digits = jnp.where(part == 0, row >> 5, jnp.where(part == 1, row & 31, 0))
    lane = iota((docs, 2 * LANES), 1) - source * SLOTS
    doc = iota((docs, 2 * LANES), 0)
    meets = (doc == first + lane) & (doc <= last) & (lane >= 0) & (lane < USED)
    found = dot(small(digits), ones(meets))
    where = found[0:1, :] * 32.0 + found[1:2, :]
    line = iota((SLOTS, LANES), 0)
    second = jnp.where(line == SLOTS - 1, where[:, LANES:], 0.0)
    return jnp.where(line == SLOTS - 2, where[:, :LANES], second)


def most_rows(lengths, owner, tokens):
    docs = owner.shape[1]
    part = iota((8, docs), 0)
    digits = jnp.where(part == 0, lengths >> 7, jnp.where(part == 1, lengths & 127, 0))
    until = ones(iota((docs, docs), 0) <= iota((docs, docs), 1))
    sums = dot(small(digits), until)
    end = (sums[0:1, :] * 128.0 + sums[1:2, :]).astype(jnp.int32)
    start = end - lengths
    line = iota((LANES, docs), 0)
    device = (line >> 5) * 32 + (line & 15) * 2 + ((line >> 4) & 1)
    touches = (start < (device + 1) * tokens) & (end > device * tokens)
    owned = ((owner >> 3) & 15) == line
    counts = dot_rows(ones(touches), ones(owned))
    return jnp.max(jnp.sum(counts.reshape(8, 16, LANES), axis=0)).astype(jnp.int32)


def sums_kernel(
    pieces, seg_hbm, owner_hbm, hidden_hbm, out_ref, seg, owner, hidden, sems
):
    tokens = hidden.shape[0]
    rows = tokens // pieces
    copies = [
        pltpu.make_async_copy(seg_hbm, seg, sems.at[pieces * SPLIT]),
        pltpu.make_async_copy(owner_hbm, owner, sems.at[pieces * SPLIT + 1]),
    ]
    few = rows // SPLIT
    for p in range(pieces * SPLIT):
        here = pl.ds(p * few, few)
        copies.append(pltpu.make_async_copy(hidden_hbm.at[here], hidden.at[here], sems.at[p]))
    for copy in copies:
        copy.start()
    copies[0].wait()
    first = seg[0:1, 0:1]
    last = seg[0:1, tokens - 1 : tokens]
    copies[1].wait()
    marks = marks_of(first, last, owner[...])
    slot = iota((SLOTS, rows), 0) + first
    sums = None
    for p in range(pieces):
        picker = ones(slot == seg[:, p * rows : (p + 1) * rows])
        for copy in copies[2 + p * SPLIT : 2 + (p + 1) * SPLIT]:
            copy.wait()
        term = dot(picker, hidden[p * rows : (p + 1) * rows, :])
        sums = term if sums is None else sums + term
    for c in range(out_ref.shape[0]):
        out_ref[c] = sums[:, c * LANES : (c + 1) * LANES] + marks


def local_sums(seg_ids, owner_slot, hidden, chunks):
    tokens, width = hidden.shape
    docs = owner_slot.shape[0]
    pieces = 4
    return pl.pallas_call(
        functools.partial(sums_kernel, pieces),
        in_specs=[pl.BlockSpec(memory_space=pltpu.HBM)] * 3,
        out_specs=pl.BlockSpec(memory_space=pltpu.VMEM),
        out_shape=pltpu.VMEM((chunks, SLOTS, LANES), jnp.float32),
        scratch_shapes=[
            pltpu.VMEM((1, tokens), jnp.int32),
            pltpu.VMEM((1, docs), jnp.int32),
            pltpu.VMEM((tokens, width), hidden.dtype),
            pltpu.SemaphoreType.DMA((pieces * SPLIT + 2,)),
        ],
        compiler_params=pltpu.CompilerParams(vmem_limit_bytes=WIDE),
        name="local_sums",
    )(seg_ids.reshape(1, -1), owner_slot.reshape(1, -1), hidden)


def slots_of(in_ref):
    sources = in_ref.shape[0]
    values = in_ref[...].reshape(sources * SLOTS, LANES)
    empty = jnp.zeros((2 * LANES - sources * SLOTS, LANES), jnp.float32)
    marks = jnp.sum(in_ref[:, SLOTS - 2 : SLOTS, :], axis=0).astype(jnp.int32)
    where = jnp.concatenate([marks[0:1, :], marks[1:2, :]], axis=1)
    plane = jnp.where(where > 0, (where - 1) >> 5, -1)
    bound = iota((16, 2 * LANES), 0) == plane
    ahead = iota((2 * LANES, 2 * LANES), 0) < iota((2 * LANES, 2 * LANES), 1)
    seen = dot(ones(bound), ones(ahead))
    rank = jnp.sum(jnp.where(bound, seen, 0.0), axis=0, keepdims=True).astype(jnp.int32)
    return jnp.concatenate([values, empty], axis=0), where, plane, bound, rank


def place_kernel(in_ref, out_ref, ready_ref):
    planes = out_ref.shape[0] // ROWS
    ready_ref[...] = jnp.zeros_like(ready_ref)
    values, where, plane, bound, rank = slots_of(in_ref)
    target = jnp.where((where > 0) & (rank < FIT), plane * ROWS + rank, -1)
    out_ref[...] = picked(ones(iota((planes * ROWS, 2 * LANES), 0) == target), values)
    number = (((where - 1) & 31) + 1) * jnp.where((rank & 1) == 1, 64, 1)
    lane = iota((LANES, 2 * LANES), 0) - plane_place(lax.axis_index("z")) * PAIRS
    numbers = dot_rows(small(jnp.where(bound, number, 0)), ones((lane == rank >> 1) & (rank < FIT)))
    for p in range(planes):
        out_ref[p * ROWS + FIT : (p + 1) * ROWS, :] = numbers[p : p + 1, :]


def place(slots, planes):
    return pl.pallas_call(
        place_kernel,
        out_specs=[
            pl.BlockSpec(memory_space=pltpu.VMEM),
            pl.BlockSpec(memory_space=pltpu.VMEM),
        ],
        out_shape=[
            pltpu.VMEM((planes * ROWS, LANES), jnp.float32),
            pltpu.VMEM((8, LANES), jnp.int32),
        ],
        compiler_params=pltpu.CompilerParams(vmem_limit_bytes=GRANT),
        name="place",
    )(slots)


def crowded_kernel(tokens, ready_ref, owner_ref, length_ref, over_ref):
    most = most_rows(length_ref[...], owner_ref[...], tokens)
    over_ref[0] = (most + jnp.max(ready_ref[...]) > FIT).astype(jnp.int32)


def crowded(ready, owner_slot, lengths, tokens):
    docs = owner_slot.shape[0]
    return pl.pallas_call(
        functools.partial(crowded_kernel, tokens),
        out_specs=pl.BlockSpec(memory_space=pltpu.SMEM),
        out_shape=jax.ShapeDtypeStruct((1,), jnp.int32),
        cost_estimate=pl.CostEstimate(
            flops=64 * docs * docs, bytes_accessed=8 * docs, transcendentals=0
        ),
        compiler_params=pltpu.CompilerParams(vmem_limit_bytes=GRANT),
        name="crowded",
    )(ready, owner_slot.reshape(1, -1), lengths.reshape(1, -1))


def place_rest_kernel(in_ref, out_ref):
    planes, per_plane, _ = out_ref.shape
    values, where, _, _, rank = slots_of(in_ref)
    row = iota((planes * per_plane, 2 * LANES), 0) + 1
    out_ref[...] = picked(ones((row == where) & (rank >= FIT)), values).reshape(out_ref.shape)


def place_rest(slots, planes, per_plane):
    return pl.pallas_call(
        place_rest_kernel,
        out_shape=jax.ShapeDtypeStruct((planes, per_plane, LANES), jnp.float32),
        compiler_params=pltpu.CompilerParams(vmem_limit_bytes=GRANT),
        name="place_rest",
    )(slots)


def average_kernel(owner_ref, length_ref, bias_ref, in_ref, *rest_and_out):
    out_ref = rest_and_out[-1]
    count = in_ref.shape[0]
    planes = count // ROWS
    per_plane = owner_ref.shape[1] // planes
    marks = in_ref[FIT:ROWS, :]
    for p in range(1, planes):
        marks = marks + in_ref[p * ROWS + FIT : (p + 1) * ROWS, :]
    marks = marks.astype(jnp.int32)
    part = iota((8, LANES), 0)
    halves = jnp.where(part == 0, marks & 63, jnp.where(part == 1, marks >> 6, 0))
    line = iota((LANES, count), 1)
    source = (line * 171) >> 11
    spread = dot(small(halves), ones(iota((LANES, count), 0) == source * PAIRS + ((line - source * ROWS) >> 1)))
    line = line[0:1, :]
    line = line - ((line * 171) >> 11) * ROWS
    where = jnp.where((line & 1) == 1, spread[1:2, :], spread[0:1, :]).astype(jnp.int32)
    where = jnp.where(line < FIT, where, 0)
    picker = ones(iota((per_plane, count), 0) + 1 == where)
    total = picked(picker, in_ref[...])
    for rest_ref in rest_and_out[:-1]:
        total = total + jnp.sum(rest_ref[...], axis=0)
    mine = plane_place(lax.axis_index("z")) * per_plane
    row = iota((per_plane, owner_ref.shape[1]), 0) + mine
    length = jnp.sum(
        jnp.where(row == plane_row(owner_ref[...]), length_ref[...], 0).astype(jnp.float32),
        axis=1,
        keepdims=True,
    )
    chunk = chunk_place()
    average = total / length + bias_ref[pl.ds(chunk, 1), :]
    owners, copies, rows, _ = out_ref.shape
    for o in range(owners):
        for y in range(copies):
            out_ref[o ^ 1, y] = average[o * rows : (o + 1) * rows, :]


def averages_for_owners(arrived, owner_slot, lengths, pool_bias, owners, copies, *rest):
    rows = owner_slot.shape[0] // (arrived.shape[0] // ROWS * owners)
    return pl.pallas_call(
        average_kernel,
        out_shape=jax.ShapeDtypeStruct((owners, copies, rows, LANES), jnp.float32),
        compiler_params=pltpu.CompilerParams(vmem_limit_bytes=GRANT),
        name="average",
    )(owner_slot.reshape(1, -1), lengths.reshape(1, -1), pool_bias.reshape(-1, LANES), arrived, *rest)


def norm_kernel(in_ref, out_ref):
    chunks, slices, rows, _ = in_ref.shape
    every = in_ref[...]
    square = jnp.sum(every * every, axis=(0, 1))
    energy = jnp.sum(square, axis=1, keepdims=True) / (chunks * slices * LANES)
    scale = lax.rsqrt(energy + 1e-06)
    mine = slice_place()
    for c, device in enumerate(CHUNK_GROUP[0]):
        values = in_ref[device ^ 1, mine] * scale
        out_ref[:, c * LANES : (c + 1) * LANES] = values.astype(jnp.bfloat16)


def normed(arrived):
    chunks, _, rows, _ = arrived.shape
    return pl.pallas_call(
        norm_kernel,
        out_shape=jax.ShapeDtypeStruct((rows, chunks * LANES), jnp.bfloat16),
        compiler_params=pltpu.CompilerParams(vmem_limit_bytes=GRANT),
        name="norm",
    )(arrived)


def swap(array, axes, group):
    return lax.all_to_all(
        array, axes, split_axis=0, concat_axis=0, tiled=True, axis_index_groups=group
    )


def local(hidden, seg_ids, lengths, owner_slot, pool_bias):
    chunks = lax.axis_size(("x", "c"))
    planes = lax.axis_size("z")
    slices = lax.axis_size("y")
    per_plane = lengths.shape[0] // planes
    slots = swap(local_sums(seg_ids, owner_slot, hidden, chunks), ("x", "c"), CHUNK_GROUP)
    placed, ready = place(slots, planes)
    over = crowded(ready, owner_slot, lengths, hidden.shape[0])
    rows = swap(placed.reshape(-1, 4, LANES), "z", PLANE_GROUP).reshape(placed.shape)
    args = (owner_slot, lengths, pool_bias, chunks, slices)

    def with_rest(rows, kept):
        rest = swap(place_rest(kept, planes, per_plane), "z", PLANE_GROUP)
        return averages_for_owners(rows, *args, rest)

    def alone(rows, kept):
        return averages_for_owners(rows, *args)

    average = lax.cond(over[0] > 0, with_rest, alone, rows, slots)
    mine = swap(average.reshape(chunks * slices, -1, LANES), ("x", "c", "y"), OWNER_GROUP)
    return normed(mine.reshape(average.shape))


def solution(mesh):
    torus = Mesh(mesh.devices.reshape(4, 16, 2, mesh.shape["hid"]), ("x", "z", "c", "y"))
    seq = ("x", "z", "c")
    return jax.shard_map(
        local,
        mesh=torus,
        in_specs=(P(seq, "y"), P(seq), P(), P(), P("y")),
        out_specs=P(seq, "y"),
        check_vma=False,
    )
```

```python
import functools

import jax
import jax.numpy as jnp
from jax import lax
from jax.experimental import pallas as pl
from jax.experimental.pallas import tpu as pltpu
from jax.sharding import Mesh
from jax.sharding import PartitionSpec as P

USED = 17
SLOTS = 20
LANES = 128
FIT = 11
ROWS = 12
PAIRS = 8
GRANT = 16 * 1024 * 1024
WIDE = 56 * 1024 * 1024


def chunk_place():
    return (((lax.axis_index("x") + 2) & 3) * 2 + lax.axis_index("c")) ^ 1


def plane_place(z):
    return (z + 6) & 15


def slice_place():
    return (lax.axis_index("y") + 2) & 3


CHUNK_GROUP = [[(((j >> 1) + 2) & 3) * 2 + (j & 1) ^ 1 for j in range(8)]]
PLANE_GROUP = [[(j + 10) & 15 for j in range(16)]]
OWNER_GROUP = [[((j & ~3) ^ 4) + ((j + 2) & 3) for j in range(32)]]


def plane_row(owner):
    return plane_place(owner >> 3) * 32 + (owner >> 7) * 8 + (owner & 7)


def ones(mask):
    return jnp.where(mask, 1.0, 0.0).astype(jnp.bfloat16)


def iota(shape, dim):
    return lax.broadcasted_iota(jnp.int32, shape, dim)


def small(array):
    return array.astype(jnp.float32).astype(jnp.bfloat16)


def dot(left, right):
    return jnp.dot(left, right, preferred_element_type=jnp.float32)


def dot_rows(left, right):
    return lax.dot_general(
        left, right, (((1,), (1,)), ((), ())), preferred_element_type=jnp.float32
    )


def picked(picker, values):
    high = values.astype(jnp.bfloat16)
    left_over = values - high.astype(jnp.float32)
    middle = left_over.astype(jnp.bfloat16)
    low = (left_over - middle.astype(jnp.float32)).astype(jnp.bfloat16)
    parts = dot(picker, jnp.concatenate([high, middle, low], axis=1))
    return parts[:, :LANES] + (parts[:, LANES : 2 * LANES] + parts[:, 2 * LANES :])


def marks_of(first, last, owner):
    docs = owner.shape[1]
    source = chunk_place()
    row = plane_row(owner) + 1
    part = iota((8, docs), 0)
    digits = jnp.where(part == 0, row >> 5, jnp.where(part == 1, row & 31, 0))
    lane = iota((docs, 2 * LANES), 1) - source * SLOTS
    doc = iota((docs, 2 * LANES), 0)
    meets = (doc == first + lane) & (doc <= last) & (lane >= 0) & (lane < USED)
    found = dot(small(digits), ones(meets))
    where = found[0:1, :] * 32.0 + found[1:2, :]
    line = iota((SLOTS, LANES), 0)
    second = jnp.where(line == SLOTS - 1, where[:, LANES:], 0.0)
    return jnp.where(line == SLOTS - 2, where[:, :LANES], second)


def most_rows(lengths, owner, tokens):
    docs = owner.shape[1]
    part = iota((8, docs), 0)
    digits = jnp.where(part == 0, lengths >> 7, jnp.where(part == 1, lengths & 127, 0))
    until = ones(iota((docs, docs), 0) <= iota((docs, docs), 1))
    sums = dot(small(digits), until)
    end = (sums[0:1, :] * 128.0 + sums[1:2, :]).astype(jnp.int32)
    start = end - lengths
    line = iota((LANES, docs), 0)
    device = (line >> 5) * 32 + (line & 15) * 2 + ((line >> 4) & 1)
    touches = (start < (device + 1) * tokens) & (end > device * tokens)
    owned = ((owner >> 3) & 15) == line
    counts = dot_rows(ones(touches), ones(owned))
    return jnp.max(jnp.sum(counts.reshape(8, 16, LANES), axis=0)).astype(jnp.int32)


def sums_kernel(
    pieces, seg_hbm, owner_hbm, hidden_hbm, out_ref, seg, owner, hidden, sems
):
    tokens = hidden.shape[0]
    rows = tokens // pieces
    copies = [
        pltpu.make_async_copy(seg_hbm, seg, sems.at[pieces]),
        pltpu.make_async_copy(owner_hbm, owner, sems.at[pieces + 1]),
    ]
    for p in range(pieces):
        here = pl.ds(p * rows, rows)
        copies.append(pltpu.make_async_copy(hidden_hbm.at[here], hidden.at[here], sems.at[p]))
    for copy in copies:
        copy.start()
    copies[0].wait()
    first = seg[0:1, 0:1]
    last = seg[0:1, tokens - 1 : tokens]
    copies[1].wait()
    marks = marks_of(first, last, owner[...])
    slot = iota((SLOTS, rows), 0) + first
    sums = None
    for p in range(pieces):
        picker = ones(slot == seg[:, p * rows : (p + 1) * rows])
        copies[2 + p].wait()
        term = dot(picker, hidden[p * rows : (p + 1) * rows, :])
        sums = term if sums is None else sums + term
    for c in range(out_ref.shape[0] // SLOTS):
        out_ref[c * SLOTS : (c + 1) * SLOTS, :] = sums[:, c * LANES : (c + 1) * LANES] + marks


def local_sums(seg_ids, owner_slot, hidden, chunks):
    tokens, width = hidden.shape
    docs = owner_slot.shape[0]
    pieces = 4
    return pl.pallas_call(
        functools.partial(sums_kernel, pieces),
        in_specs=[pl.BlockSpec(memory_space=pltpu.HBM)] * 3,
        out_specs=pl.BlockSpec(memory_space=pltpu.VMEM),
        out_shape=pltpu.VMEM((chunks * SLOTS, LANES), jnp.float32),
        scratch_shapes=[
            pltpu.VMEM((1, tokens), jnp.int32),
            pltpu.VMEM((1, docs), jnp.int32),
            pltpu.VMEM((tokens, width), hidden.dtype),
            pltpu.SemaphoreType.DMA((pieces + 2,)),
        ],
        compiler_params=pltpu.CompilerParams(vmem_limit_bytes=WIDE),
        name="local_sums",
    )(seg_ids.reshape(1, -1), owner_slot.reshape(1, -1), hidden)


def slots_of(in_ref):
    count = in_ref.shape[0]
    values = in_ref[...]
    empty = jnp.zeros((2 * LANES - count, LANES), jnp.float32)
    marks = in_ref[SLOTS - 2 : SLOTS, :]
    for row in range(2 * SLOTS, count + SLOTS, SLOTS):
        marks = marks + in_ref[row - 2 : row, :]
    marks = marks.astype(jnp.int32)
    where = jnp.concatenate([marks[0:1, :], marks[1:2, :]], axis=1)
    plane = jnp.where(where > 0, (where - 1) >> 5, -1)
    bound = iota((16, 2 * LANES), 0) == plane
    ahead = iota((2 * LANES, 2 * LANES), 0) < iota((2 * LANES, 2 * LANES), 1)
    seen = dot(ones(bound), ones(ahead))
    rank = jnp.sum(jnp.where(bound, seen, 0.0), axis=0, keepdims=True).astype(jnp.int32)
    return jnp.concatenate([values, empty], axis=0), where, plane, bound, rank


def place_kernel(in_ref, out_ref, ready_ref):
    planes = out_ref.shape[0] // ROWS
    ready_ref[...] = jnp.zeros_like(ready_ref)
    values, where, plane, bound, rank = slots_of(in_ref)
    target = jnp.where((where > 0) & (rank < FIT), plane * ROWS + rank, -1)
    out_ref[...] = picked(ones(iota((planes * ROWS, 2 * LANES), 0) == target), values)
    number = (((where - 1) & 31) + 1) * jnp.where((rank & 1) == 1, 64, 1)
    lane = iota((LANES, 2 * LANES), 0) - plane_place(lax.axis_index("z")) * PAIRS
    numbers = dot_rows(small(jnp.where(bound, number, 0)), ones((lane == rank >> 1) & (rank < FIT)))
    for p in range(planes):
        out_ref[p * ROWS + FIT : (p + 1) * ROWS, :] = numbers[p : p + 1, :]


def place(slots, planes):
    return pl.pallas_call(
        place_kernel,
        out_specs=[
            pl.BlockSpec(memory_space=pltpu.VMEM),
            pl.BlockSpec(memory_space=pltpu.VMEM),
        ],
        out_shape=[
            pltpu.VMEM((planes * ROWS, LANES), jnp.float32),
            pltpu.VMEM((8, LANES), jnp.int32),
        ],
        compiler_params=pltpu.CompilerParams(vmem_limit_bytes=GRANT),
        name="place",
    )(slots)


def crowded_kernel(tokens, ready_ref, owner_ref, length_ref, over_ref):
    most = most_rows(length_ref[...], owner_ref[...], tokens)
    over_ref[0] = (most + jnp.max(ready_ref[...]) > FIT).astype(jnp.int32)


def crowded(ready, owner_slot, lengths, tokens):
    docs = owner_slot.shape[0]
    return pl.pallas_call(
        functools.partial(crowded_kernel, tokens),
        out_specs=pl.BlockSpec(memory_space=pltpu.SMEM),
        out_shape=jax.ShapeDtypeStruct((1,), jnp.int32),
        cost_estimate=pl.CostEstimate(
            flops=64 * docs * docs, bytes_accessed=8 * docs, transcendentals=0
        ),
        compiler_params=pltpu.CompilerParams(vmem_limit_bytes=GRANT),
        name="crowded",
    )(ready, owner_slot.reshape(1, -1), lengths.reshape(1, -1))


def place_rest_kernel(in_ref, out_ref):
    planes, per_plane, _ = out_ref.shape
    values, where, _, _, rank = slots_of(in_ref)
    row = iota((planes * per_plane, 2 * LANES), 0) + 1
    out_ref[...] = picked(ones((row == where) & (rank >= FIT)), values).reshape(out_ref.shape)


def place_rest(slots, planes, per_plane):
    return pl.pallas_call(
        place_rest_kernel,
        out_shape=jax.ShapeDtypeStruct((planes, per_plane, LANES), jnp.float32),
        compiler_params=pltpu.CompilerParams(vmem_limit_bytes=GRANT),
        name="place_rest",
    )(slots)


def average_kernel(owner_ref, length_ref, bias_ref, in_ref, *rest_and_out):
    out_ref = rest_and_out[-1]
    count = in_ref.shape[0]
    planes = count // ROWS
    per_plane = owner_ref.shape[1] // planes
    marks = in_ref[FIT:ROWS, :]
    for p in range(1, planes):
        marks = marks + in_ref[p * ROWS + FIT : (p + 1) * ROWS, :]
    marks = marks.astype(jnp.int32)
    part = iota((8, LANES), 0)
    halves = jnp.where(part == 0, marks & 63, jnp.where(part == 1, marks >> 6, 0))
    line = iota((LANES, count), 1)
    source = (line * 171) >> 11
    spread = dot(small(halves), ones(iota((LANES, count), 0) == source * PAIRS + ((line - source * ROWS) >> 1)))
    line = line[0:1, :]
    line = line - ((line * 171) >> 11) * ROWS
    where = jnp.where((line & 1) == 1, spread[1:2, :], spread[0:1, :]).astype(jnp.int32)
    where = jnp.where(line < FIT, where, 0)
    picker = ones(iota((per_plane, count), 0) + 1 == where)
    total = picked(picker, in_ref[...])
    for rest_ref in rest_and_out[:-1]:
        total = total + jnp.sum(rest_ref[...], axis=0)
    mine = plane_place(lax.axis_index("z")) * per_plane
    row = iota((per_plane, owner_ref.shape[1]), 0) + mine
    length = jnp.sum(
        jnp.where(row == plane_row(owner_ref[...]), length_ref[...], 0).astype(jnp.float32),
        axis=1,
        keepdims=True,
    )
    chunk = chunk_place()
    average = total / length + bias_ref[pl.ds(chunk, 1), :]
    owners, copies, rows, _ = out_ref.shape
    for o in range(owners):
        for y in range(copies):
            out_ref[o ^ 1, y] = average[o * rows : (o + 1) * rows, :]


def averages_for_owners(arrived, owner_slot, lengths, pool_bias, owners, copies, *rest):
    rows = owner_slot.shape[0] // (arrived.shape[0] // ROWS * owners)
    return pl.pallas_call(
        average_kernel,
        out_shape=jax.ShapeDtypeStruct((owners, copies, rows, LANES), jnp.float32),
        compiler_params=pltpu.CompilerParams(vmem_limit_bytes=GRANT),
        name="average",
    )(owner_slot.reshape(1, -1), lengths.reshape(1, -1), pool_bias.reshape(-1, LANES), arrived, *rest)


def norm_kernel(in_ref, out_ref):
    chunks, slices, rows, _ = in_ref.shape
    every = in_ref[...]
    square = jnp.sum(every * every, axis=(0, 1))
    energy = jnp.sum(square, axis=1, keepdims=True) / (chunks * slices * LANES)
    scale = lax.rsqrt(energy + 1e-06)
    mine = slice_place()
    for c, device in enumerate(CHUNK_GROUP[0]):
        values = in_ref[device ^ 1, mine] * scale
        out_ref[:, c * LANES : (c + 1) * LANES] = values.astype(jnp.bfloat16)


def normed(arrived):
    chunks, _, rows, _ = arrived.shape
    return pl.pallas_call(
        norm_kernel,
        out_shape=jax.ShapeDtypeStruct((rows, chunks * LANES), jnp.bfloat16),
        compiler_params=pltpu.CompilerParams(vmem_limit_bytes=GRANT),
        name="norm",
    )(arrived)


def swap(array, axes, group):
    return lax.all_to_all(
        array, axes, split_axis=0, concat_axis=0, tiled=True, axis_index_groups=group
    )


def local(hidden, seg_ids, lengths, owner_slot, pool_bias):
    chunks = lax.axis_size(("x", "c"))
    planes = lax.axis_size("z")
    slices = lax.axis_size("y")
    per_plane = lengths.shape[0] // planes
    sums = local_sums(seg_ids, owner_slot, hidden, chunks)
    slots = swap(sums.reshape(-1, 4, LANES), ("x", "c"), CHUNK_GROUP).reshape(sums.shape)
    placed, ready = place(slots, planes)
    over = crowded(ready, owner_slot, lengths, hidden.shape[0])
    rows = swap(placed.reshape(-1, 4, LANES), "z", PLANE_GROUP).reshape(placed.shape)
    args = (owner_slot, lengths, pool_bias, chunks, slices)

    def with_rest(rows, kept):
        rest = swap(place_rest(kept, planes, per_plane), "z", PLANE_GROUP)
        return averages_for_owners(rows, *args, rest)

    def alone(rows, kept):
        return averages_for_owners(rows, *args)

    average = lax.cond(over[0] > 0, with_rest, alone, rows, slots)
    mine = swap(average.reshape(chunks * slices, -1, LANES), ("x", "c", "y"), OWNER_GROUP)
    return normed(mine.reshape(average.shape))


def solution(mesh):
    torus = Mesh(mesh.devices.reshape(4, 16, 2, mesh.shape["hid"]), ("x", "z", "c", "y"))
    seq = ("x", "z", "c")
    return jax.shard_map(
        local,
        mesh=torus,
        in_specs=(P(seq, "y"), P(seq), P(), P(), P("y")),
        out_specs=P(seq, "y"),
        check_vma=False,
    )
```

```python
import functools

import jax
import jax.numpy as jnp
from jax import lax
from jax.experimental import pallas as pl
from jax.experimental.pallas import tpu as pltpu
from jax.sharding import Mesh
from jax.sharding import PartitionSpec as P

USED = 17
SLOTS = 20
LANES = 128
FIT = 11
ROWS = 12
PAIRS = 8
GRANT = 16 * 1024 * 1024
WIDE = 56 * 1024 * 1024


def chunk_place():
    return (((lax.axis_index("x") + 2) & 3) * 2 + lax.axis_index("c")) ^ 1


def plane_place(z):
    return (z + 6 + lax.axis_index("c")) & 15


def slice_place():
    return (lax.axis_index("y") + 2) & 3


CHUNK_GROUP = [[(((j >> 1) + 2) & 3) * 2 + (j & 1) ^ 1 for j in range(8)]]
PLANE_GROUP = [[((j + 10 - c) & 15) * 2 + c for j in range(16)] for c in range(2)]
OWNER_GROUP = [[((j & ~3) ^ 4) + ((j + 2) & 3) for j in range(32)]]


def plane_row(owner):
    return ((owner >> 3) & 15) * 32 + (owner >> 7) * 8 + (owner & 7)


def ones(mask):
    return jnp.where(mask, 1.0, 0.0).astype(jnp.bfloat16)


def iota(shape, dim):
    return lax.broadcasted_iota(jnp.int32, shape, dim)


def small(array):
    return array.astype(jnp.float32).astype(jnp.bfloat16)


def dot(left, right):
    return jnp.dot(left, right, preferred_element_type=jnp.float32)


def dot_rows(left, right):
    return lax.dot_general(
        left, right, (((1,), (1,)), ((), ())), preferred_element_type=jnp.float32
    )


def picked(picker, values):
    high = values.astype(jnp.bfloat16)
    left_over = values - high.astype(jnp.float32)
    middle = left_over.astype(jnp.bfloat16)
    low = (left_over - middle.astype(jnp.float32)).astype(jnp.bfloat16)
    parts = dot(picker, jnp.concatenate([high, middle, low], axis=1))
    return parts[:, :LANES] + (parts[:, LANES : 2 * LANES] + parts[:, 2 * LANES :])


def marks_of(first, last, owner):
    docs = owner.shape[1]
    source = chunk_place()
    row = plane_row(owner) + 1
    part = iota((8, docs), 0)
    digits = jnp.where(part == 0, row >> 5, jnp.where(part == 1, row & 31, 0))
    lane = iota((docs, 2 * LANES), 1) - source * SLOTS
    doc = iota((docs, 2 * LANES), 0)
    meets = (doc == first + lane) & (doc <= last) & (lane >= 0) & (lane < USED)
    found = dot(small(digits), ones(meets))
    where = found[0:1, :] * 32.0 + found[1:2, :]
    line = iota((SLOTS, LANES), 0)
    second = jnp.where(line == SLOTS - 1, where[:, LANES:], 0.0)
    return jnp.where(line == SLOTS - 2, where[:, :LANES], second)


def most_rows(lengths, owner, tokens):
    docs = owner.shape[1]
    part = iota((8, docs), 0)
    digits = jnp.where(part == 0, lengths >> 7, jnp.where(part == 1, lengths & 127, 0))
    until = ones(iota((docs, docs), 0) <= iota((docs, docs), 1))
    sums = dot(small(digits), until)
    end = (sums[0:1, :] * 128.0 + sums[1:2, :]).astype(jnp.int32)
    start = end - lengths
    line = iota((LANES, docs), 0)
    device = (line >> 5) * 32 + (line & 15) * 2 + ((line >> 4) & 1)
    touches = (start < (device + 1) * tokens) & (end > device * tokens)
    owned = ((owner >> 3) & 15) == line
    counts = dot_rows(ones(touches), ones(owned))
    return jnp.max(jnp.sum(counts.reshape(8, 16, LANES), axis=0)).astype(jnp.int32)


def sums_kernel(
    pieces, seg_hbm, owner_hbm, hidden_hbm, out_ref, seg, owner, hidden, sems
):
    tokens = hidden.shape[0]
    rows = tokens // pieces
    copies = [
        pltpu.make_async_copy(seg_hbm, seg, sems.at[pieces]),
        pltpu.make_async_copy(owner_hbm, owner, sems.at[pieces + 1]),
    ]
    for p in range(pieces):
        here = pl.ds(p * rows, rows)
        copies.append(pltpu.make_async_copy(hidden_hbm.at[here], hidden.at[here], sems.at[p]))
    for copy in copies:
        copy.start()
    copies[0].wait()
    first = seg[0:1, 0:1]
    last = seg[0:1, tokens - 1 : tokens]
    copies[1].wait()
    marks = marks_of(first, last, owner[...])
    slot = iota((SLOTS, rows), 0) + first
    sums = None
    for p in range(pieces):
        picker = ones(slot == seg[:, p * rows : (p + 1) * rows])
        copies[2 + p].wait()
        term = dot(picker, hidden[p * rows : (p + 1) * rows, :])
        sums = term if sums is None else sums + term
    for c in range(out_ref.shape[0] // SLOTS):
        out_ref[c * SLOTS : (c + 1) * SLOTS, :] = sums[:, c * LANES : (c + 1) * LANES] + marks


def local_sums(seg_ids, owner_slot, hidden, chunks):
    tokens, width = hidden.shape
    docs = owner_slot.shape[0]
    pieces = 4
    return pl.pallas_call(
        functools.partial(sums_kernel, pieces),
        in_specs=[pl.BlockSpec(memory_space=pltpu.HBM)] * 3,
        out_specs=pl.BlockSpec(memory_space=pltpu.VMEM),
        out_shape=pltpu.VMEM((chunks * SLOTS, LANES), jnp.float32),
        scratch_shapes=[
            pltpu.VMEM((1, tokens), jnp.int32),
            pltpu.VMEM((1, docs), jnp.int32),
            pltpu.VMEM((tokens, width), hidden.dtype),
            pltpu.SemaphoreType.DMA((pieces + 2,)),
        ],
        compiler_params=pltpu.CompilerParams(vmem_limit_bytes=WIDE),
        name="local_sums",
    )(seg_ids.reshape(1, -1), owner_slot.reshape(1, -1), hidden)


def slots_of(in_ref):
    count = in_ref.shape[0]
    values = in_ref[...]
    empty = jnp.zeros((2 * LANES - count, LANES), jnp.float32)
    marks = in_ref[SLOTS - 2 : SLOTS, :]
    for row in range(2 * SLOTS, count + SLOTS, SLOTS):
        marks = marks + in_ref[row - 2 : row, :]
    marks = marks.astype(jnp.int32)
    where = jnp.concatenate([marks[0:1, :], marks[1:2, :]], axis=1)
    plane = jnp.where(where > 0, plane_place((where - 1) >> 5), -1)
    where = jnp.where(where > 0, plane * 32 + ((where - 1) & 31) + 1, 0)
    bound = iota((16, 2 * LANES), 0) == plane
    ahead = iota((2 * LANES, 2 * LANES), 0) < iota((2 * LANES, 2 * LANES), 1)
    seen = dot(ones(bound), ones(ahead))
    rank = jnp.sum(jnp.where(bound, seen, 0.0), axis=0, keepdims=True).astype(jnp.int32)
    return jnp.concatenate([values, empty], axis=0), where, plane, bound, rank


def place_kernel(in_ref, out_ref, ready_ref):
    planes = out_ref.shape[0] // ROWS
    ready_ref[...] = jnp.zeros_like(ready_ref)
    values, where, plane, bound, rank = slots_of(in_ref)
    target = jnp.where((where > 0) & (rank < FIT), plane * ROWS + rank, -1)
    out_ref[...] = picked(ones(iota((planes * ROWS, 2 * LANES), 0) == target), values)
    number = (((where - 1) & 31) + 1) * jnp.where((rank & 1) == 1, 64, 1)
    lane = iota((LANES, 2 * LANES), 0) - plane_place(lax.axis_index("z")) * PAIRS
    numbers = dot_rows(small(jnp.where(bound, number, 0)), ones((lane == rank >> 1) & (rank < FIT)))
    for p in range(planes):
        out_ref[p * ROWS + FIT : (p + 1) * ROWS, :] = numbers[p : p + 1, :]


def place(slots, planes):
    return pl.pallas_call(
        place_kernel,
        out_specs=[
            pl.BlockSpec(memory_space=pltpu.VMEM),
            pl.BlockSpec(memory_space=pltpu.VMEM),
        ],
        out_shape=[
            pltpu.VMEM((planes * ROWS, LANES), jnp.float32),
            pltpu.VMEM((8, LANES), jnp.int32),
        ],
        compiler_params=pltpu.CompilerParams(vmem_limit_bytes=GRANT),
        name="place",
    )(slots)


def crowded_kernel(tokens, ready_ref, owner_ref, length_ref, over_ref):
    most = most_rows(length_ref[...], owner_ref[...], tokens)
    over_ref[0] = (most + jnp.max(ready_ref[...]) > FIT).astype(jnp.int32)


def crowded(ready, owner_slot, lengths, tokens):
    docs = owner_slot.shape[0]
    return pl.pallas_call(
        functools.partial(crowded_kernel, tokens),
        out_specs=pl.BlockSpec(memory_space=pltpu.SMEM),
        out_shape=jax.ShapeDtypeStruct((1,), jnp.int32),
        cost_estimate=pl.CostEstimate(
            flops=64 * docs * docs, bytes_accessed=8 * docs, transcendentals=0
        ),
        compiler_params=pltpu.CompilerParams(vmem_limit_bytes=GRANT),
        name="crowded",
    )(ready, owner_slot.reshape(1, -1), lengths.reshape(1, -1))


def place_rest_kernel(in_ref, out_ref):
    planes, per_plane, _ = out_ref.shape
    values, where, _, _, rank = slots_of(in_ref)
    row = iota((planes * per_plane, 2 * LANES), 0) + 1
    out_ref[...] = picked(ones((row == where) & (rank >= FIT)), values).reshape(out_ref.shape)


def place_rest(slots, planes, per_plane):
    return pl.pallas_call(
        place_rest_kernel,
        out_shape=jax.ShapeDtypeStruct((planes, per_plane, LANES), jnp.float32),
        compiler_params=pltpu.CompilerParams(vmem_limit_bytes=GRANT),
        name="place_rest",
    )(slots)


def average_kernel(owner_ref, length_ref, bias_ref, in_ref, *rest_and_out):
    out_ref = rest_and_out[-1]
    count = in_ref.shape[0]
    planes = count // ROWS
    per_plane = owner_ref.shape[1] // planes
    marks = in_ref[FIT:ROWS, :]
    for p in range(1, planes):
        marks = marks + in_ref[p * ROWS + FIT : (p + 1) * ROWS, :]
    marks = marks.astype(jnp.int32)
    part = iota((8, LANES), 0)
    halves = jnp.where(part == 0, marks & 63, jnp.where(part == 1, marks >> 6, 0))
    line = iota((LANES, count), 1)
    source = (line * 171) >> 11
    spread = dot(small(halves), ones(iota((LANES, count), 0) == source * PAIRS + ((line - source * ROWS) >> 1)))
    line = line[0:1, :]
    line = line - ((line * 171) >> 11) * ROWS
    where = jnp.where((line & 1) == 1, spread[1:2, :], spread[0:1, :]).astype(jnp.int32)
    where = jnp.where(line < FIT, where, 0)
    picker = ones(iota((per_plane, count), 0) + 1 == where)
    total = picked(picker, in_ref[...])
    for rest_ref in rest_and_out[:-1]:
        total = total + jnp.sum(rest_ref[...], axis=0)
    mine = lax.axis_index("z") * per_plane
    row = iota((per_plane, owner_ref.shape[1]), 0) + mine
    length = jnp.sum(
        jnp.where(row == plane_row(owner_ref[...]), length_ref[...], 0).astype(jnp.float32),
        axis=1,
        keepdims=True,
    )
    chunk = chunk_place()
    average = total / length + bias_ref[pl.ds(chunk, 1), :]
    owners, copies, rows, _ = out_ref.shape
    for o in range(owners):
        for y in range(copies):
            out_ref[o ^ 1, y] = average[o * rows : (o + 1) * rows, :]


def averages_for_owners(arrived, owner_slot, lengths, pool_bias, owners, copies, *rest):
    rows = owner_slot.shape[0] // (arrived.shape[0] // ROWS * owners)
    return pl.pallas_call(
        average_kernel,
        out_shape=jax.ShapeDtypeStruct((owners, copies, rows, LANES), jnp.float32),
        compiler_params=pltpu.CompilerParams(vmem_limit_bytes=GRANT),
        name="average",
    )(owner_slot.reshape(1, -1), lengths.reshape(1, -1), pool_bias.reshape(-1, LANES), arrived, *rest)


def norm_kernel(in_ref, out_ref):
    chunks, slices, rows, _ = in_ref.shape
    every = in_ref[...]
    square = jnp.sum(every * every, axis=(0, 1))
    energy = jnp.sum(square, axis=1, keepdims=True) / (chunks * slices * LANES)
    scale = lax.rsqrt(energy + 1e-06)
    mine = slice_place()
    for c, device in enumerate(CHUNK_GROUP[0]):
        values = in_ref[device ^ 1, mine] * scale
        out_ref[:, c * LANES : (c + 1) * LANES] = values.astype(jnp.bfloat16)


def normed(arrived):
    chunks, _, rows, _ = arrived.shape
    return pl.pallas_call(
        norm_kernel,
        out_shape=jax.ShapeDtypeStruct((rows, chunks * LANES), jnp.bfloat16),
        compiler_params=pltpu.CompilerParams(vmem_limit_bytes=GRANT),
        name="norm",
    )(arrived)


def swap(array, axes, group):
    return lax.all_to_all(
        array, axes, split_axis=0, concat_axis=0, tiled=True, axis_index_groups=group
    )


def local(hidden, seg_ids, lengths, owner_slot, pool_bias):
    chunks = lax.axis_size(("x", "c"))
    planes = lax.axis_size("z")
    slices = lax.axis_size("y")
    per_plane = lengths.shape[0] // planes
    sums = local_sums(seg_ids, owner_slot, hidden, chunks)
    slots = swap(sums.reshape(-1, 4, LANES), ("x", "c"), CHUNK_GROUP).reshape(sums.shape)
    placed, ready = place(slots, planes)
    over = crowded(ready, owner_slot, lengths, hidden.shape[0])
    rows = swap(placed.reshape(-1, 4, LANES), ("z", "c"), PLANE_GROUP).reshape(placed.shape)
    args = (owner_slot, lengths, pool_bias, chunks, slices)

    def with_rest(rows, kept):
        rest = swap(place_rest(kept, planes, per_plane), ("z", "c"), PLANE_GROUP)
        return averages_for_owners(rows, *args, rest)

    def alone(rows, kept):
        return averages_for_owners(rows, *args)

    average = lax.cond(over[0] > 0, with_rest, alone, rows, slots)
    mine = swap(average.reshape(chunks * slices, -1, LANES), ("x", "c", "y"), OWNER_GROUP)
    return normed(mine.reshape(average.shape))


def solution(mesh):
    torus = Mesh(mesh.devices.reshape(4, 16, 2, mesh.shape["hid"]), ("x", "z", "c", "y"))
    seq = ("x", "z", "c")
    return jax.shard_map(
        local,
        mesh=torus,
        in_specs=(P(seq, "y"), P(seq), P(), P(), P("y")),
        out_specs=P(seq, "y"),
        check_vma=False,
    )
```

```python
import functools

import jax
import jax.numpy as jnp
from jax import lax
from jax.experimental import pallas as pl
from jax.experimental.pallas import tpu as pltpu
from jax.sharding import Mesh
from jax.sharding import PartitionSpec as P

USED = 17
SLOTS = 20
LANES = 128
FIT = 11
ROWS = 12
PAIRS = 8
GRANT = 16 * 1024 * 1024
WIDE = 56 * 1024 * 1024


def chunk_place():
    return (((lax.axis_index("x") + 2) & 3) * 2 + lax.axis_index("c")) ^ 1


def plane_place(z):
    return (z + 5 + lax.axis_index("c")) & 15


def slice_place():
    return (lax.axis_index("y") + 2) & 3


CHUNK_GROUP = [[(((j >> 1) + 2) & 3) * 2 + (j & 1) ^ 1 for j in range(8)]]
PLANE_GROUP = [[((j + 11 - c) & 15) * 2 + c for j in range(16)] for c in range(2)]
OWNER_GROUP = [[((j & ~3) ^ 4) + ((j + 2) & 3) for j in range(32)]]


def plane_row(owner):
    return ((owner >> 3) & 15) * 32 + (owner >> 7) * 8 + (owner & 7)


def ones(mask):
    return jnp.where(mask, 1.0, 0.0).astype(jnp.bfloat16)


def iota(shape, dim):
    return lax.broadcasted_iota(jnp.int32, shape, dim)


def small(array):
    return array.astype(jnp.float32).astype(jnp.bfloat16)


def dot(left, right):
    return jnp.dot(left, right, preferred_element_type=jnp.float32)


def dot_rows(left, right):
    return lax.dot_general(
        left, right, (((1,), (1,)), ((), ())), preferred_element_type=jnp.float32
    )


def picked(picker, values):
    high = values.astype(jnp.bfloat16)
    left_over = values - high.astype(jnp.float32)
    middle = left_over.astype(jnp.bfloat16)
    low = (left_over - middle.astype(jnp.float32)).astype(jnp.bfloat16)
    parts = dot(picker, jnp.concatenate([high, middle, low], axis=1))
    return parts[:, :LANES] + (parts[:, LANES : 2 * LANES] + parts[:, 2 * LANES :])


def marks_of(first, last, owner):
    docs = owner.shape[1]
    source = chunk_place()
    row = plane_row(owner) + 1
    part = iota((8, docs), 0)
    digits = jnp.where(part == 0, row >> 5, jnp.where(part == 1, row & 31, 0))
    lane = iota((docs, 2 * LANES), 1) - source * SLOTS
    doc = iota((docs, 2 * LANES), 0)
    meets = (doc == first + lane) & (doc <= last) & (lane >= 0) & (lane < USED)
    found = dot(small(digits), ones(meets))
    where = found[0:1, :] * 32.0 + found[1:2, :]
    line = iota((SLOTS, LANES), 0)
    second = jnp.where(line == SLOTS - 1, where[:, LANES:], 0.0)
    return jnp.where(line == SLOTS - 2, where[:, :LANES], second)


def most_rows(lengths, owner, tokens):
    docs = owner.shape[1]
    part = iota((8, docs), 0)
    digits = jnp.where(part == 0, lengths >> 7, jnp.where(part == 1, lengths & 127, 0))
    until = ones(iota((docs, docs), 0) <= iota((docs, docs), 1))
    sums = dot(small(digits), until)
    end = (sums[0:1, :] * 128.0 + sums[1:2, :]).astype(jnp.int32)
    start = end - lengths
    line = iota((LANES, docs), 0)
    device = (line >> 5) * 32 + (line & 15) * 2 + ((line >> 4) & 1)
    touches = (start < (device + 1) * tokens) & (end > device * tokens)
    owned = ((owner >> 3) & 15) == line
    counts = dot_rows(ones(touches), ones(owned))
    return jnp.max(jnp.sum(counts.reshape(8, 16, LANES), axis=0)).astype(jnp.int32)


def sums_kernel(
    pieces, seg_hbm, owner_hbm, hidden_hbm, out_ref, seg, owner, hidden, sems
):
    tokens = hidden.shape[0]
    rows = tokens // pieces
    copies = [
        pltpu.make_async_copy(seg_hbm, seg, sems.at[pieces]),
        pltpu.make_async_copy(owner_hbm, owner, sems.at[pieces + 1]),
    ]
    for p in range(pieces):
        here = pl.ds(p * rows, rows)
        copies.append(pltpu.make_async_copy(hidden_hbm.at[here], hidden.at[here], sems.at[p]))
    for copy in copies:
        copy.start()
    copies[0].wait()
    first = seg[0:1, 0:1]
    last = seg[0:1, tokens - 1 : tokens]
    copies[1].wait()
    marks = marks_of(first, last, owner[...])
    slot = iota((SLOTS, rows), 0) + first
    sums = None
    for p in range(pieces):
        picker = ones(slot == seg[:, p * rows : (p + 1) * rows])
        copies[2 + p].wait()
        term = dot(picker, hidden[p * rows : (p + 1) * rows, :])
        sums = term if sums is None else sums + term
    for c in range(out_ref.shape[0] // SLOTS):
        out_ref[c * SLOTS : (c + 1) * SLOTS, :] = sums[:, c * LANES : (c + 1) * LANES] + marks


def local_sums(seg_ids, owner_slot, hidden, chunks):
    tokens, width = hidden.shape
    docs = owner_slot.shape[0]
    pieces = 4
    return pl.pallas_call(
        functools.partial(sums_kernel, pieces),
        in_specs=[pl.BlockSpec(memory_space=pltpu.HBM)] * 3,
        out_specs=pl.BlockSpec(memory_space=pltpu.VMEM),
        out_shape=pltpu.VMEM((chunks * SLOTS, LANES), jnp.float32),
        scratch_shapes=[
            pltpu.VMEM((1, tokens), jnp.int32),
            pltpu.VMEM((1, docs), jnp.int32),
            pltpu.VMEM((tokens, width), hidden.dtype),
            pltpu.SemaphoreType.DMA((pieces + 2,)),
        ],
        compiler_params=pltpu.CompilerParams(vmem_limit_bytes=WIDE),
        name="local_sums",
    )(seg_ids.reshape(1, -1), owner_slot.reshape(1, -1), hidden)


def slots_of(in_ref):
    count = in_ref.shape[0]
    values = in_ref[...]
    empty = jnp.zeros((2 * LANES - count, LANES), jnp.float32)
    marks = in_ref[SLOTS - 2 : SLOTS, :]
    for row in range(2 * SLOTS, count + SLOTS, SLOTS):
        marks = marks + in_ref[row - 2 : row, :]
    marks = marks.astype(jnp.int32)
    where = jnp.concatenate([marks[0:1, :], marks[1:2, :]], axis=1)
    plane = jnp.where(where > 0, plane_place((where - 1) >> 5), -1)
    where = jnp.where(where > 0, plane * 32 + ((where - 1) & 31) + 1, 0)
    bound = iota((16, 2 * LANES), 0) == plane
    ahead = iota((2 * LANES, 2 * LANES), 0) < iota((2 * LANES, 2 * LANES), 1)
    seen = dot(ones(bound), ones(ahead))
    rank = jnp.sum(jnp.where(bound, seen, 0.0), axis=0, keepdims=True).astype(jnp.int32)
    return jnp.concatenate([values, empty], axis=0), where, plane, bound, rank


def place_kernel(in_ref, out_ref, ready_ref):
    planes = out_ref.shape[0] // ROWS
    ready_ref[...] = jnp.zeros_like(ready_ref)
    values, where, plane, bound, rank = slots_of(in_ref)
    target = jnp.where((where > 0) & (rank < FIT), plane * ROWS + rank, -1)
    out_ref[...] = picked(ones(iota((planes * ROWS, 2 * LANES), 0) == target), values)
    number = (((where - 1) & 31) + 1) * jnp.where((rank & 1) == 1, 64, 1)
    lane = iota((LANES, 2 * LANES), 0) - plane_place(lax.axis_index("z")) * PAIRS
    numbers = dot_rows(small(jnp.where(bound, number, 0)), ones((lane == rank >> 1) & (rank < FIT)))
    for p in range(planes):
        out_ref[p * ROWS + FIT : (p + 1) * ROWS, :] = numbers[p : p + 1, :]


def place(slots, planes):
    return pl.pallas_call(
        place_kernel,
        out_specs=[
            pl.BlockSpec(memory_space=pltpu.VMEM),
            pl.BlockSpec(memory_space=pltpu.VMEM),
        ],
        out_shape=[
            pltpu.VMEM((planes * ROWS, LANES), jnp.float32),
            pltpu.VMEM((8, LANES), jnp.int32),
        ],
        compiler_params=pltpu.CompilerParams(vmem_limit_bytes=GRANT),
        name="place",
    )(slots)


def crowded_kernel(tokens, ready_ref, owner_ref, length_ref, over_ref):
    most = most_rows(length_ref[...], owner_ref[...], tokens)
    over_ref[0] = (most + jnp.max(ready_ref[...]) > FIT).astype(jnp.int32)


def crowded(ready, owner_slot, lengths, tokens):
    docs = owner_slot.shape[0]
    return pl.pallas_call(
        functools.partial(crowded_kernel, tokens),
        out_specs=pl.BlockSpec(memory_space=pltpu.SMEM),
        out_shape=jax.ShapeDtypeStruct((1,), jnp.int32),
        cost_estimate=pl.CostEstimate(
            flops=64 * docs * docs, bytes_accessed=8 * docs, transcendentals=0
        ),
        compiler_params=pltpu.CompilerParams(vmem_limit_bytes=GRANT),
        name="crowded",
    )(ready, owner_slot.reshape(1, -1), lengths.reshape(1, -1))


def place_rest_kernel(in_ref, out_ref):
    planes, per_plane, _ = out_ref.shape
    values, where, _, _, rank = slots_of(in_ref)
    row = iota((planes * per_plane, 2 * LANES), 0) + 1
    out_ref[...] = picked(ones((row == where) & (rank >= FIT)), values).reshape(out_ref.shape)


def place_rest(slots, planes, per_plane):
    return pl.pallas_call(
        place_rest_kernel,
        out_shape=jax.ShapeDtypeStruct((planes, per_plane, LANES), jnp.float32),
        compiler_params=pltpu.CompilerParams(vmem_limit_bytes=GRANT),
        name="place_rest",
    )(slots)


def average_kernel(owner_ref, length_ref, bias_ref, in_ref, *rest_and_out):
    out_ref = rest_and_out[-1]
    count = in_ref.shape[0]
    planes = count // ROWS
    per_plane = owner_ref.shape[1] // planes
    marks = in_ref[FIT:ROWS, :]
    for p in range(1, planes):
        marks = marks + in_ref[p * ROWS + FIT : (p + 1) * ROWS, :]
    marks = marks.astype(jnp.int32)
    part = iota((8, LANES), 0)
    halves = jnp.where(part == 0, marks & 63, jnp.where(part == 1, marks >> 6, 0))
    line = iota((LANES, count), 1)
    source = (line * 171) >> 11
    spread = dot(small(halves), ones(iota((LANES, count), 0) == source * PAIRS + ((line - source * ROWS) >> 1)))
    line = line[0:1, :]
    line = line - ((line * 171) >> 11) * ROWS
    where = jnp.where((line & 1) == 1, spread[1:2, :], spread[0:1, :]).astype(jnp.int32)
    where = jnp.where(line < FIT, where, 0)
    picker = ones(iota((per_plane, count), 0) + 1 == where)
    total = picked(picker, in_ref[...])
    for rest_ref in rest_and_out[:-1]:
        total = total + jnp.sum(rest_ref[...], axis=0)
    mine = lax.axis_index("z") * per_plane
    row = iota((per_plane, owner_ref.shape[1]), 0) + mine
    length = jnp.sum(
        jnp.where(row == plane_row(owner_ref[...]), length_ref[...], 0).astype(jnp.float32),
        axis=1,
        keepdims=True,
    )
    chunk = chunk_place()
    average = total / length + bias_ref[pl.ds(chunk, 1), :]
    owners, copies, rows, _ = out_ref.shape
    for o in range(owners):
        for y in range(copies):
            out_ref[o ^ 1, y] = average[o * rows : (o + 1) * rows, :]


def averages_for_owners(arrived, owner_slot, lengths, pool_bias, owners, copies, *rest):
    rows = owner_slot.shape[0] // (arrived.shape[0] // ROWS * owners)
    return pl.pallas_call(
        average_kernel,
        out_shape=jax.ShapeDtypeStruct((owners, copies, rows, LANES), jnp.float32),
        compiler_params=pltpu.CompilerParams(vmem_limit_bytes=GRANT),
        name="average",
    )(owner_slot.reshape(1, -1), lengths.reshape(1, -1), pool_bias.reshape(-1, LANES), arrived, *rest)


def norm_kernel(in_ref, out_ref):
    chunks, slices, rows, _ = in_ref.shape
    every = in_ref[...]
    square = jnp.sum(every * every, axis=(0, 1))
    energy = jnp.sum(square, axis=1, keepdims=True) / (chunks * slices * LANES)
    scale = lax.rsqrt(energy + 1e-06)
    mine = slice_place()
    for c, device in enumerate(CHUNK_GROUP[0]):
        values = in_ref[device ^ 1, mine] * scale
        out_ref[:, c * LANES : (c + 1) * LANES] = values.astype(jnp.bfloat16)


def normed(arrived):
    chunks, _, rows, _ = arrived.shape
    return pl.pallas_call(
        norm_kernel,
        out_shape=jax.ShapeDtypeStruct((rows, chunks * LANES), jnp.bfloat16),
        compiler_params=pltpu.CompilerParams(vmem_limit_bytes=GRANT),
        name="norm",
    )(arrived)


def swap(array, axes, group):
    return lax.all_to_all(
        array, axes, split_axis=0, concat_axis=0, tiled=True, axis_index_groups=group
    )


def local(hidden, seg_ids, lengths, owner_slot, pool_bias):
    chunks = lax.axis_size(("x", "c"))
    planes = lax.axis_size("z")
    slices = lax.axis_size("y")
    per_plane = lengths.shape[0] // planes
    sums = local_sums(seg_ids, owner_slot, hidden, chunks)
    slots = swap(sums.reshape(-1, 4, LANES), ("x", "c"), CHUNK_GROUP).reshape(sums.shape)
    placed, ready = place(slots, planes)
    over = crowded(ready, owner_slot, lengths, hidden.shape[0])
    rows = swap(placed.reshape(-1, 4, LANES), ("z", "c"), PLANE_GROUP).reshape(placed.shape)
    args = (owner_slot, lengths, pool_bias, chunks, slices)

    def with_rest(rows, kept):
        rest = swap(place_rest(kept, planes, per_plane), ("z", "c"), PLANE_GROUP)
        return averages_for_owners(rows, *args, rest)

    def alone(rows, kept):
        return averages_for_owners(rows, *args)

    average = lax.cond(over[0] > 0, with_rest, alone, rows, slots)
    mine = swap(average.reshape(chunks * slices, -1, LANES), ("x", "c", "y"), OWNER_GROUP)
    return normed(mine.reshape(average.shape))


def solution(mesh):
    torus = Mesh(mesh.devices.reshape(4, 16, 2, mesh.shape["hid"]), ("x", "z", "c", "y"))
    seq = ("x", "z", "c")
    return jax.shard_map(
        local,
        mesh=torus,
        in_specs=(P(seq, "y"), P(seq), P(), P(), P("y")),
        out_specs=P(seq, "y"),
        check_vma=False,
    )
```

```python
import functools

import jax
import jax.numpy as jnp
from jax import lax
from jax.experimental import pallas as pl
from jax.experimental.pallas import tpu as pltpu
from jax.sharding import Mesh
from jax.sharding import PartitionSpec as P

USED = 17
SLOTS = 20
LANES = 128
FIT = 11
ROWS = 12
PAIRS = 8
GRANT = 16 * 1024 * 1024
WIDE = 56 * 1024 * 1024


def chunk_place():
    return (((lax.axis_index("x") + 2) & 3) * 2 + lax.axis_index("c")) ^ 1


def plane_place(z):
    return (z + 6) & 15


def slice_place():
    return (lax.axis_index("y") + 2) & 3


CHUNK_GROUP = [[(((j >> 1) + 2) & 3) * 2 + (j & 1) ^ 1 for j in range(8)]]
PLANE_GROUP = [[(j + 10) & 15 for j in range(16)]]
OWNER_GROUP = [[((j & ~3) ^ 4) + ((j + 2) & 3) for j in range(32)]]


def plane_row(owner):
    return plane_place(owner >> 3) * 32 + (owner >> 7) * 8 + (owner & 7)


def ones(mask):
    return jnp.where(mask, 1.0, 0.0).astype(jnp.bfloat16)


def iota(shape, dim):
    return lax.broadcasted_iota(jnp.int32, shape, dim)


def small(array):
    return array.astype(jnp.float32).astype(jnp.bfloat16)


def dot(left, right):
    return jnp.dot(left, right, preferred_element_type=jnp.float32)


def dot_rows(left, right):
    return lax.dot_general(
        left, right, (((1,), (1,)), ((), ())), preferred_element_type=jnp.float32
    )


def picked(picker, values):
    high = values.astype(jnp.bfloat16)
    left_over = values - high.astype(jnp.float32)
    middle = left_over.astype(jnp.bfloat16)
    low = (left_over - middle.astype(jnp.float32)).astype(jnp.bfloat16)
    parts = dot(picker, jnp.concatenate([high, middle, low], axis=1))
    return parts[:, :LANES] + (parts[:, LANES : 2 * LANES] + parts[:, 2 * LANES :])


def marks_of(first, last, owner):
    docs = owner.shape[1]
    source = chunk_place()
    row = plane_row(owner) + 1
    part = iota((8, docs), 0)
    digits = jnp.where(part == 0, row >> 5, jnp.where(part == 1, row & 31, 0))
    lane = iota((docs, 2 * LANES), 1) - source * SLOTS
    doc = iota((docs, 2 * LANES), 0)
    meets = (doc == first + lane) & (doc <= last) & (lane >= 0) & (lane < USED)
    found = dot(small(digits), ones(meets))
    where = found[0:1, :] * 32.0 + found[1:2, :]
    line = iota((SLOTS, LANES), 0)
    second = jnp.where(line == SLOTS - 1, where[:, LANES:], 0.0)
    return jnp.where(line == SLOTS - 2, where[:, :LANES], second)


def most_rows(lengths, owner, tokens):
    docs = owner.shape[1]
    part = iota((8, docs), 0)
    digits = jnp.where(part == 0, lengths >> 7, jnp.where(part == 1, lengths & 127, 0))
    until = ones(iota((docs, docs), 0) <= iota((docs, docs), 1))
    sums = dot(small(digits), until)
    end = (sums[0:1, :] * 128.0 + sums[1:2, :]).astype(jnp.int32)
    start = end - lengths
    line = iota((LANES, docs), 0)
    device = (line >> 5) * 32 + (line & 15) * 2 + ((line >> 4) & 1)
    touches = (start < (device + 1) * tokens) & (end > device * tokens)
    owned = ((owner >> 3) & 15) == line
    counts = dot_rows(ones(touches), ones(owned))
    return jnp.max(jnp.sum(counts.reshape(8, 16, LANES), axis=0)).astype(jnp.int32)


def sums_kernel(
    pieces, seg_hbm, owner_hbm, hidden_hbm, out_ref, seg, owner, hidden, sems
):
    tokens = hidden.shape[0]
    rows = tokens // pieces
    copies = [
        pltpu.make_async_copy(seg_hbm, seg, sems.at[pieces]),
        pltpu.make_async_copy(owner_hbm, owner, sems.at[pieces + 1]),
    ]
    for p in range(pieces):
        here = pl.ds(p * rows, rows)
        copies.append(pltpu.make_async_copy(hidden_hbm.at[here], hidden.at[here], sems.at[p]))
    for copy in copies:
        copy.start()
    copies[0].wait()
    first = seg[0:1, 0:1]
    last = seg[0:1, tokens - 1 : tokens]
    copies[1].wait()
    marks = marks_of(first, last, owner[...])
    slot = iota((SLOTS, rows), 0) + first
    sums = None
    for p in range(pieces):
        picker = ones(slot == seg[:, p * rows : (p + 1) * rows])
        copies[2 + p].wait()
        term = dot(picker, hidden[p * rows : (p + 1) * rows, :])
        sums = term if sums is None else sums + term
    for c in range(out_ref.shape[0] // SLOTS):
        out_ref[c * SLOTS : (c + 1) * SLOTS, :] = sums[:, c * LANES : (c + 1) * LANES] + marks


def local_sums(seg_ids, owner_slot, hidden, chunks):
    tokens, width = hidden.shape
    docs = owner_slot.shape[0]
    pieces = 4
    return pl.pallas_call(
        functools.partial(sums_kernel, pieces),
        in_specs=[pl.BlockSpec(memory_space=pltpu.HBM)] * 3,
        out_specs=pl.BlockSpec(memory_space=pltpu.VMEM),
        out_shape=pltpu.VMEM((chunks * SLOTS, LANES), jnp.float32),
        scratch_shapes=[
            pltpu.VMEM((1, tokens), jnp.int32),
            pltpu.VMEM((1, docs), jnp.int32),
            pltpu.VMEM((tokens, width), hidden.dtype),
            pltpu.SemaphoreType.DMA((pieces + 2,)),
        ],
        compiler_params=pltpu.CompilerParams(vmem_limit_bytes=WIDE),
        name="local_sums",
    )(seg_ids.reshape(1, -1), owner_slot.reshape(1, -1), hidden)


def slots_of(in_ref):
    count = in_ref.shape[0]
    marks = in_ref[SLOTS - 2 : SLOTS, :]
    for row in range(2 * SLOTS, count + SLOTS, SLOTS):
        marks = marks + in_ref[row - 2 : row, :]
    marks = marks.astype(jnp.int32)
    where = jnp.concatenate([marks[0:1, :], marks[1:2, : count - LANES]], axis=1)
    plane = jnp.where(where > 0, (where - 1) >> 5, -1)
    bound = iota((16, count), 0) == plane
    ahead = iota((count, count), 0) < iota((count, count), 1)
    seen = dot(ones(bound), ones(ahead))
    rank = jnp.sum(jnp.where(bound, seen, 0.0), axis=0, keepdims=True).astype(jnp.int32)
    return in_ref[...], where, plane, bound, rank


def place_kernel(in_ref, out_ref, ready_ref):
    planes = out_ref.shape[0] // ROWS
    ready_ref[...] = jnp.zeros_like(ready_ref)
    values, where, plane, bound, rank = slots_of(in_ref)
    target = jnp.where((where > 0) & (rank < FIT), plane * ROWS + rank, -1)
    out_ref[...] = picked(ones(iota((planes * ROWS, where.shape[1]), 0) == target), values)
    number = (((where - 1) & 31) + 1) * jnp.where((rank & 1) == 1, 64, 1)
    lane = iota((LANES, where.shape[1]), 0) - plane_place(lax.axis_index("z")) * PAIRS
    numbers = dot_rows(small(jnp.where(bound, number, 0)), ones((lane == rank >> 1) & (rank < FIT)))
    for p in range(planes):
        out_ref[p * ROWS + FIT : (p + 1) * ROWS, :] = numbers[p : p + 1, :]


def place(slots, planes):
    return pl.pallas_call(
        place_kernel,
        out_specs=[
            pl.BlockSpec(memory_space=pltpu.VMEM),
            pl.BlockSpec(memory_space=pltpu.VMEM),
        ],
        out_shape=[
            pltpu.VMEM((planes * ROWS, LANES), jnp.float32),
            pltpu.VMEM((8, LANES), jnp.int32),
        ],
        compiler_params=pltpu.CompilerParams(vmem_limit_bytes=GRANT),
        name="place",
    )(slots)


def crowded_kernel(tokens, ready_ref, owner_ref, length_ref, over_ref):
    most = most_rows(length_ref[...], owner_ref[...], tokens)
    over_ref[0] = (most + jnp.max(ready_ref[...]) > FIT).astype(jnp.int32)


def crowded(ready, owner_slot, lengths, tokens):
    docs = owner_slot.shape[0]
    return pl.pallas_call(
        functools.partial(crowded_kernel, tokens),
        out_specs=pl.BlockSpec(memory_space=pltpu.SMEM),
        out_shape=jax.ShapeDtypeStruct((1,), jnp.int32),
        cost_estimate=pl.CostEstimate(
            flops=64 * docs * docs, bytes_accessed=8 * docs, transcendentals=0
        ),
        compiler_params=pltpu.CompilerParams(vmem_limit_bytes=GRANT),
        name="crowded",
    )(ready, owner_slot.reshape(1, -1), lengths.reshape(1, -1))


def place_rest_kernel(in_ref, out_ref):
    planes, per_plane, _ = out_ref.shape
    values, where, _, _, rank = slots_of(in_ref)
    row = iota((planes * per_plane, where.shape[1]), 0) + 1
    out_ref[...] = picked(ones((row == where) & (rank >= FIT)), values).reshape(out_ref.shape)


def place_rest(slots, planes, per_plane):
    return pl.pallas_call(
        place_rest_kernel,
        out_shape=jax.ShapeDtypeStruct((planes, per_plane, LANES), jnp.float32),
        compiler_params=pltpu.CompilerParams(vmem_limit_bytes=GRANT),
        name="place_rest",
    )(slots)


def average_kernel(owner_ref, length_ref, bias_ref, in_ref, *rest_and_out):
    out_ref = rest_and_out[-1]
    count = in_ref.shape[0]
    planes = count // ROWS
    per_plane = owner_ref.shape[1] // planes
    marks = in_ref[FIT:ROWS, :]
    for p in range(1, planes):
        marks = marks + in_ref[p * ROWS + FIT : (p + 1) * ROWS, :]
    marks = marks.astype(jnp.int32)
    part = iota((8, LANES), 0)
    halves = jnp.where(part == 0, marks & 63, jnp.where(part == 1, marks >> 6, 0))
    line = iota((LANES, count), 1)
    source = (line * 171) >> 11
    spread = dot(small(halves), ones(iota((LANES, count), 0) == source * PAIRS + ((line - source * ROWS) >> 1)))
    line = line[0:1, :]
    line = line - ((line * 171) >> 11) * ROWS
    where = jnp.where((line & 1) == 1, spread[1:2, :], spread[0:1, :]).astype(jnp.int32)
    where = jnp.where(line < FIT, where, 0)
    picker = ones(iota((per_plane, count), 0) + 1 == where)
    total = picked(picker, in_ref[...])
    for rest_ref in rest_and_out[:-1]:
        total = total + jnp.sum(rest_ref[...], axis=0)
    mine = plane_place(lax.axis_index("z")) * per_plane
    row = iota((per_plane, owner_ref.shape[1]), 0) + mine
    length = jnp.sum(
        jnp.where(row == plane_row(owner_ref[...]), length_ref[...], 0).astype(jnp.float32),
        axis=1,
        keepdims=True,
    )
    chunk = chunk_place()
    average = total / length + bias_ref[pl.ds(chunk, 1), :]
    owners, copies, rows, _ = out_ref.shape
    for o in range(owners):
        for y in range(copies):
            out_ref[o ^ 1, y] = average[o * rows : (o + 1) * rows, :]


def averages_for_owners(arrived, owner_slot, lengths, pool_bias, owners, copies, *rest):
    rows = owner_slot.shape[0] // (arrived.shape[0] // ROWS * owners)
    return pl.pallas_call(
        average_kernel,
        out_shape=jax.ShapeDtypeStruct((owners, copies, rows, LANES), jnp.float32),
        compiler_params=pltpu.CompilerParams(vmem_limit_bytes=GRANT),
        name="average",
    )(owner_slot.reshape(1, -1), lengths.reshape(1, -1), pool_bias.reshape(-1, LANES), arrived, *rest)


def norm_kernel(in_ref, out_ref):
    chunks, slices, rows, _ = in_ref.shape
    every = in_ref[...]
    square = jnp.sum(every * every, axis=(0, 1))
    energy = jnp.sum(square, axis=1, keepdims=True) / (chunks * slices * LANES)
    scale = lax.rsqrt(energy + 1e-06)
    mine = slice_place()
    for c, device in enumerate(CHUNK_GROUP[0]):
        values = in_ref[device ^ 1, mine] * scale
        out_ref[:, c * LANES : (c + 1) * LANES] = values.astype(jnp.bfloat16)


def normed(arrived):
    chunks, _, rows, _ = arrived.shape
    return pl.pallas_call(
        norm_kernel,
        out_shape=jax.ShapeDtypeStruct((rows, chunks * LANES), jnp.bfloat16),
        compiler_params=pltpu.CompilerParams(vmem_limit_bytes=GRANT),
        name="norm",
    )(arrived)


def swap(array, axes, group):
    return lax.all_to_all(
        array, axes, split_axis=0, concat_axis=0, tiled=True, axis_index_groups=group
    )


def local(hidden, seg_ids, lengths, owner_slot, pool_bias):
    chunks = lax.axis_size(("x", "c"))
    planes = lax.axis_size("z")
    slices = lax.axis_size("y")
    per_plane = lengths.shape[0] // planes
    sums = local_sums(seg_ids, owner_slot, hidden, chunks)
    slots = swap(sums.reshape(-1, 4, LANES), ("x", "c"), CHUNK_GROUP).reshape(sums.shape)
    placed, ready = place(slots, planes)
    over = crowded(ready, owner_slot, lengths, hidden.shape[0])
    rows = swap(placed.reshape(-1, 4, LANES), "z", PLANE_GROUP).reshape(placed.shape)
    args = (owner_slot, lengths, pool_bias, chunks, slices)

    def with_rest(rows, kept):
        rest = swap(place_rest(kept, planes, per_plane), "z", PLANE_GROUP)
        return averages_for_owners(rows, *args, rest)

    def alone(rows, kept):
        return averages_for_owners(rows, *args)

    average = lax.cond(over[0] > 0, with_rest, alone, rows, slots)
    mine = swap(average.reshape(chunks * slices, -1, LANES), ("x", "c", "y"), OWNER_GROUP)
    return normed(mine.reshape(average.shape))


def solution(mesh):
    torus = Mesh(mesh.devices.reshape(4, 16, 2, mesh.shape["hid"]), ("x", "z", "c", "y"))
    seq = ("x", "z", "c")
    return jax.shard_map(
        local,
        mesh=torus,
        in_specs=(P(seq, "y"), P(seq), P(), P(), P("y")),
        out_specs=P(seq, "y"),
        check_vma=False,
    )
```

```python
import functools

import jax
import jax.numpy as jnp
from jax import lax
from jax.experimental import pallas as pl
from jax.experimental.pallas import tpu as pltpu
from jax.sharding import Mesh
from jax.sharding import PartitionSpec as P

USED = 17
SLOTS = 20
LANES = 128
FIT = 11
ROWS = 12
PAIRS = 8
GRANT = 16 * 1024 * 1024
WIDE = 56 * 1024 * 1024


def chunk_place():
    return (((lax.axis_index("x") + 2) & 3) * 2 + lax.axis_index("c")) ^ 1


def plane_place(z):
    return (z + 6) & 15


def slice_place():
    return (lax.axis_index("y") + 2) & 3


CHUNK_GROUP = [[(((j >> 1) + 2) & 3) * 2 + (j & 1) ^ 1 for j in range(8)]]
PLANE_GROUP = [[(j + 10) & 15 for j in range(16)]]
OWNER_GROUP = [[(j & ~3) + ((j + 2) & 3) for j in range(32)]]


def plane_row(owner):
    return plane_place(owner >> 3) * 32 + (owner >> 7) * 8 + (owner & 7)


def ones(mask):
    return jnp.where(mask, 1.0, 0.0).astype(jnp.bfloat16)


def iota(shape, dim):
    return lax.broadcasted_iota(jnp.int32, shape, dim)


def small(array):
    return array.astype(jnp.float32).astype(jnp.bfloat16)


def dot(left, right):
    return jnp.dot(left, right, preferred_element_type=jnp.float32)


def dot_rows(left, right):
    return lax.dot_general(
        left, right, (((1,), (1,)), ((), ())), preferred_element_type=jnp.float32
    )


def picked(picker, values):
    high = values.astype(jnp.bfloat16)
    left_over = values - high.astype(jnp.float32)
    middle = left_over.astype(jnp.bfloat16)
    low = (left_over - middle.astype(jnp.float32)).astype(jnp.bfloat16)
    parts = dot(picker, jnp.concatenate([high, middle, low], axis=1))
    return parts[:, :LANES] + (parts[:, LANES : 2 * LANES] + parts[:, 2 * LANES :])


def marks_of(first, last, owner):
    docs = owner.shape[1]
    source = chunk_place()
    row = plane_row(owner) + 1
    part = iota((8, docs), 0)
    digits = jnp.where(part == 0, row >> 5, jnp.where(part == 1, row & 31, 0))
    lane = iota((docs, 2 * LANES), 1) - source * SLOTS
    doc = iota((docs, 2 * LANES), 0)
    meets = (doc == first + lane) & (doc <= last) & (lane >= 0) & (lane < USED)
    found = dot(small(digits), ones(meets))
    where = found[0:1, :] * 32.0 + found[1:2, :]
    line = iota((SLOTS, LANES), 0)
    second = jnp.where(line == SLOTS - 1, where[:, LANES:], 0.0)
    return jnp.where(line == SLOTS - 2, where[:, :LANES], second)


def most_rows(lengths, owner, tokens):
    docs = owner.shape[1]
    part = iota((8, docs), 0)
    digits = jnp.where(part == 0, lengths >> 7, jnp.where(part == 1, lengths & 127, 0))
    until = ones(iota((docs, docs), 0) <= iota((docs, docs), 1))
    sums = dot(small(digits), until)
    end = (sums[0:1, :] * 128.0 + sums[1:2, :]).astype(jnp.int32)
    start = end - lengths
    line = iota((LANES, docs), 0)
    device = (line >> 5) * 32 + (line & 15) * 2 + ((line >> 4) & 1)
    touches = (start < (device + 1) * tokens) & (end > device * tokens)
    owned = ((owner >> 3) & 15) == line
    counts = dot_rows(ones(touches), ones(owned))
    return jnp.max(jnp.sum(counts.reshape(8, 16, LANES), axis=0)).astype(jnp.int32)


def sums_kernel(
    pieces, seg_hbm, owner_hbm, hidden_hbm, out_ref, seg, owner, hidden, sems
):
    tokens = hidden.shape[0]
    rows = tokens // pieces
    copies = [
        pltpu.make_async_copy(seg_hbm, seg, sems.at[pieces]),
        pltpu.make_async_copy(owner_hbm, owner, sems.at[pieces + 1]),
    ]
    for p in range(pieces):
        here = pl.ds(p * rows, rows)
        copies.append(pltpu.make_async_copy(hidden_hbm.at[here], hidden.at[here], sems.at[p]))
    for copy in copies:
        copy.start()
    copies[0].wait()
    first = seg[0:1, 0:1]
    last = seg[0:1, tokens - 1 : tokens]
    copies[1].wait()
    marks = marks_of(first, last, owner[...])
    slot = iota((SLOTS, rows), 0) + first
    sums = None
    for p in range(pieces):
        picker = ones(slot == seg[:, p * rows : (p + 1) * rows])
        copies[2 + p].wait()
        term = dot(picker, hidden[p * rows : (p + 1) * rows, :])
        sums = term if sums is None else sums + term
    for c in range(out_ref.shape[0] // SLOTS):
        out_ref[c * SLOTS : (c + 1) * SLOTS, :] = sums[:, c * LANES : (c + 1) * LANES] + marks


def local_sums(seg_ids, owner_slot, hidden, chunks):
    tokens, width = hidden.shape
    docs = owner_slot.shape[0]
    pieces = 4
    return pl.pallas_call(
        functools.partial(sums_kernel, pieces),
        in_specs=[pl.BlockSpec(memory_space=pltpu.HBM)] * 3,
        out_specs=pl.BlockSpec(memory_space=pltpu.VMEM),
        out_shape=pltpu.VMEM((chunks * SLOTS, LANES), jnp.float32),
        scratch_shapes=[
            pltpu.VMEM((1, tokens), jnp.int32),
            pltpu.VMEM((1, docs), jnp.int32),
            pltpu.VMEM((tokens, width), hidden.dtype),
            pltpu.SemaphoreType.DMA((pieces + 2,)),
        ],
        compiler_params=pltpu.CompilerParams(vmem_limit_bytes=WIDE),
        name="local_sums",
    )(seg_ids.reshape(1, -1), owner_slot.reshape(1, -1), hidden)


def slots_of(in_ref):
    count = in_ref.shape[0]
    marks = in_ref[SLOTS - 2 : SLOTS, :]
    for row in range(2 * SLOTS, count + SLOTS, SLOTS):
        marks = marks + in_ref[row - 2 : row, :]
    marks = marks.astype(jnp.int32)
    where = jnp.concatenate([marks[0:1, :], marks[1:2, : count - LANES]], axis=1)
    plane = jnp.where(where > 0, (where - 1) >> 5, -1)
    bound = iota((16, count), 0) == plane
    ahead = iota((count, count), 0) < iota((count, count), 1)
    seen = dot(ones(bound), ones(ahead))
    rank = jnp.sum(jnp.where(bound, seen, 0.0), axis=0, keepdims=True).astype(jnp.int32)
    return in_ref[...], where, plane, bound, rank


def place_kernel(in_ref, out_ref, ready_ref):
    planes = out_ref.shape[0] // ROWS
    ready_ref[...] = jnp.zeros_like(ready_ref)
    values, where, plane, bound, rank = slots_of(in_ref)
    target = jnp.where((where > 0) & (rank < FIT), plane * ROWS + rank, -1)
    out_ref[...] = picked(ones(iota((planes * ROWS, where.shape[1]), 0) == target), values)
    number = (((where - 1) & 31) + 1) * jnp.where((rank & 1) == 1, 64, 1)
    lane = iota((LANES, where.shape[1]), 0) - plane_place(lax.axis_index("z")) * PAIRS
    numbers = dot_rows(small(jnp.where(bound, number, 0)), ones((lane == rank >> 1) & (rank < FIT)))
    for p in range(planes):
        out_ref[p * ROWS + FIT : (p + 1) * ROWS, :] = numbers[p : p + 1, :]


def place(slots, planes):
    return pl.pallas_call(
        place_kernel,
        out_specs=[
            pl.BlockSpec(memory_space=pltpu.VMEM),
            pl.BlockSpec(memory_space=pltpu.VMEM),
        ],
        out_shape=[
            pltpu.VMEM((planes * ROWS, LANES), jnp.float32),
            pltpu.VMEM((8, LANES), jnp.int32),
        ],
        compiler_params=pltpu.CompilerParams(vmem_limit_bytes=GRANT),
        name="place",
    )(slots)


def crowded_kernel(tokens, ready_ref, owner_ref, length_ref, over_ref):
    most = most_rows(length_ref[...], owner_ref[...], tokens)
    over_ref[0] = (most + jnp.max(ready_ref[...]) > FIT).astype(jnp.int32)


def crowded(ready, owner_slot, lengths, tokens):
    docs = owner_slot.shape[0]
    return pl.pallas_call(
        functools.partial(crowded_kernel, tokens),
        out_specs=pl.BlockSpec(memory_space=pltpu.SMEM),
        out_shape=jax.ShapeDtypeStruct((1,), jnp.int32),
        cost_estimate=pl.CostEstimate(
            flops=64 * docs * docs, bytes_accessed=8 * docs, transcendentals=0
        ),
        compiler_params=pltpu.CompilerParams(vmem_limit_bytes=GRANT),
        name="crowded",
    )(ready, owner_slot.reshape(1, -1), lengths.reshape(1, -1))


def place_rest_kernel(in_ref, out_ref):
    planes, per_plane, _ = out_ref.shape
    values, where, _, _, rank = slots_of(in_ref)
    row = iota((planes * per_plane, where.shape[1]), 0) + 1
    out_ref[...] = picked(ones((row == where) & (rank >= FIT)), values).reshape(out_ref.shape)


def place_rest(slots, planes, per_plane):
    return pl.pallas_call(
        place_rest_kernel,
        out_shape=jax.ShapeDtypeStruct((planes, per_plane, LANES), jnp.float32),
        compiler_params=pltpu.CompilerParams(vmem_limit_bytes=GRANT),
        name="place_rest",
    )(slots)


def average_kernel(owner_ref, length_ref, bias_ref, in_ref, *rest_and_out):
    out_ref = rest_and_out[-1]
    count = in_ref.shape[0]
    planes = count // ROWS
    per_plane = owner_ref.shape[1] // planes
    marks = in_ref[FIT:ROWS, :]
    for p in range(1, planes):
        marks = marks + in_ref[p * ROWS + FIT : (p + 1) * ROWS, :]
    marks = marks.astype(jnp.int32)
    part = iota((8, LANES), 0)
    halves = jnp.where(part == 0, marks & 63, jnp.where(part == 1, marks >> 6, 0))
    line = iota((LANES, count), 1)
    source = (line * 171) >> 11
    spread = dot(small(halves), ones(iota((LANES, count), 0) == source * PAIRS + ((line - source * ROWS) >> 1)))
    line = line[0:1, :]
    line = line - ((line * 171) >> 11) * ROWS
    where = jnp.where((line & 1) == 1, spread[1:2, :], spread[0:1, :]).astype(jnp.int32)
    where = jnp.where(line < FIT, where, 0)
    picker = ones(iota((per_plane, count), 0) + 1 == where)
    total = picked(picker, in_ref[...])
    for rest_ref in rest_and_out[:-1]:
        total = total + jnp.sum(rest_ref[...], axis=0)
    mine = plane_place(lax.axis_index("z")) * per_plane
    row = iota((per_plane, owner_ref.shape[1]), 0) + mine
    length = jnp.sum(
        jnp.where(row == plane_row(owner_ref[...]), length_ref[...], 0).astype(jnp.float32),
        axis=1,
        keepdims=True,
    )
    chunk = chunk_place()
    average = total / length + bias_ref[pl.ds(chunk, 1), :]
    owners, copies, rows, _ = out_ref.shape
    for o in range(owners):
        for y in range(copies):
            out_ref[o, y] = average[o * rows : (o + 1) * rows, :]


def averages_for_owners(arrived, owner_slot, lengths, pool_bias, owners, copies, *rest):
    rows = owner_slot.shape[0] // (arrived.shape[0] // ROWS * owners)
    return pl.pallas_call(
        average_kernel,
        out_shape=jax.ShapeDtypeStruct((owners, copies, rows, LANES), jnp.float32),
        compiler_params=pltpu.CompilerParams(vmem_limit_bytes=GRANT),
        name="average",
    )(owner_slot.reshape(1, -1), lengths.reshape(1, -1), pool_bias.reshape(-1, LANES), arrived, *rest)


def norm_kernel(in_ref, out_ref):
    chunks, slices, rows, _ = in_ref.shape
    every = in_ref[...]
    square = jnp.sum(every * every, axis=(0, 1))
    energy = jnp.sum(square, axis=1, keepdims=True) / (chunks * slices * LANES)
    scale = lax.rsqrt(energy + 1e-06)
    mine = slice_place()
    for c, device in enumerate(CHUNK_GROUP[0]):
        values = in_ref[device, mine] * scale
        out_ref[:, c * LANES : (c + 1) * LANES] = values.astype(jnp.bfloat16)


def normed(arrived):
    chunks, _, rows, _ = arrived.shape
    return pl.pallas_call(
        norm_kernel,
        out_shape=jax.ShapeDtypeStruct((rows, chunks * LANES), jnp.bfloat16),
        compiler_params=pltpu.CompilerParams(vmem_limit_bytes=GRANT),
        name="norm",
    )(arrived)


def swap(array, axes, group):
    return lax.all_to_all(
        array, axes, split_axis=0, concat_axis=0, tiled=True, axis_index_groups=group
    )


def local(hidden, seg_ids, lengths, owner_slot, pool_bias):
    chunks = lax.axis_size(("x", "c"))
    planes = lax.axis_size("z")
    slices = lax.axis_size("y")
    per_plane = lengths.shape[0] // planes
    sums = local_sums(seg_ids, owner_slot, hidden, chunks)
    slots = swap(sums.reshape(-1, 4, LANES), ("x", "c"), CHUNK_GROUP).reshape(sums.shape)
    placed, ready = place(slots, planes)
    over = crowded(ready, owner_slot, lengths, hidden.shape[0])
    rows = swap(placed.reshape(-1, 4, LANES), "z", PLANE_GROUP).reshape(placed.shape)
    args = (owner_slot, lengths, pool_bias, chunks, slices)

    def with_rest(rows, kept):
        rest = swap(place_rest(kept, planes, per_plane), "z", PLANE_GROUP)
        return averages_for_owners(rows, *args, rest)

    def alone(rows, kept):
        return averages_for_owners(rows, *args)

    average = lax.cond(over[0] > 0, with_rest, alone, rows, slots)
    mine = swap(average.reshape(chunks * slices, -1, LANES), ("x", "c", "y"), OWNER_GROUP)
    return normed(mine.reshape(average.shape))


def solution(mesh):
    torus = Mesh(mesh.devices.reshape(4, 16, 2, mesh.shape["hid"]), ("x", "z", "c", "y"))
    seq = ("x", "z", "c")
    return jax.shard_map(
        local,
        mesh=torus,
        in_specs=(P(seq, "y"), P(seq), P(), P(), P("y")),
        out_specs=P(seq, "y"),
        check_vma=False,
    )
```

```python
import functools

import jax
import jax.numpy as jnp
from jax import lax
from jax.experimental import pallas as pl
from jax.experimental.pallas import tpu as pltpu
from jax.sharding import Mesh
from jax.sharding import PartitionSpec as P

USED = 17
SLOTS = 20
LANES = 128
FIT = 11
ROWS = 12
PAIRS = 8
GRANT = 16 * 1024 * 1024
WIDE = 56 * 1024 * 1024


def chunk_place():
    return (((lax.axis_index("x") + 2) & 3) * 2 + lax.axis_index("c")) ^ 1


def plane_place(z):
    return (z + 6) & 15


def slice_place():
    return lax.axis_index("y")


CHUNK_GROUP = [[(((j >> 1) + 2) & 3) * 2 + (j & 1) ^ 1 for j in range(8)]]
PLANE_GROUP = [[(j + 10) & 15 for j in range(16)]]
OWNER_GROUP = [[j ^ 20 for j in range(32)]]


def plane_row(owner):
    return plane_place(owner >> 3) * 32 + (owner >> 7) * 8 + (owner & 7)


def ones(mask):
    return jnp.where(mask, 1.0, 0.0).astype(jnp.bfloat16)


def iota(shape, dim):
    return lax.broadcasted_iota(jnp.int32, shape, dim)


def small(array):
    return array.astype(jnp.float32).astype(jnp.bfloat16)


def dot(left, right):
    return jnp.dot(left, right, preferred_element_type=jnp.float32)


def dot_rows(left, right):
    return lax.dot_general(
        left, right, (((1,), (1,)), ((), ())), preferred_element_type=jnp.float32
    )


def picked(picker, values):
    high = values.astype(jnp.bfloat16)
    left_over = values - high.astype(jnp.float32)
    middle = left_over.astype(jnp.bfloat16)
    low = (left_over - middle.astype(jnp.float32)).astype(jnp.bfloat16)
    parts = dot(picker, jnp.concatenate([high, middle, low], axis=1))
    return parts[:, :LANES] + (parts[:, LANES : 2 * LANES] + parts[:, 2 * LANES :])


def marks_of(first, last, owner):
    docs = owner.shape[1]
    source = chunk_place()
    row = plane_row(owner) + 1
    part = iota((8, docs), 0)
    digits = jnp.where(part == 0, row >> 5, jnp.where(part == 1, row & 31, 0))
    lane = iota((docs, 2 * LANES), 1) - source * SLOTS
    doc = iota((docs, 2 * LANES), 0)
    meets = (doc == first + lane) & (doc <= last) & (lane >= 0) & (lane < USED)
    found = dot(small(digits), ones(meets))
    where = found[0:1, :] * 32.0 + found[1:2, :]
    line = iota((SLOTS, LANES), 0)
    second = jnp.where(line == SLOTS - 1, where[:, LANES:], 0.0)
    return jnp.where(line == SLOTS - 2, where[:, :LANES], second)


def most_rows(lengths, owner, tokens):
    docs = owner.shape[1]
    part = iota((8, docs), 0)
    digits = jnp.where(part == 0, lengths >> 7, jnp.where(part == 1, lengths & 127, 0))
    until = ones(iota((docs, docs), 0) <= iota((docs, docs), 1))
    sums = dot(small(digits), until)
    end = (sums[0:1, :] * 128.0 + sums[1:2, :]).astype(jnp.int32)
    start = end - lengths
    line = iota((LANES, docs), 0)
    device = (line >> 5) * 32 + (line & 15) * 2 + ((line >> 4) & 1)
    touches = (start < (device + 1) * tokens) & (end > device * tokens)
    owned = ((owner >> 3) & 15) == line
    counts = dot_rows(ones(touches), ones(owned))
    return jnp.max(jnp.sum(counts.reshape(8, 16, LANES), axis=0)).astype(jnp.int32)


def sums_kernel(
    pieces, seg_hbm, owner_hbm, hidden_hbm, out_ref, seg, owner, hidden, sems
):
    tokens = hidden.shape[0]
    rows = tokens // pieces
    copies = [
        pltpu.make_async_copy(seg_hbm, seg, sems.at[pieces]),
        pltpu.make_async_copy(owner_hbm, owner, sems.at[pieces + 1]),
    ]
    for p in range(pieces):
        here = pl.ds(p * rows, rows)
        copies.append(pltpu.make_async_copy(hidden_hbm.at[here], hidden.at[here], sems.at[p]))
    for copy in copies:
        copy.start()
    copies[0].wait()
    first = seg[0:1, 0:1]
    last = seg[0:1, tokens - 1 : tokens]
    copies[1].wait()
    marks = marks_of(first, last, owner[...])
    slot = iota((SLOTS, rows), 0) + first
    sums = None
    for p in range(pieces):
        picker = ones(slot == seg[:, p * rows : (p + 1) * rows])
        copies[2 + p].wait()
        term = dot(picker, hidden[p * rows : (p + 1) * rows, :])
        sums = term if sums is None else sums + term
    for c in range(out_ref.shape[0] // SLOTS):
        out_ref[c * SLOTS : (c + 1) * SLOTS, :] = sums[:, c * LANES : (c + 1) * LANES] + marks


def local_sums(seg_ids, owner_slot, hidden, chunks):
    tokens, width = hidden.shape
    docs = owner_slot.shape[0]
    pieces = 4
    return pl.pallas_call(
        functools.partial(sums_kernel, pieces),
        in_specs=[pl.BlockSpec(memory_space=pltpu.HBM)] * 3,
        out_specs=pl.BlockSpec(memory_space=pltpu.VMEM),
        out_shape=pltpu.VMEM((chunks * SLOTS, LANES), jnp.float32),
        scratch_shapes=[
            pltpu.VMEM((1, tokens), jnp.int32),
            pltpu.VMEM((1, docs), jnp.int32),
            pltpu.VMEM((tokens, width), hidden.dtype),
            pltpu.SemaphoreType.DMA((pieces + 2,)),
        ],
        compiler_params=pltpu.CompilerParams(vmem_limit_bytes=WIDE),
        name="local_sums",
    )(seg_ids.reshape(1, -1), owner_slot.reshape(1, -1), hidden)


def slots_of(in_ref):
    count = in_ref.shape[0]
    marks = in_ref[SLOTS - 2 : SLOTS, :]
    for row in range(2 * SLOTS, count + SLOTS, SLOTS):
        marks = marks + in_ref[row - 2 : row, :]
    marks = marks.astype(jnp.int32)
    where = jnp.concatenate([marks[0:1, :], marks[1:2, : count - LANES]], axis=1)
    plane = jnp.where(where > 0, (where - 1) >> 5, -1)
    bound = iota((16, count), 0) == plane
    ahead = iota((count, count), 0) < iota((count, count), 1)
    seen = dot(ones(bound), ones(ahead))
    rank = jnp.sum(jnp.where(bound, seen, 0.0), axis=0, keepdims=True).astype(jnp.int32)
    return in_ref[...], where, plane, bound, rank


def place_kernel(in_ref, out_ref, ready_ref):
    planes = out_ref.shape[0] // ROWS
    ready_ref[...] = jnp.zeros_like(ready_ref)
    values, where, plane, bound, rank = slots_of(in_ref)
    target = jnp.where((where > 0) & (rank < FIT), plane * ROWS + rank, -1)
    out_ref[...] = picked(ones(iota((planes * ROWS, where.shape[1]), 0) == target), values)
    number = (((where - 1) & 31) + 1) * jnp.where((rank & 1) == 1, 64, 1)
    lane = iota((LANES, where.shape[1]), 0) - plane_place(lax.axis_index("z")) * PAIRS
    numbers = dot_rows(small(jnp.where(bound, number, 0)), ones((lane == rank >> 1) & (rank < FIT)))
    for p in range(planes):
        out_ref[p * ROWS + FIT : (p + 1) * ROWS, :] = numbers[p : p + 1, :]


def place(slots, planes):
    return pl.pallas_call(
        place_kernel,
        out_specs=[
            pl.BlockSpec(memory_space=pltpu.VMEM),
            pl.BlockSpec(memory_space=pltpu.VMEM),
        ],
        out_shape=[
            pltpu.VMEM((planes * ROWS, LANES), jnp.float32),
            pltpu.VMEM((8, LANES), jnp.int32),
        ],
        compiler_params=pltpu.CompilerParams(vmem_limit_bytes=GRANT),
        name="place",
    )(slots)


def crowded_kernel(tokens, ready_ref, owner_ref, length_ref, over_ref):
    most = most_rows(length_ref[...], owner_ref[...], tokens)
    over_ref[0] = (most + jnp.max(ready_ref[...]) > FIT).astype(jnp.int32)


def crowded(ready, owner_slot, lengths, tokens):
    docs = owner_slot.shape[0]
    return pl.pallas_call(
        functools.partial(crowded_kernel, tokens),
        out_specs=pl.BlockSpec(memory_space=pltpu.SMEM),
        out_shape=jax.ShapeDtypeStruct((1,), jnp.int32),
        cost_estimate=pl.CostEstimate(
            flops=64 * docs * docs, bytes_accessed=8 * docs, transcendentals=0
        ),
        compiler_params=pltpu.CompilerParams(vmem_limit_bytes=GRANT),
        name="crowded",
    )(ready, owner_slot.reshape(1, -1), lengths.reshape(1, -1))


def place_rest_kernel(in_ref, out_ref):
    planes, per_plane, _ = out_ref.shape
    values, where, _, _, rank = slots_of(in_ref)
    row = iota((planes * per_plane, where.shape[1]), 0) + 1
    out_ref[...] = picked(ones((row == where) & (rank >= FIT)), values).reshape(out_ref.shape)


def place_rest(slots, planes, per_plane):
    return pl.pallas_call(
        place_rest_kernel,
        out_shape=jax.ShapeDtypeStruct((planes, per_plane, LANES), jnp.float32),
        compiler_params=pltpu.CompilerParams(vmem_limit_bytes=GRANT),
        name="place_rest",
    )(slots)


def average_kernel(owner_ref, length_ref, bias_ref, in_ref, *rest_and_out):
    out_ref = rest_and_out[-1]
    count = in_ref.shape[0]
    planes = count // ROWS
    per_plane = owner_ref.shape[1] // planes
    marks = in_ref[FIT:ROWS, :]
    for p in range(1, planes):
        marks = marks + in_ref[p * ROWS + FIT : (p + 1) * ROWS, :]
    marks = marks.astype(jnp.int32)
    part = iota((8, LANES), 0)
    halves = jnp.where(part == 0, marks & 63, jnp.where(part == 1, marks >> 6, 0))
    line = iota((LANES, count), 1)
    source = (line * 171) >> 11
    spread = dot(small(halves), ones(iota((LANES, count), 0) == source * PAIRS + ((line - source * ROWS) >> 1)))
    line = line[0:1, :]
    line = line - ((line * 171) >> 11) * ROWS
    where = jnp.where((line & 1) == 1, spread[1:2, :], spread[0:1, :]).astype(jnp.int32)
    where = jnp.where(line < FIT, where, 0)
    picker = ones(iota((per_plane, count), 0) + 1 == where)
    total = picked(picker, in_ref[...])
    for rest_ref in rest_and_out[:-1]:
        total = total + jnp.sum(rest_ref[...], axis=0)
    mine = plane_place(lax.axis_index("z")) * per_plane
    row = iota((per_plane, owner_ref.shape[1]), 0) + mine
    length = jnp.sum(
        jnp.where(row == plane_row(owner_ref[...]), length_ref[...], 0).astype(jnp.float32),
        axis=1,
        keepdims=True,
    )
    chunk = chunk_place()
    average = total / length + bias_ref[pl.ds(chunk, 1), :]
    owners, copies, rows, _ = out_ref.shape
    for o in range(owners):
        for y in range(copies):
            out_ref[o ^ 5, y] = average[o * rows : (o + 1) * rows, :]


def averages_for_owners(arrived, owner_slot, lengths, pool_bias, owners, copies, *rest):
    rows = owner_slot.shape[0] // (arrived.shape[0] // ROWS * owners)
    return pl.pallas_call(
        average_kernel,
        out_shape=jax.ShapeDtypeStruct((owners, copies, rows, LANES), jnp.float32),
        compiler_params=pltpu.CompilerParams(vmem_limit_bytes=GRANT),
        name="average",
    )(owner_slot.reshape(1, -1), lengths.reshape(1, -1), pool_bias.reshape(-1, LANES), arrived, *rest)


def norm_kernel(in_ref, out_ref):
    chunks, slices, rows, _ = in_ref.shape
    every = in_ref[...]
    square = jnp.sum(every * every, axis=(0, 1))
    energy = jnp.sum(square, axis=1, keepdims=True) / (chunks * slices * LANES)
    scale = lax.rsqrt(energy + 1e-06)
    mine = slice_place()
    for c, device in enumerate(CHUNK_GROUP[0]):
        values = in_ref[device ^ 5, mine] * scale
        out_ref[:, c * LANES : (c + 1) * LANES] = values.astype(jnp.bfloat16)


def normed(arrived):
    chunks, _, rows, _ = arrived.shape
    return pl.pallas_call(
        norm_kernel,
        out_shape=jax.ShapeDtypeStruct((rows, chunks * LANES), jnp.bfloat16),
        compiler_params=pltpu.CompilerParams(vmem_limit_bytes=GRANT),
        name="norm",
    )(arrived)


def swap(array, axes, group):
    return lax.all_to_all(
        array, axes, split_axis=0, concat_axis=0, tiled=True, axis_index_groups=group
    )


def local(hidden, seg_ids, lengths, owner_slot, pool_bias):
    chunks = lax.axis_size(("x", "c"))
    planes = lax.axis_size("z")
    slices = lax.axis_size("y")
    per_plane = lengths.shape[0] // planes
    sums = local_sums(seg_ids, owner_slot, hidden, chunks)
    slots = swap(sums.reshape(-1, 4, LANES), ("x", "c"), CHUNK_GROUP).reshape(sums.shape)
    placed, ready = place(slots, planes)
    over = crowded(ready, owner_slot, lengths, hidden.shape[0])
    rows = swap(placed.reshape(-1, 4, LANES), "z", PLANE_GROUP).reshape(placed.shape)
    args = (owner_slot, lengths, pool_bias, chunks, slices)

    def with_rest(rows, kept):
        rest = swap(place_rest(kept, planes, per_plane), "z", PLANE_GROUP)
        return averages_for_owners(rows, *args, rest)

    def alone(rows, kept):
        return averages_for_owners(rows, *args)

    average = lax.cond(over[0] > 0, with_rest, alone, rows, slots)
    mine = swap(average.reshape(chunks * slices, -1, LANES), ("x", "c", "y"), OWNER_GROUP)
    return normed(mine.reshape(average.shape))


def solution(mesh):
    torus = Mesh(mesh.devices.reshape(4, 16, 2, mesh.shape["hid"]), ("x", "z", "c", "y"))
    seq = ("x", "z", "c")
    return jax.shard_map(
        local,
        mesh=torus,
        in_specs=(P(seq, "y"), P(seq), P(), P(), P("y")),
        out_specs=P(seq, "y"),
        check_vma=False,
    )
```
